8 devices in a mesh: dp: 2 (over z, y), ep: 4 (over x, core).
Axes of the slice: x: 2, y: 2, z: 1, core: 2. Of those that a mesh axis runs over, the one named last changes fastest.
Arguments:
- x_a: bfloat16 [2048, 2304], P(('dp', 'ep')), parts along dimension 0
- route_a: int32 [2048, 2], P(('dp', 'ep')), parts along dimension 0
- gate_a: float32 [2048, 2], P(('dp', 'ep')), parts along dimension 0
- h_b: bfloat16 [2048, 2304], P(('dp', 'ep')), parts along dimension 0
- attn_b: bfloat16 [2048, 2304], P(('dp', 'ep')), parts along dimension 0
- route_b: int32 [2048, 2], P(('dp', 'ep')), parts along dimension 0
- gate_b: float32 [2048, 2], P(('dp', 'ep')), parts along dimension 0
- w_qkv: bfloat16 [2304, 6912], replicated
- w_o: bfloat16 [2304, 2304], replicated
- w_gate: bfloat16 [8, 2304, 5760], P('ep')
- w_up: bfloat16 [8, 2304, 5760], P('ep')
- w_down: bfloat16 [8, 5760, 2304], P('ep')
Outputs:
- output 1: bfloat16 [2048, 2304], P(('dp', 'ep')), parts along dimension 0
- output 2: bfloat16 [2048, 2304], P(('dp', 'ep')), parts along dimension 0
- output 3: bfloat16 [2048, 6912], P(('dp', 'ep')), parts along dimension 0
There are 2 independent parts. The reference program is written for one: setup_inputs(seed, part) draws one part's arguments, and reference() takes and returns one part's arrays. A program takes and returns all parts, laid end to end along the dimension named above; an argument that names none is the same for every part.
All inputs are finite; a program needn't handle non-finite values.
Results may differ from the reference program's by a relative error of at most 0.0121025.
Values are sent between devices in bfloat16 or wider.
A program may use at most 1 GiB of HBM per device.

```python
import jax
import jax.numpy as jnp
from jax import lax

MODEL_DIM = 2304
FF_DIM = 5760
NUM_EXPERTS = 8
TOP_K = 2
NUM_HEADS = 36
KV_HEADS = 36
HEAD_DIM = 64
TOKENS_DEV = 256
GROUP_DEVS = 4

CAPACITY = min(TOKENS_DEV, 2 * ((TOKENS_DEV * TOP_K + NUM_EXPERTS - 1) // NUM_EXPERTS))
LOCAL_EXPERTS = NUM_EXPERTS // GROUP_DEVS
QKV_DIM = (NUM_HEADS + 2 * KV_HEADS) * HEAD_DIM
ATTN_DIM = NUM_HEADS * HEAD_DIM
GROUP_ROWS = GROUP_DEVS * TOKENS_DEV
HOT_DEVS = max(1, GROUP_DEVS // 4)


def source_routing(rng_key, dev_order):
    key_local, key_want, key_rows = jax.random.split(rng_key, 3)
    local_order = jax.vmap(lambda sub_key: jax.random.permutation(sub_key, LOCAL_EXPERTS))(jax.random.split(key_local, GROUP_DEVS))
    visits = jnp.arange(NUM_EXPERTS)
    visit_dev = dev_order[visits % GROUP_DEVS]
    visit_expert = visit_dev * LOCAL_EXPERTS + local_order[visit_dev, visits // GROUP_DEVS]
    wanted = jax.random.randint(key_want, (NUM_EXPERTS,), 1, CAPACITY + 1)
    wanted = jnp.where(visits % GROUP_DEVS < HOT_DEVS, CAPACITY, wanted)
    wanted = jnp.where(visits < GROUP_DEVS, 1, wanted)
    wanted = jnp.where(visits == 0, CAPACITY, wanted)
    n_entries = TOKENS_DEV * TOP_K
    first_pass = jnp.clip(n_entries - (jnp.cumsum(wanted) - wanted), 0, wanted)
    room_left = CAPACITY - first_pass
    left_over = n_entries - jnp.sum(first_pass)
    second_pass = jnp.clip(left_over - (jnp.cumsum(room_left) - room_left), 0, room_left)
    run_ends = jnp.cumsum(first_pass + second_pass)
    positions = jnp.arange(n_entries)
    run_index = jnp.sum((run_ends[None, :] <= positions[:, None]).astype(jnp.int32), axis=1)
    choices = visit_expert[run_index].reshape(TOP_K, TOKENS_DEV).T
    return choices[jax.random.permutation(key_rows, TOKENS_DEV)]


def group_routing(rng_key):
    key_order, key_src = jax.random.split(rng_key)
    dev_order = jax.random.permutation(key_order, GROUP_DEVS)
    per_source = jax.vmap(lambda sub_key: source_routing(sub_key, dev_order))(jax.random.split(key_src, GROUP_DEVS))
    return per_source.reshape(GROUP_ROWS, TOP_K).astype(jnp.int32)


def setup_inputs(seed: int = 0, part: int = 0) -> dict:
    root_key = jax.random.key(seed)
    shared_keys = jax.random.split(jax.random.fold_in(root_key, 1), 5)
    part_keys = jax.random.split(jax.random.fold_in(jax.random.fold_in(root_key, 2), part), 7)

    def normal_bf16(sub_key, arr_shape, scale_by):
        return (jax.random.normal(sub_key, arr_shape, jnp.float32) * scale_by).astype(jnp.bfloat16)

    return {
        'x_a': normal_bf16(part_keys[0], (GROUP_ROWS, MODEL_DIM), 1.0),
        'route_a': group_routing(part_keys[1]),
        'gate_a': jax.nn.softmax(jax.random.normal(part_keys[2], (GROUP_ROWS, TOP_K), jnp.float32), axis=-1),
        'h_b': normal_bf16(part_keys[3], (GROUP_ROWS, MODEL_DIM), 1.0),
        'attn_b': normal_bf16(part_keys[4], (GROUP_ROWS, ATTN_DIM), 1.0),
        'route_b': group_routing(part_keys[5]),
        'gate_b': jax.nn.softmax(jax.random.normal(part_keys[6], (GROUP_ROWS, TOP_K), jnp.float32), axis=-1),
        'w_qkv': normal_bf16(shared_keys[0], (MODEL_DIM, QKV_DIM), MODEL_DIM ** -0.5),
        'w_o': normal_bf16(shared_keys[1], (ATTN_DIM, MODEL_DIM), ATTN_DIM ** -0.5),
        'w_gate': normal_bf16(shared_keys[2], (NUM_EXPERTS, MODEL_DIM, FF_DIM), MODEL_DIM ** -0.5),
        'w_up': normal_bf16(shared_keys[3], (NUM_EXPERTS, MODEL_DIM, FF_DIM), MODEL_DIM ** -0.5),
        'w_down': normal_bf16(shared_keys[4], (NUM_EXPERTS, FF_DIM, MODEL_DIM), FF_DIM ** -0.5),
    }


def expert_layer(tokens, route_ids, gate_vals, w_gate, w_up, w_down):
    n_entries = GROUP_ROWS * TOP_K
    per_source = route_ids.reshape(GROUP_DEVS, TOKENS_DEV * TOP_K)
    one_hot = (per_source[:, :, None] == jnp.arange(NUM_EXPERTS)[None, None, :]).astype(jnp.int32)
    slot_rank = jnp.sum((jnp.cumsum(one_hot, axis=1) - 1) * one_hot, axis=2)
    buffer_row = jnp.arange(GROUP_DEVS)[:, None] * CAPACITY + slot_rank
    entry_ids = jnp.arange(n_entries)
    slot_table = jnp.full((NUM_EXPERTS, GROUP_DEVS * CAPACITY), n_entries, jnp.int32)
    slot_table = slot_table.at[per_source.reshape(-1), buffer_row.reshape(-1)].set(entry_ids)
    padded = jnp.concatenate([tokens, jnp.zeros((1, MODEL_DIM), tokens.dtype)], axis=0)

    def one_expert(results, inputs):
        rows_ids, gate_w, up_w, down_w = inputs
        expert_in = padded[rows_ids // TOP_K]
        gate_act = jnp.dot(expert_in, gate_w, preferred_element_type=jnp.float32)
        up_act = jnp.dot(expert_in, up_w, preferred_element_type=jnp.float32)
        hidden = (jax.nn.silu(gate_act) * up_act).astype(jnp.bfloat16)
        expert_out = jnp.dot(hidden, down_w, preferred_element_type=jnp.float32).astype(jnp.bfloat16)
        return results.at[rows_ids].set(expert_out), None

    results = jnp.zeros((n_entries + 1, MODEL_DIM), jnp.bfloat16)
    results = lax.scan(one_expert, results, (slot_table, w_gate, w_up, w_down))[0]
    per_choice = results[:n_entries].reshape(GROUP_ROWS, TOP_K, MODEL_DIM)
    mixture = jnp.zeros((GROUP_ROWS, MODEL_DIM), jnp.float32)
    for choice in range(TOP_K):
        mixture = mixture + gate_vals[:, choice:choice + 1] * per_choice[:, choice].astype(jnp.float32)
    return (tokens.astype(jnp.float32) + mixture).astype(jnp.bfloat16)


def reference(x_a, route_a, gate_a, h_b, attn_b, route_b, gate_b, w_qkv, w_o, w_gate, w_up, w_down):
    out_a = expert_layer(x_a, route_a, gate_a, w_gate, w_up, w_down)
    qkv_b = jnp.dot(h_b, w_qkv, preferred_element_type=jnp.float32).astype(jnp.bfloat16)
    proj_b = jnp.dot(attn_b, w_o, preferred_element_type=jnp.float32).astype(jnp.bfloat16)
    mid_b = (h_b.astype(jnp.float32) + proj_b.astype(jnp.float32)).astype(jnp.bfloat16)
    out_b = expert_layer(mid_b, route_b, gate_b, w_gate, w_up, w_down)
    return (out_a, out_b, qkv_b)
```

```python
import functools

import jax
import jax.numpy as jnp
from jax import lax
from jax.experimental import pallas as pl
from jax.experimental.pallas import tpu as pltpu
from jax.sharding import PartitionSpec as P

BF16, F32, I32 = jnp.bfloat16, jnp.float32, jnp.int32
N_SRC = 4
SLOTS = 128
VARIANTS = (256, 384, 512)
VMEM_LIMIT = 63 * 2 ** 20

COL_POS, COL_GATE, COL_ALL, COL_MID_OWN, COL_MID_CNT, COL_TOP = 0, 8, 16, 21, 24, 27


def swap(x, k):
    return lax.ppermute(x, 'ep', [(i, i ^ k) for i in range(N_SRC)])


def route_kernel(me_ref, m0, m1, m2, m3, pos_a, tab_a, cnt_a, pos_b, tab_b, cnt_b):
    me = me_ref[0]
    metas = (m0, m1, m2, m3)
    n_tok = m0.shape[1]
    before = (lax.broadcasted_iota(I32, (n_tok, n_tok), 0)
              < lax.broadcasted_iota(I32, (n_tok, n_tok), 1)).astype(BF16)
    for mb, (pos_ref, tab_ref, cnt_ref) in enumerate(((pos_a, tab_a, cnt_a), (pos_b, tab_b, cnt_b))):
        sel, gate = [], []
        for l in range(2):
            e = (2 * me + l).astype(F32)
            for s in range(N_SRC):
                r = metas[s][...]
                h0 = (r[2 * mb:2 * mb + 1] == e).astype(F32)
                h1 = (r[2 * mb + 1:2 * mb + 2] == e).astype(F32)
                sel.append(h0 + h1)
                gate.append(h0 * r[4 + 2 * mb:5 + 2 * mb] + h1 * r[5 + 2 * mb:6 + 2 * mb])
        sel = jnp.concatenate(sel, axis=0)
        rank = jnp.dot(sel.astype(BF16), before, preferred_element_type=F32)
        pos = jnp.where(sel > 0, rank, -1.0)
        pos_ref[...] = pos
        cnt_ref[...] = jnp.broadcast_to(jnp.sum(sel, axis=1, keepdims=True), cnt_ref.shape).astype(I32)

        def owners(s):
            r = metas[s][...]
            counts, gates = [], []
            for k in range(N_SRC):
                lo = (2 * jnp.bitwise_xor(me, k)).astype(F32)
                o0 = jnp.logical_or(r[2 * mb:2 * mb + 1] == lo, r[2 * mb:2 * mb + 1] == lo + 1).astype(F32)
                o1 = jnp.logical_or(r[2 * mb + 1:2 * mb + 2] == lo, r[2 * mb + 1:2 * mb + 2] == lo + 1).astype(F32)
                counts.append(o0 + o1)
                gates.append(o0 * r[4 + 2 * mb:5 + 2 * mb] + o1 * r[5 + 2 * mb:6 + 2 * mb])
            return counts, gates

        def coefs(mix, gates):
            return [jnp.where(mix, 1.0, 0.0)] + [jnp.where(mix, g, 1.0) for g in gates]

        c, g = owners(0)
        whole = jnp.maximum(jnp.maximum(c[0], c[1]), jnp.maximum(c[2], c[3])) > 1.5
        rows = [pos] + gate + coefs(jnp.logical_not(whole), g)
        rows += coefs(jnp.logical_and(c[0] == 1.0, c[1] == 1.0), g[:2])
        c2, g2 = owners(2)
        rows += coefs(jnp.logical_and(c2[0] == 1.0, c2[1] == 1.0), g2[:2])
        rows += coefs(c[0] + c[1] == 1.0, [g[0] + g[1], g[2] + g[3]])
        rows = jnp.concatenate(rows + [jnp.zeros((128 - COL_TOP - 3, n_tok), F32)], axis=0)
        tab_ref[...] = rows.T


def route(me, metas):
    n_tok = metas[0].shape[1]
    one = [jax.ShapeDtypeStruct((8, n_tok), F32), jax.ShapeDtypeStruct((n_tok, 128), F32),
           jax.ShapeDtypeStruct((8, 128), I32)]
    return pl.pallas_call(
        route_kernel, out_shape=one + one,
        in_specs=[pl.BlockSpec(memory_space=pltpu.SMEM)] + [pl.BlockSpec(memory_space=pltpu.VMEM)] * 4,
        out_specs=[pl.BlockSpec(memory_space=pltpu.VMEM)] * 6,
        name='route',
    )(me, *metas)


def ffn_kernel(cfg, cnt, *refs):
    it = iter(refs)
    (gu, d0, dn, fc, dc, split, emit_h) = cfg
    pos = next(it) if gu else None
    tab = next(it)
    us = [next(it) for _ in range(N_SRC)]
    wg, wu = (next(it), next(it)) if gu else (None, None)
    h_in = None if gu else next(it)
    wd = next(it)
    outs = [next(it) for _ in range(3 if split else 4)]
    h_out = next(it) if emit_h else None
    x = next(it) if gu else None
    h = next(it)
    y = next(it)
    w1 = next(it) if gu else None
    w2 = next(it)
    s1 = next(it) if gu else None
    s2 = next(it)
    sh = next(it) if (emit_h or not gu) else None

    i = pl.program_id(0)
    ff = h.shape[2]
    nc = ff // fc
    n1 = 2 * nc if gu else 0
    ns1 = w1.shape[0] if gu else 0
    ns2 = w2.shape[0]

    def up(n):
        return lax.div(n + 15, 16) * 16

    def offset(l, s):
        off = 0
        for q in range(s):
            off = off + up(cnt[l * N_SRC + q, 0])
        return off

    def total(l):
        return offset(l, N_SRC)

    def copies1(j):
        l, c, s = lax.div(j, nc), lax.rem(j, nc), lax.rem(j, ns1)
        cols = pl.ds(pl.multiple_of(c * fc, 128), fc)
        return [pltpu.make_async_copy(wg.at[l, :, cols], w1.at[s, :, pl.ds(0, fc)], s1.at[s, 0]),
                pltpu.make_async_copy(wu.at[l, :, cols], w1.at[s, :, pl.ds(fc, fc)], s1.at[s, 1])]

    def copies2(j):
        s = lax.rem(j, ns2)
        cols = pl.ds(pl.multiple_of((d0 + j) * dc, 128), dc)
        return [pltpu.make_async_copy(wd.at[l, :, cols], w2.at[s, l], s2.at[s, l]) for l in range(2)]

    def start(copies):
        for c in copies:
            c.start()

    def for_rows(l, body):
        m, lo = total(l), 0
        for rows in VARIANTS:
            pl.when(jnp.logical_and(m > lo, m <= rows))(functools.partial(body, rows))
            lo = rows

    def h_copies(l, rows, out):
        a, b = h.at[l, pl.ds(0, rows)], (h_out if out else h_in).at[l, pl.ds(0, rows)]
        return pltpu.make_async_copy(a, b, sh.at[l]) if out else pltpu.make_async_copy(b, a, sh.at[l])

    if gu:
        @pl.when(i == 0)
        def _():
            for j in range(ns1 - 1):
                start(copies1(j))
            for l in range(2):
                for s in range(N_SRC):
                    q = l * N_SRC + s
                    pick = (lax.broadcasted_iota(I32, (SLOTS, us[s].shape[0]), 0).astype(F32) == pos[q:q + 1, :])
                    rows = jnp.dot(pick.astype(BF16), us[s][...], preferred_element_type=F32)
                    x[l, pl.ds(pl.multiple_of(offset(l, s), 16), SLOTS), :] = rows.astype(BF16)

        @pl.when(i + ns1 - 1 < n1)
        def _():
            start(copies1(i + ns1 - 1))

        @pl.when(i == n1 - 2)
        def _():
            for j in range(ns2 - 1):
                start(copies2(j))

        @pl.when(i < n1)
        def _():
            for c in copies1(i):
                c.wait()
            l, s = lax.div(i, nc), lax.rem(i, ns1)
            cols = pl.ds(pl.multiple_of(lax.rem(i, nc) * fc, 128), fc)

            def body(rows):
                r = jnp.dot(x[l, :rows], w1[s], preferred_element_type=F32)
                h[l, :rows, cols] = (jax.nn.silu(r[:, :fc]) * r[:, fc:]).astype(BF16)
            for_rows(l, body)
    else:
        @pl.when(i == 0)
        def _():
            for j in range(ns2 - 1):
                start(copies2(j))
            for l in range(2):
                for_rows(l, lambda rows, l=l: h_copies(l, rows, False).start())
            for l in range(2):
                for_rows(l, lambda rows, l=l: h_copies(l, rows, False).wait())

    @pl.when(i >= n1)
    def _():
        j = i - n1

        @pl.when(j + ns2 - 1 < dn)
        def _():
            start(copies2(j + ns2 - 1))

        if emit_h:
            @pl.when(j == 0)
            def _():
                for l in range(2):
                    for_rows(l, lambda rows, l=l: h_copies(l, rows, True).start())

        for c in copies2(j):
            c.wait()
        s = lax.rem(j, ns2)
        for l in range(2):
            def body(rows, l=l):
                y[l, :rows] = jnp.dot(h[l, :rows], w2[s, l], preferred_element_type=F32).astype(BF16)
            for_rows(l, body)
        t = tab[...]
        ucols = pl.ds(pl.multiple_of((d0 + j) * dc, 128), dc)
        for q in range(N_SRC):
            vals, has = [], []
            n_tok = us[q].shape[0]
            for l in range(2):
                k = l * N_SRC + q
                p = t[:, COL_POS + k:COL_POS + k + 1]
                rows = y[l, pl.ds(pl.multiple_of(offset(l, q), 16), SLOTS), :].astype(F32)
                live = lax.broadcasted_iota(I32, rows.shape, 0) < cnt[k, 0]
                rows = jnp.where(live, rows, 0.0).astype(BF16)
                pick = (p == lax.broadcasted_iota(I32, (n_tok, SLOTS), 1).astype(F32)).astype(BF16)
                vals.append(jnp.dot(pick, rows, preferred_element_type=F32))
                has.append(p >= 0.0)
            g0 = t[:, COL_GATE + q:COL_GATE + q + 1]
            g1 = t[:, COL_GATE + N_SRC + q:COL_GATE + N_SRC + q + 1]
            u = us[q][:, ucols] if gu else us[q][...]
            full = u.astype(F32) + (g0 * vals[0] + g1 * vals[1])
            both = jnp.broadcast_to(jnp.logical_and(has[0], has[1]), full.shape)
            res = jnp.where(both, full, vals[0] + vals[1]).astype(BF16)
            if split:
                if q == 0:
                    outs[0][...] = res
                elif q == 2:
                    outs[1][...] = res
                else:
                    outs[2][(q // 2) * n_tok:(q // 2 + 1) * n_tok] = res
            else:
                outs[q][...] = res

        if emit_h:
            @pl.when(j == dn - 1)
            def _():
                for l in range(2):
                    for_rows(l, lambda rows, l=l: h_copies(l, rows, True).wait())


def ffn(cnt, pos, tab, us, wg, wu, wd, *, h_in=None, d0=0, dn=None, split=False, emit_h=False, name):
    n_tok, d = us[0].shape
    ff = wd.shape[1]
    gu = h_in is None
    fc, dc = 640, 256
    dn = d // dc if dn is None else dn
    n1 = 2 * (ff // fc) if gu else 0
    ns1, ns2 = 2, 2
    rows = N_SRC * SLOTS
    cfg = (gu, d0, dn, fc, dc, split, emit_h)
    whole = lambda a: pl.BlockSpec(a.shape, lambda i, c: (0,) * a.ndim, pipeline_mode=pl.Buffered(1))
    hbm = pl.BlockSpec(memory_space=pl.ANY)
    col = lambda i, c: (0, jnp.maximum(i - n1, 0))
    args, specs = [], []
    if gu:
        args.append(pos)
        specs.append(whole(pos))
    args += [tab] + list(us)
    specs += [whole(tab)] + [whole(u) if gu else pl.BlockSpec((n_tok, dc), lambda i, c: (0, d0 + i)) for u in us]
    if gu:
        args += [wg, wu]
        specs += [hbm, hbm]
    else:
        args.append(h_in)
        specs.append(hbm)
    args.append(wd)
    specs.append(hbm)
    heights = (n_tok, n_tok, 2 * n_tok) if split else (n_tok,) * 4
    outs = [jax.ShapeDtypeStruct((r, dn * dc), BF16) for r in heights]
    out_specs = [pl.BlockSpec((r, dc), col) for r in heights]
    if emit_h:
        outs.append(jax.ShapeDtypeStruct((2, rows, ff), BF16))
        out_specs.append(hbm)
    scratch = [pltpu.VMEM((2, rows, d), BF16)] if gu else []
    scratch += [pltpu.VMEM((2, rows, ff), BF16), pltpu.VMEM((2, rows, dc), BF16)]
    if gu:
        scratch.append(pltpu.VMEM((ns1, d, 2 * fc), BF16))
    scratch.append(pltpu.VMEM((ns2, 2, ff, dc), BF16))
    if gu:
        scratch.append(pltpu.SemaphoreType.DMA((ns1, 2)))
    scratch.append(pltpu.SemaphoreType.DMA((ns2, 2)))
    if emit_h or not gu:
        scratch.append(pltpu.SemaphoreType.DMA((2,)))
    flops = (4 * d * ff * rows * 2 if gu else 0) + 2 * dn * dc * ff * rows * 2
    return pl.pallas_call(
        functools.partial(ffn_kernel, cfg), out_shape=outs,
        grid_spec=pltpu.PrefetchScalarGridSpec(num_scalar_prefetch=1, grid=(n1 + dn,), in_specs=specs,
                                               out_specs=out_specs, scratch_shapes=scratch),
        compiler_params=pltpu.CompilerParams(vmem_limit_bytes=VMEM_LIMIT),
        cost_estimate=pl.CostEstimate(flops=flops, bytes_accessed=flops // 512, transcendentals=0),
        name=name,
    )(cnt, *args)


def mix_kernel(col, tab, u, *refs):
    t = tab[...]
    acc = None
    for k, r in enumerate(refs[:-1]):
        term = t[:, col + 1 + k:col + 2 + k] * r[...].astype(F32)
        acc = term if acc is None else acc + term
    refs[-1][...] = (t[:, col:col + 1] * u[...].astype(F32) + acc).astype(BF16)


def mix(tab, col, u, rows, *, c0=0, name):
    n_tok = u.shape[0]
    width = rows[0][0].shape[1]
    bw = 768
    return pl.pallas_call(
        functools.partial(mix_kernel, col),
        out_shape=jax.ShapeDtypeStruct((n_tok, width), BF16),
        grid=(width // bw,),
        in_specs=[pl.BlockSpec(tab.shape, lambda i: (0, 0)),
                  pl.BlockSpec((n_tok, bw), lambda i: (0, c0 // bw + i))]
        + [pl.BlockSpec((n_tok, bw), lambda i, b=b: (b, i)) for _, b in rows],
        out_specs=pl.BlockSpec((n_tok, bw), lambda i: (0, i)),
        cost_estimate=pl.CostEstimate(flops=8 * 10 ** 8, bytes_accessed=10 ** 6, transcendentals=0),
        name=name,
    )(tab, u, *[a for a, _ in rows])


def solution(mesh):
    def local_step(x_a, route_a, gate_a, h_b, attn_b, route_b, gate_b, w_qkv, w_o, w_gate, w_up, w_down):
        me = lax.axis_index('ep').astype(I32).reshape(1)
        meta = jnp.concatenate([route_a.T.astype(F32), route_b.T.astype(F32), gate_a.T, gate_b.T], axis=0)
        m_cnt = swap(meta, 2)
        m_par, m_dia = swap(meta, 1), swap(meta, 3)
        x_cnt = swap(x_a, 2)
        x_par = swap(x_a, 1)
        proj_b = jnp.dot(attn_b, w_o, preferred_element_type=F32).astype(BF16)
        mid_b = (h_b.astype(F32) + proj_b.astype(F32)).astype(BF16)
        x_dia = swap(x_cnt, 1)
        b_par, b_cnt, b_dia = swap(mid_b, 1), swap(mid_b, 2), swap(mid_b, 3)
        qkv_b = jnp.dot(h_b, w_qkv, preferred_element_type=F32).astype(BF16)
        pos_a, tab_a, cnt_a, pos_b, tab_b, cnt_b = route(me, (meta, m_par, m_cnt, m_dia))

        ra = ffn(cnt_a, pos_a, tab_a, (x_a, x_par, x_cnt, x_dia), w_gate, w_up, w_down, name='ffn_a')
        a_par, a_cnt, a_dia = swap(ra[1], 1), swap(ra[2], 2), swap(ra[3], 3)

        us = (mid_b, b_par, b_cnt, b_dia)
        kw = dict(split=True, dn=3)
        o0, c0, s0, h = ffn(cnt_b, pos_b, tab_b, us, w_gate, w_up, w_down, emit_h=True, name='ffn_b0', **kw)
        parts = [(o0, c0, s0)]
        for k in (1, 2):
            parts.append(ffn(cnt_b, None, tab_b, us, None, None, w_down, h_in=h, d0=3 * k, name='ffn_b%d' % k, **kw))
        out_a = mix(tab_a, COL_ALL, x_a, [(ra[0], 0), (a_par, 0), (a_cnt, 0), (a_dia, 0)], name='mix_a')
        outs = []
        for k, (own, cnt, snd) in enumerate(parts):
            got = swap(snd, 1)
            there = mix(tab_b, COL_MID_CNT, b_cnt, [(cnt, 0), (got, 1)], c0=768 * k, name='mid_cnt%d' % k)
            back = swap(there, 2)
            here = mix(tab_b, COL_MID_OWN, mid_b, [(own, 0), (got, 0)], c0=768 * k, name='mid_own%d' % k)
            outs.append(mix(tab_b, COL_TOP, mid_b, [(here, 0), (back, 0)], c0=768 * k, name='top%d' % k))
        return out_a, jnp.concatenate(outs, axis=1), qkv_b

    row = P(('dp', 'ep'), None)
    full = P(None, None)
    expert = P('ep', None, None)
    return jax.shard_map(
        local_step, mesh=mesh,
        in_specs=(row,) * 7 + (full, full, expert, expert, expert),
        out_specs=(row, row, row), check_vma=False)
```

```python
import functools

import jax
import jax.numpy as jnp
from jax import lax
from jax.experimental import pallas as pl
from jax.experimental.pallas import tpu as pltpu
from jax.sharding import PartitionSpec as P


BF16, F32, I32 = jnp.bfloat16, jnp.float32, jnp.int32
N_SRC = 4
SLOTS = 128
HALF = 512
VARIANTS = (256, 384, 512)
FC, DC = 640, 256
MIB = 2 ** 20

COL_POS, COL_BOTH, COL_OWN, COL_CNT, COL_TOP = 0, 16, 28, 31, 34


def swap(x, k):
    return lax.ppermute(x, 'ep', [(i, i ^ k) for i in range(N_SRC)])


def after(x, dep):
    return lax.optimization_barrier((x, dep))[0]


def route_kernel(me_ref, meta_ref, pos_ref, tab_ref, cnt_ref):
    me = me_ref[0]
    n_tok = meta_ref.shape[2]
    before = (lax.broadcasted_iota(I32, (n_tok, n_tok), 0)
              < lax.broadcasted_iota(I32, (n_tok, n_tok), 1)).astype(BF16)
    metas = [meta_ref[jnp.bitwise_xor(me, s)] for s in range(N_SRC)]
    for mb in range(2):
        r0 = [m[2 * mb:2 * mb + 1] for m in metas]
        r1 = [m[2 * mb + 1:2 * mb + 2] for m in metas]
        g0 = [m[4 + 2 * mb:5 + 2 * mb] for m in metas]
        g1 = [m[5 + 2 * mb:6 + 2 * mb] for m in metas]
        sel, gate = [], []
        for l in range(2):
            e = (2 * me + l).astype(F32)
            for s in range(N_SRC):
                h0 = (r0[s] == e).astype(F32)
                h1 = (r1[s] == e).astype(F32)
                sel.append(h0 + h1)
                gate.append(h0 * g0[s] + h1 * g1[s])
        both = []
        for s in range(N_SRC):
            b = sel[s] + sel[N_SRC + s] > 1.5
            both += [b.astype(F32), jnp.where(b, gate[s], 1.0), jnp.where(b, gate[N_SRC + s], 1.0)]
        sel = jnp.concatenate(sel, axis=0)
        rank = jnp.dot(sel.astype(BF16), before, preferred_element_type=F32)
        pos = jnp.where(sel > 0, rank, -1.0)
        pos_ref[mb] = pos
        cnt_ref[mb] = jnp.broadcast_to(jnp.sum(sel, axis=1, keepdims=True), cnt_ref.shape[1:]).astype(I32)

        def owners(s):
            counts, gates = [], []
            for k in range(N_SRC):
                lo = (2 * jnp.bitwise_xor(me, k)).astype(F32)
                o0 = jnp.logical_or(r0[s] == lo, r0[s] == lo + 1).astype(F32)
                o1 = jnp.logical_or(r1[s] == lo, r1[s] == lo + 1).astype(F32)
                counts.append(o0 + o1)
                gates.append(o0 * g0[s] + o1 * g1[s])
            return counts, gates

        def coefs(mix, gates):
            return [jnp.where(mix, 1.0, 0.0)] + [jnp.where(mix, g, 1.0) for g in gates]

        c, g = owners(0)
        c2, g2 = owners(2)
        rows = [pos] + gate + both
        rows += coefs(jnp.logical_and(c[0] == 1.0, c[1] == 1.0), g[:2])
        rows += coefs(jnp.logical_and(c2[0] == 1.0, c2[1] == 1.0), g2[:2])
        rows += coefs(c[0] + c[1] == 1.0, [g[0] + g[1], g[2] + g[3]])
        rows = jnp.concatenate(rows + [jnp.zeros((128 - COL_TOP - 3, n_tok), F32)], axis=0)
        tab_ref[mb] = rows.T


def route(me, meta):
    n_tok = meta.shape[2]
    return pl.pallas_call(
        route_kernel,
        out_shape=[jax.ShapeDtypeStruct((2, 8, n_tok), F32), jax.ShapeDtypeStruct((2, n_tok, 128), F32),
                   jax.ShapeDtypeStruct((2, 8, 128), I32)],
        in_specs=[pl.BlockSpec(memory_space=pltpu.SMEM), pl.BlockSpec(memory_space=pltpu.VMEM)],
        out_specs=[pl.BlockSpec(memory_space=pltpu.VMEM)] * 3,
        name='route',
    )(me, meta)


def offset(cnt, l, loc, k):
    off = 0
    for q in range(k):
        n = cnt[q // 2, l * N_SRC + 2 * loc + q % 2, 0]
        off = off + lax.div(n + 15, 16) * 16
    return off


def for_rows(m, body):
    lo = 0
    for rows in VARIANTS:
        pl.when(jnp.logical_and(m > lo, m <= rows))(functools.partial(body, rows))
        lo = rows


def up_kernel(loc, ff, cnt, pos, ua0, ua1, ub0, ub1, wg, wu, h, x, w, sem):
    i = pl.program_id(0)
    us = (ua0, ua1, ub0, ub1)
    nc = ff // FC
    n, ns = 2 * nc, w.shape[0]

    def copies(j):
        l, c, s = lax.div(j, nc), lax.rem(j, nc), lax.rem(j, ns)
        cols = pl.ds(pl.multiple_of(c * FC, 128), FC)
        return [pltpu.make_async_copy(wg.at[l, :, cols], w.at[s, :, pl.ds(0, FC)], sem.at[s, 0]),
                pltpu.make_async_copy(wu.at[l, :, cols], w.at[s, :, pl.ds(FC, FC)], sem.at[s, 1])]

    @pl.when(i == 0)
    def _():
        for j in range(ns - 1):
            for c in copies(j):
                c.start()
        x[...] = jnp.zeros_like(x)
        for l in range(2):
            for k in range(4):
                q = l * N_SRC + 2 * loc + k % 2
                p = pos[k // 2, q:q + 1, :]
                pick = (lax.broadcasted_iota(I32, (SLOTS, p.shape[1]), 0).astype(F32) == p).astype(BF16)
                rows = jnp.dot(pick, us[k][...], preferred_element_type=F32)
                x[l, pl.ds(pl.multiple_of(offset(cnt, l, loc, k), 16), SLOTS), :] = rows.astype(BF16)

    @pl.when(i + ns - 1 < n)
    def _():
        for c in copies(i + ns - 1):
            c.start()

    for c in copies(i):
        c.wait()
    l, s = lax.div(i, nc), lax.rem(i, ns)

    def body(rows):
        r = jnp.dot(x[l, :rows], w[s], preferred_element_type=F32)
        h[0, :rows] = (jax.nn.silu(r[:, :FC]) * r[:, FC:]).astype(BF16)

    for_rows(offset(cnt, l, loc, 4), body)


def up(loc, cnt, pos, us, wg, wu):
    d, ff = wg.shape[1:]
    ns = 3
    vmem, hbm = pl.BlockSpec(memory_space=pltpu.VMEM), pl.BlockSpec(memory_space=pl.ANY)
    flops = 4 * d * ff * 2 * HALF
    return pl.pallas_call(
        functools.partial(up_kernel, loc, ff),
        out_shape=jax.ShapeDtypeStruct((2, HALF, ff), BF16),
        grid_spec=pltpu.PrefetchScalarGridSpec(
            num_scalar_prefetch=1, grid=(2 * (ff // FC),), in_specs=[vmem] * 5 + [hbm, hbm],
            out_specs=pl.BlockSpec((1, HALF, FC), lambda i, c: (lax.div(i, ff // FC), 0, lax.rem(i, ff // FC))),
            scratch_shapes=[pltpu.VMEM((2, HALF, d), BF16), pltpu.VMEM((ns, d, 2 * FC), BF16),
                            pltpu.SemaphoreType.DMA((ns, 2))]),
        compiler_params=pltpu.CompilerParams(vmem_limit_bytes=63 * MIB),
        cost_estimate=pl.CostEstimate(flops=flops, bytes_accessed=flops // 512, transcendentals=0),
    )(cnt, pos, *us, wg, wu)


def down_kernel(d0, cnt, tab, *refs):
    us, (h0, h1, wd, keep, send, h, y, w, pick, coef, sem, sem_h) = refs[:8], refs[8:]
    i = pl.program_id(0)
    n, ns = pl.num_programs(0), w.shape[0]
    n_tok = tab.shape[1]
    l = lax.rem(i, 2)

    def copy(j):
        s = lax.rem(j, ns)
        cols = pl.ds(pl.multiple_of(d0 + lax.div(j, 2) * DC, 128), DC)
        return pltpu.make_async_copy(wd.at[lax.rem(j, 2), :, cols], w.at[s], sem.at[s])

    def h_copy(e, loc, rows):
        src = (h0, h1)[loc].at[e, pl.ds(0, rows)]
        return pltpu.make_async_copy(src, h.at[loc, e, pl.ds(0, rows)], sem_h.at[loc, e])

    @pl.when(i == 0)
    def _():
        copy(0).start()
        for e in range(2):
            for loc in range(2):
                for_rows(offset(cnt, e, loc, 4), lambda rows, e=e, loc=loc: h_copy(e, loc, rows).start())
        for j in range(1, ns - 1):
            copy(j).start()
        y[...] = jnp.zeros_like(y)
        lane = lax.broadcasted_iota(I32, (n_tok, SLOTS), 1).astype(F32)
        for mb in range(2):
            t = tab[mb]
            for q in range(2 * N_SRC):
                pick[mb, q] = (t[:, COL_POS + q:COL_POS + q + 1] == lane).astype(BF16)
            for q in range(3 * N_SRC):
                coef[mb, q] = jnp.broadcast_to(t[:, COL_BOTH + q:COL_BOTH + q + 1], (n_tok, 128))

    @pl.when(i + ns - 1 < n)
    def _():
        copy(i + ns - 1).start()

    copy(i).wait()
    s = lax.rem(i, ns)
    for loc in range(2):
        m = offset(cnt, l, loc, 4)

        @pl.when(i < 2)
        def _(loc=loc, m=m):
            for_rows(m, lambda rows: h_copy(l, loc, rows).wait())

        def body(rows, loc=loc):
            y[l, loc, :rows] = jnp.dot(h[loc, l, :rows], w[s], preferred_element_type=F32).astype(BF16)

        for_rows(m, body)

    @pl.when(l == 1)
    def _():
        for mb in range(2):
            for q in range(N_SRC):
                loc, k = q // 2, 2 * mb + q % 2
                vals = []
                for e in range(2):
                    rows = y[e, loc, pl.ds(pl.multiple_of(offset(cnt, e, loc, k), 16), SLOTS), :]
                    vals.append(jnp.dot(pick[mb, e * N_SRC + q], rows, preferred_element_type=F32))
                u = us[mb * N_SRC + q]
                out = send if q % 2 else keep
                for c in range(DC // 128):
                    cs = slice(c * 128, (c + 1) * 128)
                    mixed = coef[mb, 3 * q + 1] * vals[0][:, cs] + coef[mb, 3 * q + 2] * vals[1][:, cs]
                    res = coef[mb, 3 * q] * u[:, cs].astype(F32) + mixed
                    r0 = (2 * mb + loc) * n_tok
                    out[r0:r0 + n_tok, cs] = res.astype(BF16)


def down(cnt, tab, us, h0, h1, wd, d0, width):
    n_tok, _ = us[0].shape
    ff = wd.shape[1]
    ns = 4
    vmem, hbm = pl.BlockSpec(memory_space=pltpu.VMEM), pl.BlockSpec(memory_space=pl.ANY)
    flops = 2 * width * ff * 4 * HALF
    out = jax.ShapeDtypeStruct((4 * n_tok, width), BF16)
    out_spec = pl.BlockSpec((4 * n_tok, DC), lambda i, c: (0, lax.div(i, 2)))
    return pl.pallas_call(
        functools.partial(down_kernel, d0), out_shape=[out, out],
        grid_spec=pltpu.PrefetchScalarGridSpec(
            num_scalar_prefetch=1, grid=(2 * (width // DC),),
            in_specs=[vmem] + [pl.BlockSpec((n_tok, DC), lambda i, c: (0, d0 // DC + lax.div(i, 2)))] * 8
            + [hbm, hbm, hbm],
            out_specs=[out_spec, out_spec],
            scratch_shapes=[pltpu.VMEM((2, 2, HALF, ff), BF16), pltpu.VMEM((2, 2, HALF, DC), BF16),
                            pltpu.VMEM((ns, ff, DC), BF16),
                            pltpu.VMEM((2, 2 * N_SRC, n_tok, SLOTS), BF16),
                            pltpu.VMEM((2, 3 * N_SRC, n_tok, 128), F32),
                            pltpu.SemaphoreType.DMA((ns,)), pltpu.SemaphoreType.DMA((2, 2))]),
        compiler_params=pltpu.CompilerParams(vmem_limit_bytes=63 * MIB),
        cost_estimate=pl.CostEstimate(flops=flops, bytes_accessed=flops // 512, transcendentals=0),
    )(cnt, tab, *us, h0, h1, wd)


def lincomb(t, col, u, a, b):
    return (t[:, col:col + 1] * u.astype(F32)
            + (t[:, col + 1:col + 2] * a.astype(F32) + t[:, col + 2:col + 3] * b.astype(F32))).astype(BF16)


def there_kernel(tab, u0, u1, keep, got, out):
    n = u0.shape[0]
    for mb, u in enumerate((u0, u1)):
        r = slice((2 * mb + 1) * n, (2 * mb + 2) * n)
        out[mb * n:(mb + 1) * n] = lincomb(tab[mb], COL_CNT, u[...], keep[r], got[r])


def top_kernel(tab, u0, u1, keep, got, back, *refs):
    n = u0.shape[0]
    for mb, (u, out) in enumerate(((u0, refs[-2]), (u1, refs[-1]))):
        r = slice(2 * mb * n, (2 * mb + 1) * n)
        here = lincomb(tab[mb], COL_OWN, u[...], keep[r], got[r])
        out[...] = lincomb(tab[mb], COL_TOP, u[...], here, back[mb * n:(mb + 1) * n])


def mix_specs(tab, u, keep, d0):
    n, width = u.shape[0], keep.shape[1]
    cols = pl.BlockSpec((n, width), lambda i: (0, d0 // width))
    full = lambda a: pl.BlockSpec(a, lambda i: (0,) * len(a))
    return n, width, cols, full, [full(tab.shape), cols, cols, full(keep.shape), full(keep.shape)]


def there_rows(tab, us, keep, got, d0):
    n, width, _, full, specs = mix_specs(tab, us[0], keep, d0)
    return pl.pallas_call(
        there_kernel, out_shape=jax.ShapeDtypeStruct((2 * n, width), BF16), grid=(1,),
        in_specs=specs, out_specs=full((2 * n, width)),
        cost_estimate=pl.CostEstimate(flops=10 ** 9, bytes_accessed=10 ** 6, transcendentals=0),
    )(tab, *us, keep, got)


def top_rows(tab, us, keep, got, back, d0, prev):
    _, _, cols, full, specs = mix_specs(tab, us[0], keep, d0)
    specs = specs + [full(back.shape)] + [pl.BlockSpec(memory_space=pl.ANY)] * len(prev)
    out = jax.ShapeDtypeStruct(us[0].shape, BF16)
    return pl.pallas_call(
        top_kernel, out_shape=[out, out], grid=(1,), in_specs=specs, out_specs=[cols, cols],
        input_output_aliases={6: 0, 7: 1} if prev else {},
        cost_estimate=pl.CostEstimate(flops=10 ** 9, bytes_accessed=10 ** 6, transcendentals=0),
    )(tab, *us, keep, got, back, *prev)


def dense_kernel(x, w, *refs):
    refs[-1][...] = jnp.dot(x[...], w[...], preferred_element_type=F32).astype(BF16)


def dense_part(x, w, c0, width, prev):
    n, d = x.shape
    bw = 256
    return pl.pallas_call(
        dense_kernel, out_shape=jax.ShapeDtypeStruct((n, w.shape[1]), BF16), grid=(width // bw,),
        in_specs=[pl.BlockSpec((n, d), lambda i: (0, 0)), pl.BlockSpec((d, bw), lambda i: (0, c0 // bw + i))]
        + [pl.BlockSpec(memory_space=pl.ANY)] * len(prev),
        out_specs=pl.BlockSpec((n, bw), lambda i: (0, c0 // bw + i)),
        input_output_aliases={2: 0} if prev else {},
        cost_estimate=pl.CostEstimate(flops=2 * n * d * width, bytes_accessed=2 * d * width, transcendentals=0),
    )(x, w, *prev)


WIDTH = 768


def solution(mesh):
    def layer(x_a, route_a, gate_a, h_b, attn_b, route_b, gate_b, w_qkv, w_o, w_gate, w_up, w_down):
        d = x_a.shape[1]
        me = lax.axis_index('ep').astype(I32).reshape(1)
        meta = jnp.concatenate([route_a.T.astype(F32), route_b.T.astype(F32), gate_a.T, gate_b.T], axis=0)
        meta = lax.all_gather(meta, 'ep')
        x_a = after(x_a, meta)
        x_par, x_cnt = swap(x_a, 1), swap(x_a, 2)
        proj_b = jnp.dot(attn_b, w_o, preferred_element_type=F32).astype(BF16)
        mid_b = (h_b.astype(F32) + proj_b.astype(F32)).astype(BF16)
        b_par, b_cnt = swap(mid_b, 1), swap(mid_b, 2)
        pos, tab, cnt = route(me, meta)

        h_loc = up(0, cnt, pos, (x_a, x_par, mid_b, b_par), w_gate, w_up)
        x_cnt, b_cnt = after((x_cnt, b_cnt), h_loc)
        x_dia, b_dia = swap(x_cnt, 1), swap(b_cnt, 1)
        h_rem = up(1, cnt, pos, (x_cnt, x_dia, b_cnt, b_dia), w_gate, w_up)

        us = (x_a, x_par, x_cnt, x_dia, mid_b, b_par, b_cnt, b_dia)
        own, other = (x_a, mid_b), (x_cnt, b_cnt)
        tag, parts, qkv = h_rem, [], []
        for k in range(d // WIDTH):
            keep, send = down(after(cnt, tag), tab, us, h_loc, h_rem, w_down, k * WIDTH, WIDTH)
            got = swap(send, 1)
            qkv = [dense_part(after(h_b, keep), w_qkv, k * d, d, qkv)]
            there = there_rows(after(tab, qkv[0]), other, keep, got, k * WIDTH)
            parts.append((keep, got, swap(there, 2)))
            tag = there
        out = []
        for k, (keep, got, back) in enumerate(parts):
            out = top_rows(tab, own, keep, got, back, k * WIDTH, out)
        return out[0], out[1], qkv[0]

    row = P(('dp', 'ep'), None)
    full = P(None, None)
    expert = P('ep', None, None)
    return jax.shard_map(
        layer, mesh=mesh,
        in_specs=(row,) * 7 + (full, full, expert, expert, expert),
        out_specs=(row, row, row), check_vma=False)
```

```python
import functools

import jax
import jax.numpy as jnp
from jax import lax
from jax.experimental import pallas as pl
from jax.experimental.pallas import tpu as pltpu
from jax.sharding import PartitionSpec as P


BF16, F32, I32 = jnp.bfloat16, jnp.float32, jnp.int32
N_SRC = 4
SLOTS = 128
HALF = 512
VARIANTS = (256, 384, 512)
FC, DC = 640, 256
MIB = 2 ** 20

COL_POS, COL_BOTH, COL_OWN, COL_CNT, COL_TOP = 0, 16, 28, 31, 34


def swap(x, k):
    return lax.ppermute(x, 'ep', [(i, i ^ k) for i in range(N_SRC)])


def after(x, dep):
    return lax.optimization_barrier((x, dep))[0]


def route_kernel(me_ref, m0, m1, m2, m3, pos_ref, tab_ref, cnt_ref):
    me = me_ref[0]
    n_tok = m0.shape[1]
    before = (lax.broadcasted_iota(I32, (n_tok, n_tok), 0)
              < lax.broadcasted_iota(I32, (n_tok, n_tok), 1)).astype(BF16)
    metas = [m[...] for m in (m0, m1, m2, m3)]
    for mb in range(2):
        r0 = [m[2 * mb:2 * mb + 1] for m in metas]
        r1 = [m[2 * mb + 1:2 * mb + 2] for m in metas]
        g0 = [m[4 + 2 * mb:5 + 2 * mb] for m in metas]
        g1 = [m[5 + 2 * mb:6 + 2 * mb] for m in metas]
        sel, gate = [], []
        for l in range(2):
            e = (2 * me + l).astype(F32)
            for s in range(N_SRC):
                h0 = (r0[s] == e).astype(F32)
                h1 = (r1[s] == e).astype(F32)
                sel.append(h0 + h1)
                gate.append(h0 * g0[s] + h1 * g1[s])
        both = []
        for s in range(N_SRC):
            b = sel[s] + sel[N_SRC + s] > 1.5
            both += [b.astype(F32), jnp.where(b, gate[s], 1.0), jnp.where(b, gate[N_SRC + s], 1.0)]
        sel = jnp.concatenate(sel, axis=0)
        rank = jnp.dot(sel.astype(BF16), before, preferred_element_type=F32)
        pos = jnp.where(sel > 0, rank, -1.0)
        pos_ref[mb] = pos
        cnt_ref[mb] = jnp.broadcast_to(jnp.sum(sel, axis=1, keepdims=True), cnt_ref.shape[1:]).astype(I32)

        def owners(s):
            counts, gates = [], []
            for k in range(N_SRC):
                lo = (2 * jnp.bitwise_xor(me, k)).astype(F32)
                o0 = jnp.logical_or(r0[s] == lo, r0[s] == lo + 1).astype(F32)
                o1 = jnp.logical_or(r1[s] == lo, r1[s] == lo + 1).astype(F32)
                counts.append(o0 + o1)
                gates.append(o0 * g0[s] + o1 * g1[s])
            return counts, gates

        def coefs(mix, gates):
            return [jnp.where(mix, 1.0, 0.0)] + [jnp.where(mix, g, 1.0) for g in gates]

        c, g = owners(0)
        c2, g2 = owners(2)
        rows = [pos] + gate + both
        rows += coefs(jnp.logical_and(c[0] == 1.0, c[1] == 1.0), g[:2])
        rows += coefs(jnp.logical_and(c2[0] == 1.0, c2[1] == 1.0), g2[:2])
        rows += coefs(c[0] + c[1] == 1.0, [g[0] + g[1], g[2] + g[3]])
        rows = jnp.concatenate(rows + [jnp.zeros((128 - COL_TOP - 3, n_tok), F32)], axis=0)
        tab_ref[mb] = rows.T


def route(me, metas):
    n_tok = metas[0].shape[1]
    return pl.pallas_call(
        route_kernel,
        out_shape=[jax.ShapeDtypeStruct((2, 8, n_tok), F32), jax.ShapeDtypeStruct((2, n_tok, 128), F32),
                   jax.ShapeDtypeStruct((2, 8, 128), I32)],
        in_specs=[pl.BlockSpec(memory_space=pltpu.SMEM)] + [pl.BlockSpec(memory_space=pltpu.VMEM)] * 4,
        out_specs=[pl.BlockSpec(memory_space=pltpu.VMEM)] * 3,
        name='route',
    )(me, *metas)


def offset(cnt, l, loc, k):
    off = 0
    for q in range(4 if not isinstance(k, int) else k):
        n = lax.div(cnt[q // 2, l * N_SRC + 2 * loc + q % 2, 0] + 15, 16) * 16
        off = off + (n if isinstance(k, int) else jnp.where(q < k, n, 0))
    return off


def for_rows(m, body):
    lo = 0
    for rows in VARIANTS:
        pl.when(jnp.logical_and(m > lo, m <= rows))(functools.partial(body, rows))
        lo = rows


def up_kernel(loc, ff, cnt, pos, ua0, ua1, ub0, ub1, wg, wu, h, x, w, sem):
    i = pl.program_id(0)
    us = (ua0, ua1, ub0, ub1)
    nc = ff // FC
    n, ns = 2 * nc, w.shape[0]

    def copies(j):
        l, c, s = lax.div(j, nc), lax.rem(j, nc), lax.rem(j, ns)
        cols = pl.ds(pl.multiple_of(c * FC, 128), FC)
        return [pltpu.make_async_copy(wg.at[l, :, cols], w.at[s, :, pl.ds(0, FC)], sem.at[s, 0]),
                pltpu.make_async_copy(wu.at[l, :, cols], w.at[s, :, pl.ds(FC, FC)], sem.at[s, 1])]

    @pl.when(i == 0)
    def _():
        for j in range(ns - 1):
            for c in copies(j):
                c.start()
        x[...] = jnp.zeros_like(x)
        for l in range(2):
            for k in range(4):
                q = l * N_SRC + 2 * loc + k % 2
                p = pos[k // 2, q:q + 1, :]
                pick = (lax.broadcasted_iota(I32, (SLOTS, p.shape[1]), 0).astype(F32) == p).astype(BF16)
                rows = jnp.dot(pick, us[k][...], preferred_element_type=F32)
                x[l, pl.ds(pl.multiple_of(offset(cnt, l, loc, k), 16), SLOTS), :] = rows.astype(BF16)

    @pl.when(i + ns - 1 < n)
    def _():
        for c in copies(i + ns - 1):
            c.start()

    for c in copies(i):
        c.wait()
    l, s = lax.div(i, nc), lax.rem(i, ns)

    def body(rows):
        r = jnp.dot(x[l, :rows], w[s], preferred_element_type=F32)
        h[0, :rows] = (jax.nn.silu(r[:, :FC]) * r[:, FC:]).astype(BF16)

    for_rows(offset(cnt, l, loc, 4), body)


def up(loc, cnt, pos, us, wg, wu):
    d, ff = wg.shape[1:]
    ns = 3
    vmem, hbm = pl.BlockSpec(memory_space=pltpu.VMEM), pl.BlockSpec(memory_space=pl.ANY)
    flops = 4 * d * ff * 2 * HALF
    return pl.pallas_call(
        functools.partial(up_kernel, loc, ff),
        out_shape=jax.ShapeDtypeStruct((2, HALF, ff), BF16),
        grid_spec=pltpu.PrefetchScalarGridSpec(
            num_scalar_prefetch=1, grid=(2 * (ff // FC),), in_specs=[vmem] * 5 + [hbm, hbm],
            out_specs=pl.BlockSpec((1, HALF, FC), lambda i, c: (lax.div(i, ff // FC), 0, lax.rem(i, ff // FC))),
            scratch_shapes=[pltpu.VMEM((2, HALF, d), BF16), pltpu.VMEM((ns, d, 2 * FC), BF16),
                            pltpu.SemaphoreType.DMA((ns, 2))]),
        compiler_params=pltpu.CompilerParams(vmem_limit_bytes=63 * MIB),
        cost_estimate=pl.CostEstimate(flops=flops, bytes_accessed=flops // 512, transcendentals=0),
    )(cnt, pos, *us, wg, wu)


def down_kernel(d0, cnt, tab, *refs):
    us, (h0, h1, wd, keep, send, h, uv, y, w, pick, coef, sem, sem_h, sem_u) = refs[:8], refs[8:]
    i = pl.program_id(0)
    n, ns = pl.num_programs(0), w.shape[0]
    n_tok = tab.shape[1]
    l = lax.rem(i, 2)

    def copy(j):
        s = lax.rem(j, ns)
        cols = pl.ds(pl.multiple_of(d0 + lax.div(j, 2) * DC, 128), DC)
        return pltpu.make_async_copy(wd.at[lax.rem(j, 2), :, cols], w.at[s], sem.at[s])

    def h_copy(e, loc, rows):
        src = (h0, h1)[loc].at[e, pl.ds(0, rows)]
        return pltpu.make_async_copy(src, h.at[loc, e, pl.ds(0, rows)], sem_h.at[loc, e])

    def u_copy(q):
        return pltpu.make_async_copy(us[q].at[:, pl.ds(d0, uv.shape[2])], uv.at[q], sem_u.at[q])

    @pl.when(i == 0)
    def _():
        copy(0).start()
        for e in range(2):
            for loc in range(2):
                for_rows(offset(cnt, e, loc, 4), lambda rows, e=e, loc=loc: h_copy(e, loc, rows).start())
        for j in range(1, ns - 1):
            copy(j).start()
        y[...] = jnp.zeros_like(y)
        lane = lax.broadcasted_iota(I32, (n_tok, SLOTS), 1).astype(F32)
        for mb in range(2):
            t = tab[mb]
            for q in range(2 * N_SRC):
                pick[mb, q] = (t[:, COL_POS + q:COL_POS + q + 1] == lane).astype(BF16)
            for q in range(3 * N_SRC):
                coef[mb, q] = jnp.broadcast_to(t[:, COL_BOTH + q:COL_BOTH + q + 1], (n_tok, 128))

    @pl.when(i + ns - 1 < n)
    def _():
        copy(i + ns - 1).start()

    @pl.when(i == 1)
    def _():
        for q in range(8):
            u_copy(q).start()

    copy(i).wait()
    s = lax.rem(i, ns)
    cols = pl.ds(pl.multiple_of(lax.div(i, 2) * DC, 128), DC)
    for loc in range(2):
        m = offset(cnt, l, loc, 4)

        @pl.when(i < 2)
        def _(loc=loc, m=m):
            for_rows(m, lambda rows: h_copy(l, loc, rows).wait())

        def body(rows, loc=loc):
            y[l, loc, :rows, cols] = jnp.dot(h[loc, l, :rows], w[s], preferred_element_type=F32).astype(BF16)

        for_rows(m, body)

    @pl.when(i == n - 1)
    def _():
        for q in range(8):
            u_copy(q).wait()

        def part(step, carry):
            mb, loc = lax.div(step, 2), lax.rem(step, 2)
            for par, out in enumerate((keep, send)):
                q = 2 * loc + par
                vals = []
                for e in range(2):
                    r0 = pl.multiple_of(offset(cnt, e, loc, 2 * mb + par), 16)
                    vals.append(jnp.dot(pick[mb, e * N_SRC + q], y[e, loc, pl.ds(r0, SLOTS), :],
                                        preferred_element_type=F32))
                a, c0, c1 = [coef[mb, 3 * q + k] for k in range(3)]
                for c in range(uv.shape[2] // 128):
                    cs = slice(c * 128, (c + 1) * 128)
                    mixed = c0 * vals[0][:, cs] + c1 * vals[1][:, cs]
                    out[pl.ds(pl.multiple_of(step * n_tok, 256), n_tok), cs] = (
                        a * uv[mb * N_SRC + q, :, cs].astype(F32) + mixed).astype(BF16)
            return carry

        lax.fori_loop(0, 4, part, 0)


def down(cnt, tab, us, h0, h1, wd, d0, width):
    n_tok, _ = us[0].shape
    ff = wd.shape[1]
    ns = 3
    hbm = pl.BlockSpec(memory_space=pl.ANY)
    flops = 2 * width * ff * 4 * HALF
    out = jax.ShapeDtypeStruct((4 * n_tok, width), BF16)
    out_spec = pl.BlockSpec((4 * n_tok, width), lambda i, c: (0, 0), pipeline_mode=pl.Buffered(1))
    return pl.pallas_call(
        functools.partial(down_kernel, d0), out_shape=[out, out],
        grid_spec=pltpu.PrefetchScalarGridSpec(
            num_scalar_prefetch=1, grid=(2 * (width // DC),),
            in_specs=[pl.BlockSpec(tab.shape, lambda i, c: (0, 0, 0), pipeline_mode=pl.Buffered(1))] + [hbm] * 11,
            out_specs=[out_spec, out_spec],
            scratch_shapes=[pltpu.VMEM((2, 2, HALF, ff), BF16), pltpu.VMEM((8, n_tok, width), BF16),
                            pltpu.VMEM((2, 2, HALF, width), BF16), pltpu.VMEM((ns, ff, DC), BF16),
                            pltpu.VMEM((2, 2 * N_SRC, n_tok, SLOTS), BF16),
                            pltpu.VMEM((2, 3 * N_SRC, n_tok, 128), F32),
                            pltpu.SemaphoreType.DMA((ns,)), pltpu.SemaphoreType.DMA((2, 2)),
                            pltpu.SemaphoreType.DMA((8,))]),
        compiler_params=pltpu.CompilerParams(vmem_limit_bytes=63 * MIB),
        cost_estimate=pl.CostEstimate(flops=flops, bytes_accessed=flops // 512, transcendentals=0),
    )(cnt, tab, *us, h0, h1, wd)


def lincomb(t, col, u, a, b):
    return (t[:, col:col + 1] * u.astype(F32)
            + (t[:, col + 1:col + 2] * a.astype(F32) + t[:, col + 2:col + 3] * b.astype(F32))).astype(BF16)


def there_kernel(tab, u0, u1, k0, k1, g0, g1, out):
    n = u0.shape[0]
    for mb, (u, keep, got) in enumerate(((u0, k0, g0), (u1, k1, g1))):
        out[mb * n:(mb + 1) * n] = lincomb(tab[mb], COL_CNT, u[...], keep[...], got[...])


def top_kernel(tab, u0, u1, k0, k1, g0, g1, b0, b1, *refs):
    for mb, (u, keep, got, back) in enumerate(((u0, k0, g0, b0), (u1, k1, g1, b1))):
        here = lincomb(tab[mb], COL_OWN, u[...], keep[...], got[...])
        refs[mb - 2][...] = lincomb(tab[mb], COL_TOP, u[...], here, back[...])


def mix_args(tab, us, keep, got, d0, row):
    n = us[0].shape[0]
    at = lambda r, c=0: pl.BlockSpec((n, DC), lambda i: (r, c + i))
    specs = [pl.BlockSpec(tab.shape, lambda i: (0, 0, 0)), at(0, d0 // DC), at(0, d0 // DC),
             at(row), at(row + 2), at(row), at(row + 2)]
    return n, at, specs, (tab, *us, keep, keep, got, got)


def there_rows(tab, us, keep, got, d0):
    n, _, specs, args = mix_args(tab, us, keep, got, d0, 1)
    width = keep.shape[1]
    return pl.pallas_call(
        there_kernel, out_shape=jax.ShapeDtypeStruct((2 * n, width), BF16), grid=(width // DC,),
        in_specs=specs, out_specs=pl.BlockSpec((2 * n, DC), lambda i: (0, i)),
        cost_estimate=pl.CostEstimate(flops=10 ** 9, bytes_accessed=10 ** 6, transcendentals=0),
    )(*args)


def top_rows(tab, us, keep, got, back, d0, prev):
    _, at, specs, args = mix_args(tab, us, keep, got, d0, 0)
    specs = specs + [at(0), at(1)] + [pl.BlockSpec(memory_space=pl.ANY)] * len(prev)
    out = jax.ShapeDtypeStruct(us[0].shape, BF16)
    return pl.pallas_call(
        top_kernel, out_shape=[out, out], grid=(keep.shape[1] // DC,), in_specs=specs,
        out_specs=[at(0, d0 // DC)] * 2, input_output_aliases={9: 0, 10: 1} if prev else {},
        cost_estimate=pl.CostEstimate(flops=10 ** 9, bytes_accessed=10 ** 6, transcendentals=0),
    )(*args, back, back, *prev)


def dense_kernel(x, w, *refs):
    refs[-1][...] = jnp.dot(x[...], w[...], preferred_element_type=F32).astype(BF16)


def residual_kernel(x, w, r, out):
    p = jnp.dot(x[...], w[...], preferred_element_type=F32).astype(BF16)
    out[...] = (r[...].astype(F32) + p.astype(F32)).astype(BF16)


def dense_part(x, w, c0, width, prev=(), residual=None):
    n, d = x.shape
    bw = 768
    cols = pl.BlockSpec((n, bw), lambda i: (0, c0 // bw + i))
    extra = list(prev) if residual is None else [residual]
    return pl.pallas_call(
        dense_kernel if residual is None else residual_kernel,
        out_shape=jax.ShapeDtypeStruct((n, w.shape[1]), BF16), grid=(width // bw,),
        in_specs=[pl.BlockSpec((n, d), lambda i: (0, 0)), pl.BlockSpec((d, bw), lambda i: (0, c0 // bw + i))]
        + [pl.BlockSpec(memory_space=pl.ANY) if residual is None else cols] * len(extra),
        out_specs=cols, input_output_aliases={2: 0} if prev else {},
        cost_estimate=pl.CostEstimate(flops=2 * n * d * width, bytes_accessed=2 * d * width, transcendentals=0),
    )(x, w, *extra)


CHUNKS = (1024, 768, 512)


def solution(mesh):
    def layer(x_a, route_a, gate_a, h_b, attn_b, route_b, gate_b, w_qkv, w_o, w_gate, w_up, w_down):
        d = x_a.shape[1]
        me = lax.axis_index('ep').astype(I32).reshape(1)
        meta = jnp.concatenate([route_a.T.astype(F32), route_b.T.astype(F32), gate_a.T, gate_b.T], axis=0)
        metas = [meta] + [swap(meta, k) for k in (1, 2, 3)]
        x_par, x_cnt = swap(x_a, 1), swap(x_a, 2)
        mid_b = dense_part(attn_b, w_o, 0, d, residual=h_b)
        b_par, b_cnt = swap(mid_b, 1), swap(mid_b, 2)
        pos, tab, cnt = route(me, metas)

        h_loc = up(0, cnt, pos, (x_a, x_par, mid_b, b_par), w_gate, w_up)
        x_cnt, b_cnt = after((x_cnt, b_cnt), h_loc)
        x_dia, b_dia = swap(x_cnt, 1), swap(b_cnt, 1)
        qkv = [dense_part(after(h_b, h_loc), w_qkv, 0, d)]
        h_rem = up(1, cnt, pos, (x_cnt, x_dia, b_cnt, b_dia), w_gate, w_up)

        us = (x_a, x_par, x_cnt, x_dia, mid_b, b_par, b_cnt, b_dia)
        own, other = (x_a, mid_b), (x_cnt, b_cnt)
        tag, parts, d0, out = (h_rem, qkv[0]), [], 0, []
        for k, width in enumerate(CHUNKS):
            keep, send = down(after(cnt, tag), tab, us, h_loc, h_rem, w_down, d0, width)
            got = swap(send, 1)
            if k < 2:
                qkv = [dense_part(after(h_b, keep), w_qkv, (k + 1) * d, d, qkv)]
            else:
                out = top_rows(tab, own, *parts[0], [])
            tag = there_rows(tab, other, keep, got, d0)
            parts.append((after(keep, tag), got, swap(tag, 2), d0))
            d0 += width
        for part in parts[1:]:
            out = top_rows(tab, own, *part, out)
        return out[0], out[1], qkv[0]

    row = P(('dp', 'ep'), None)
    full = P(None, None)
    expert = P('ep', None, None)
    return jax.shard_map(
        layer, mesh=mesh,
        in_specs=(row,) * 7 + (full, full, expert, expert, expert),
        out_specs=(row, row, row), check_vma=False)
```

```python
import functools

import jax
import jax.numpy as jnp
from jax import lax
from jax.experimental import pallas as pl
from jax.experimental.pallas import tpu as pltpu
from jax.sharding import PartitionSpec as P


BF16, F32, I32 = jnp.bfloat16, jnp.float32, jnp.int32
N_SRC = 4
SLOTS = 128
HALF = 512
VARIANTS = (256, 384, 512)
FC, DC = 640, 256
MIB = 2 ** 20

COL_POS, COL_BOTH, COL_OWN, COL_CNT, COL_TOP = 0, 16, 28, 31, 34


def swap(x, k):
    return lax.ppermute(x, 'ep', [(i, i ^ k) for i in range(N_SRC)])


def after(x, dep):
    return lax.optimization_barrier((x, dep))[0]


def route_kernel(me_ref, m0, m1, m2, m3, pos_ref, tab_ref, cnt_ref, mid_ref, top_ref):
    me = me_ref[0]
    n_tok = m0.shape[1]
    before = (lax.broadcasted_iota(I32, (n_tok, n_tok), 0)
              < lax.broadcasted_iota(I32, (n_tok, n_tok), 1)).astype(BF16)
    metas = [m[...] for m in (m0, m1, m2, m3)]
    for mb in range(2):
        r0 = [m[2 * mb:2 * mb + 1] for m in metas]
        r1 = [m[2 * mb + 1:2 * mb + 2] for m in metas]
        g0 = [m[4 + 2 * mb:5 + 2 * mb] for m in metas]
        g1 = [m[5 + 2 * mb:6 + 2 * mb] for m in metas]
        sel, gate = [], []
        for l in range(2):
            e = (2 * me + l).astype(F32)
            for s in range(N_SRC):
                h0 = (r0[s] == e).astype(F32)
                h1 = (r1[s] == e).astype(F32)
                sel.append(h0 + h1)
                gate.append(h0 * g0[s] + h1 * g1[s])
        both = []
        for s in range(N_SRC):
            b = sel[s] + sel[N_SRC + s] > 1.5
            both += [b.astype(F32), jnp.where(b, gate[s], 1.0), jnp.where(b, gate[N_SRC + s], 1.0)]
        sel = jnp.concatenate(sel, axis=0)
        rank = jnp.dot(sel.astype(BF16), before, preferred_element_type=F32)
        pos = jnp.where(sel > 0, rank, -1.0)
        pos_ref[mb] = pos
        cnt_ref[mb] = jnp.broadcast_to(jnp.sum(sel, axis=1, keepdims=True), cnt_ref.shape[1:]).astype(I32)

        def owners(s):
            counts, gates = [], []
            for k in range(N_SRC):
                lo = (2 * jnp.bitwise_xor(me, k)).astype(F32)
                o0 = jnp.logical_or(r0[s] == lo, r0[s] == lo + 1).astype(F32)
                o1 = jnp.logical_or(r1[s] == lo, r1[s] == lo + 1).astype(F32)
                counts.append(o0 + o1)
                gates.append(o0 * g0[s] + o1 * g1[s])
            return counts, gates

        def coefs(mix, gates):
            return [jnp.where(mix, 1.0, 0.0)] + [jnp.where(mix, g, 1.0) for g in gates]

        c, g = owners(0)
        c2, g2 = owners(2)
        rows = [pos] + gate + both
        rows += coefs(jnp.logical_and(c[0] == 1.0, c[1] == 1.0), g[:2])
        rows += coefs(jnp.logical_and(c2[0] == 1.0, c2[1] == 1.0), g2[:2])
        rows += coefs(c[0] + c[1] == 1.0, [g[0] + g[1], g[2] + g[3]])
        rows = jnp.concatenate(rows + [jnp.zeros((128 - COL_TOP - 3, n_tok), F32)], axis=0)
        t = rows.T
        tab_ref[mb] = t
        for ref, cols in ((mid_ref, range(COL_CNT, COL_CNT + 3)),
                          (top_ref, [*range(COL_OWN, COL_OWN + 3), *range(COL_TOP, COL_TOP + 3)])):
            for k, c in enumerate(cols):
                ref[len(cols) * mb + k] = jnp.broadcast_to(t[:, c:c + 1], (n_tok, 128))


def route(me, metas):
    n_tok = metas[0].shape[1]
    return pl.pallas_call(
        route_kernel,
        out_shape=[jax.ShapeDtypeStruct((2, 8, n_tok), F32), jax.ShapeDtypeStruct((2, n_tok, 128), F32),
                   jax.ShapeDtypeStruct((2, 8, 128), I32), jax.ShapeDtypeStruct((6, n_tok, 128), F32),
                   jax.ShapeDtypeStruct((12, n_tok, 128), F32)],
        in_specs=[pl.BlockSpec(memory_space=pltpu.SMEM)] + [pl.BlockSpec(memory_space=pltpu.VMEM)] * 4,
        out_specs=[pl.BlockSpec(memory_space=pltpu.VMEM)] * 5,
        name='route',
    )(me, *metas)


def offset(cnt, l, loc, k):
    off = 0
    for q in range(4 if not isinstance(k, int) else k):
        n = lax.div(cnt[q // 2, l * N_SRC + 2 * loc + q % 2, 0] + 15, 16) * 16
        off = off + (n if isinstance(k, int) else jnp.where(q < k, n, 0))
    return off


def for_rows(m, body):
    lo = 0
    for rows in VARIANTS:
        pl.when(jnp.logical_and(m > lo, m <= rows))(functools.partial(body, rows))
        lo = rows


def up_kernel(loc, ff, cnt, pos, ua0, ua1, ub0, ub1, wg, wu, h, x, w, sem):
    i = pl.program_id(0)
    us = (ua0, ua1, ub0, ub1)
    nc = ff // FC
    n, ns = 2 * nc, w.shape[0]

    def copies(j):
        l, c, s = lax.div(j, nc), lax.rem(j, nc), lax.rem(j, ns)
        cols = pl.ds(pl.multiple_of(c * FC, 128), FC)
        return [pltpu.make_async_copy(wg.at[l, :, cols], w.at[s, :, pl.ds(0, FC)], sem.at[s, 0]),
                pltpu.make_async_copy(wu.at[l, :, cols], w.at[s, :, pl.ds(FC, FC)], sem.at[s, 1])]

    @pl.when(i == 0)
    def _():
        for j in range(ns - 1):
            for c in copies(j):
                c.start()
        x[...] = jnp.zeros_like(x)
        for l in range(2):
            for k in range(4):
                q = l * N_SRC + 2 * loc + k % 2
                p = pos[k // 2, q:q + 1, :]
                pick = (lax.broadcasted_iota(I32, (SLOTS, p.shape[1]), 0).astype(F32) == p).astype(BF16)
                rows = jnp.dot(pick, us[k][...], preferred_element_type=F32)
                x[l, pl.ds(pl.multiple_of(offset(cnt, l, loc, k), 16), SLOTS), :] = rows.astype(BF16)

    @pl.when(i + ns - 1 < n)
    def _():
        for c in copies(i + ns - 1):
            c.start()

    for c in copies(i):
        c.wait()
    l, s = lax.div(i, nc), lax.rem(i, ns)

    def body(rows):
        r = jnp.dot(x[l, :rows], w[s], preferred_element_type=F32)
        h[0, :rows] = (jax.nn.silu(r[:, :FC]) * r[:, FC:]).astype(BF16)

    for_rows(offset(cnt, l, loc, 4), body)


def up(loc, cnt, pos, us, wg, wu):
    d, ff = wg.shape[1:]
    ns = 3
    vmem, hbm = pl.BlockSpec(memory_space=pltpu.VMEM), pl.BlockSpec(memory_space=pl.ANY)
    flops = 4 * d * ff * 2 * HALF
    return pl.pallas_call(
        functools.partial(up_kernel, loc, ff),
        out_shape=jax.ShapeDtypeStruct((2, HALF, ff), BF16),
        grid_spec=pltpu.PrefetchScalarGridSpec(
            num_scalar_prefetch=1, grid=(2 * (ff // FC),), in_specs=[vmem] * 5 + [hbm, hbm],
            out_specs=pl.BlockSpec((1, HALF, FC), lambda i, c: (lax.div(i, ff // FC), 0, lax.rem(i, ff // FC))),
            scratch_shapes=[pltpu.VMEM((2, HALF, d), BF16), pltpu.VMEM((ns, d, 2 * FC), BF16),
                            pltpu.SemaphoreType.DMA((ns, 2))]),
        compiler_params=pltpu.CompilerParams(vmem_limit_bytes=63 * MIB),
        cost_estimate=pl.CostEstimate(flops=flops, bytes_accessed=flops // 512, transcendentals=0),
    )(cnt, pos, *us, wg, wu)


def down_kernel(d0, cnt, tab, *refs):
    us, (h0, h1, wd, keep, send, h, uv, y, w, pick, coef, sem, sem_h, sem_u) = refs[:8], refs[8:]
    i = pl.program_id(0)
    n, ns = pl.num_programs(0), w.shape[0]
    n_tok = tab.shape[1]
    l = lax.rem(i, 2)

    def copy(j):
        s = lax.rem(j, ns)
        cols = pl.ds(pl.multiple_of(d0 + lax.div(j, 2) * DC, 128), DC)
        return pltpu.make_async_copy(wd.at[lax.rem(j, 2), :, cols], w.at[s], sem.at[s])

    def h_copy(e, loc, rows):
        src = (h0, h1)[loc].at[e, pl.ds(0, rows)]
        return pltpu.make_async_copy(src, h.at[loc, e, pl.ds(0, rows)], sem_h.at[loc, e])

    def u_copy(q):
        return pltpu.make_async_copy(us[q].at[:, pl.ds(d0, uv.shape[2])], uv.at[q], sem_u.at[q])

    @pl.when(i == 0)
    def _():
        copy(0).start()
        for_rows(offset(cnt, 0, 0, 4), lambda rows: h_copy(0, 0, rows).start())
        y[...] = jnp.zeros_like(y)
        lane = lax.broadcasted_iota(I32, (n_tok, SLOTS), 1).astype(F32)
        for mb in range(2):
            t = tab[mb]
            for q in range(2 * N_SRC):
                pick[mb, q] = (t[:, COL_POS + q:COL_POS + q + 1] == lane).astype(BF16)
            for q in range(3 * N_SRC):
                coef[mb, q] = jnp.broadcast_to(t[:, COL_BOTH + q:COL_BOTH + q + 1], (n_tok, 128))

    @pl.when(jnp.logical_and(i > 1, i + ns - 1 < n))
    def _():
        copy(i + ns - 1).start()

    @pl.when(i == 2)
    def _():
        for q in range(8):
            u_copy(q).start()

    copy(i).wait()
    s = lax.rem(i, ns)
    cols = pl.ds(pl.multiple_of(lax.div(i, 2) * DC, 128), DC)
    for loc in range(2):
        m = offset(cnt, l, loc, 4)

        @pl.when(i < 2)
        def _(loc=loc, m=m):
            for_rows(m, lambda rows: h_copy(l, loc, rows).wait())

        for e, part, then in ((0, 0, (0, 1)), (0, 1, (1, 0)), (1, 0, (1, 1))):
            if part == loc:
                @pl.when(i == e)
                def _(e=e, part=part, then=then):
                    for_rows(offset(cnt, *then, 4), lambda rows: h_copy(*then, rows).start())
                    if part == 1:
                        copy(1).start()
                    if e == 1:
                        for j in range(2, ns + 1):
                            copy(j).start()

        def body(rows, loc=loc):
            y[l, loc, :rows, cols] = jnp.dot(h[loc, l, :rows], w[s], preferred_element_type=F32).astype(BF16)

        for_rows(m, body)

    @pl.when(i == n - 1)
    def _():
        for q in range(8):
            u_copy(q).wait()

        def part(step, carry):
            mb, loc = lax.div(step, 2), lax.rem(step, 2)
            for par, out in enumerate((keep, send)):
                q = 2 * loc + par
                vals = []
                for e in range(2):
                    r0 = pl.multiple_of(offset(cnt, e, loc, 2 * mb + par), 16)
                    vals.append(jnp.dot(pick[mb, e * N_SRC + q], y[e, loc, pl.ds(r0, SLOTS), :],
                                        preferred_element_type=F32))
                a, c0, c1 = [coef[mb, 3 * q + k] for k in range(3)]
                for c in range(uv.shape[2] // 128):
                    cs = slice(c * 128, (c + 1) * 128)
                    mixed = c0 * vals[0][:, cs] + c1 * vals[1][:, cs]
                    out[pl.ds(pl.multiple_of(step * n_tok, 256), n_tok), cs] = (
                        a * uv[mb * N_SRC + q, :, cs].astype(F32) + mixed).astype(BF16)
            return carry

        lax.fori_loop(0, 4, part, 0)


def down(cnt, tab, us, h0, h1, wd, d0, width):
    n_tok, _ = us[0].shape
    ff = wd.shape[1]
    ns = 3
    hbm = pl.BlockSpec(memory_space=pl.ANY)
    flops = 2 * width * ff * 4 * HALF
    out = jax.ShapeDtypeStruct((4 * n_tok, width), BF16)
    out_spec = pl.BlockSpec((4 * n_tok, width), lambda i, c: (0, 0), pipeline_mode=pl.Buffered(1))
    return pl.pallas_call(
        functools.partial(down_kernel, d0), out_shape=[out, out],
        grid_spec=pltpu.PrefetchScalarGridSpec(
            num_scalar_prefetch=1, grid=(2 * (width // DC),),
            in_specs=[pl.BlockSpec(tab.shape, lambda i, c: (0, 0, 0), pipeline_mode=pl.Buffered(1))] + [hbm] * 11,
            out_specs=[out_spec, out_spec],
            scratch_shapes=[pltpu.VMEM((2, 2, HALF, ff), BF16), pltpu.VMEM((8, n_tok, width), BF16),
                            pltpu.VMEM((2, 2, HALF, width), BF16), pltpu.VMEM((ns, ff, DC), BF16),
                            pltpu.VMEM((2, 2 * N_SRC, n_tok, SLOTS), BF16),
                            pltpu.VMEM((2, 3 * N_SRC, n_tok, 128), F32),
                            pltpu.SemaphoreType.DMA((ns,)), pltpu.SemaphoreType.DMA((2, 2)),
                            pltpu.SemaphoreType.DMA((8,))]),
        compiler_params=pltpu.CompilerParams(vmem_limit_bytes=63 * MIB),
        cost_estimate=pl.CostEstimate(flops=flops, bytes_accessed=flops // 512, transcendentals=0),
    )(cnt, tab, *us, h0, h1, wd)


def lincomb(c, k, u, a, b):
    return (c[k] * u.astype(F32) + (c[k + 1] * a.astype(F32) + c[k + 2] * b.astype(F32))).astype(BF16)


def lanes(width):
    return [slice(c * 128, (c + 1) * 128) for c in range(width // 128)]


def there_kernel(coef, u0, u1, k0, k1, g0, g1, out):
    n = u0.shape[0]
    for mb, (u, keep, got) in enumerate(((u0, k0, g0), (u1, k1, g1))):
        for c in lanes(DC):
            out[mb * n:(mb + 1) * n, c] = lincomb(coef, 3 * mb, u[:, c], keep[:, c], got[:, c])


def top_kernel(coef, u0, u1, k0, k1, g0, g1, b0, b1, *refs):
    for mb, (u, keep, got, back) in enumerate(((u0, k0, g0, b0), (u1, k1, g1, b1))):
        for c in lanes(DC):
            here = lincomb(coef, 6 * mb, u[:, c], keep[:, c], got[:, c])
            refs[mb - 2][:, c] = lincomb(coef, 6 * mb + 3, u[:, c], here, back[:, c])


def mix_args(coef, us, keep, got, d0, row):
    n = us[0].shape[0]
    at = lambda r, c=0: pl.BlockSpec((n, DC), lambda i: (r, c + i))
    specs = [pl.BlockSpec(coef.shape, lambda i: (0, 0, 0)), at(0, d0 // DC), at(0, d0 // DC),
             at(row), at(row + 2), at(row), at(row + 2)]
    return n, at, specs, (coef, *us, keep, keep, got, got)


def there_rows(coef, us, keep, got, d0):
    n, _, specs, args = mix_args(coef, us, keep, got, d0, 1)
    width = keep.shape[1]
    return pl.pallas_call(
        there_kernel, out_shape=jax.ShapeDtypeStruct((2 * n, width), BF16), grid=(width // DC,),
        in_specs=specs, out_specs=pl.BlockSpec((2 * n, DC), lambda i: (0, i)),
        cost_estimate=pl.CostEstimate(flops=10 ** 9, bytes_accessed=10 ** 6, transcendentals=0),
    )(*args)


def top_rows(coef, us, keep, got, back, d0, prev):
    _, at, specs, args = mix_args(coef, us, keep, got, d0, 0)
    specs = specs + [at(0), at(1)] + [pl.BlockSpec(memory_space=pl.ANY)] * len(prev)
    out = jax.ShapeDtypeStruct(us[0].shape, BF16)
    return pl.pallas_call(
        top_kernel, out_shape=[out, out], grid=(keep.shape[1] // DC,), in_specs=specs,
        out_specs=[at(0, d0 // DC)] * 2, input_output_aliases={9: 0, 10: 1} if prev else {},
        cost_estimate=pl.CostEstimate(flops=10 ** 9, bytes_accessed=10 ** 6, transcendentals=0),
    )(*args, back, back, *prev)


def dense_kernel(c0, residual, x, w, *refs):
    o, wv, sem = refs[-3:]
    i = pl.program_id(0)
    nb, _, bw = wv.shape
    ahead = 4

    def copy(j):
        return pltpu.make_async_copy(w.at[:, pl.ds(pl.multiple_of(c0 + j * bw, 128), bw)], wv.at[j], sem.at[j])

    @pl.when(i == 0)
    def _():
        for j in range(ahead):
            copy(j).start()

    @pl.when(i + ahead < nb)
    def _():
        copy(i + ahead).start()

    copy(i).wait()
    p = jnp.dot(x[...], wv[i], preferred_element_type=F32).astype(BF16)
    if residual:
        p = (refs[0][...].astype(F32) + p.astype(F32)).astype(BF16)
    o[...] = p


def dense_part(x, w, c0, width, prev=(), residual=None):
    n, d = x.shape
    bw = 256
    cols = pl.BlockSpec((n, bw), lambda i: (0, c0 // bw + i))
    extra = list(prev) if residual is None else [residual]
    return pl.pallas_call(
        functools.partial(dense_kernel, c0, residual is not None),
        out_shape=jax.ShapeDtypeStruct((n, w.shape[1]), BF16), grid=(width // bw,),
        in_specs=[pl.BlockSpec((n, d), lambda i: (0, 0)), pl.BlockSpec(memory_space=pl.ANY)]
        + [pl.BlockSpec(memory_space=pl.ANY) if residual is None else cols] * len(extra),
        out_specs=cols, input_output_aliases={2: 0} if prev else {},
        scratch_shapes=[pltpu.VMEM((width // bw, d, bw), BF16), pltpu.SemaphoreType.DMA((width // bw,))],
        compiler_params=pltpu.CompilerParams(vmem_limit_bytes=60 * MIB),
        cost_estimate=pl.CostEstimate(flops=2 * n * d * width, bytes_accessed=2 * d * width, transcendentals=0),
    )(x, w, *extra)


CHUNKS = (1024, 768, 512)


def solution(mesh):
    def layer(x_a, route_a, gate_a, h_b, attn_b, route_b, gate_b, w_qkv, w_o, w_gate, w_up, w_down):
        d = x_a.shape[1]
        me = lax.axis_index('ep').astype(I32).reshape(1)
        meta = jnp.concatenate([route_a.T.astype(F32), route_b.T.astype(F32), gate_a.T, gate_b.T], axis=0)
        metas = [meta] + [swap(meta, k) for k in (1, 2, 3)]
        x_par, x_cnt = swap(x_a, 1), swap(x_a, 2)
        mid_b = dense_part(attn_b, w_o, 0, d, residual=h_b)
        b_par, b_cnt = swap(mid_b, 1), swap(mid_b, 2)
        pos, tab, cnt, mid, top = route(me, metas)

        h_loc = up(0, cnt, pos, (x_a, x_par, mid_b, b_par), w_gate, w_up)
        x_cnt, b_cnt = after((x_cnt, b_cnt), h_loc)
        x_dia, b_dia = swap(x_cnt, 1), swap(b_cnt, 1)
        qkv = [dense_part(after(h_b, h_loc), w_qkv, 0, d)]
        h_rem = up(1, cnt, pos, (x_cnt, x_dia, b_cnt, b_dia), w_gate, w_up)

        us = (x_a, x_par, x_cnt, x_dia, mid_b, b_par, b_cnt, b_dia)
        own, other = (x_a, mid_b), (x_cnt, b_cnt)
        tag, parts, d0, out = (h_rem, qkv[0]), [], 0, []
        for k, width in enumerate(CHUNKS):
            keep, send = down(after(cnt, tag), tab, us, h_loc, h_rem, w_down, d0, width)
            got = swap(send, 1)
            if k < 2:
                qkv = [dense_part(after(h_b, keep), w_qkv, (k + 1) * d, d, qkv)]
            tag = there_rows(mid, other, keep, got, d0)
            parts.append((after(keep, tag), got, swap(tag, 2), d0))
            d0 += width
        for part in parts:
            out = top_rows(top, own, *part, out)
        return out[0], out[1], qkv[0]

    row = P(('dp', 'ep'), None)
    full = P(None, None)
    expert = P('ep', None, None)
    return jax.shard_map(
        layer, mesh=mesh,
        in_specs=(row,) * 7 + (full, full, expert, expert, expert),
        out_specs=(row, row, row), check_vma=False)
```

```python
import functools

import jax
import jax.numpy as jnp
from jax import lax
from jax.experimental import pallas as pl
from jax.experimental.pallas import tpu as pltpu
from jax.sharding import PartitionSpec as P


BF16, F32, I32 = jnp.bfloat16, jnp.float32, jnp.int32
N_SRC = 4
SLOTS = 128
HALF = 512
VARIANTS = (256, 384, 512)
FC, DC = 640, 768
MIB = 2 ** 20

COL_POS, COL_BOTH, COL_OWN, COL_CNT, COL_TOP = 0, 16, 28, 31, 34


def swap(x, k):
    return lax.ppermute(x, 'ep', [(i, i ^ k) for i in range(N_SRC)])


def after(x, dep):
    return lax.optimization_barrier((x, dep))[0]


def route_kernel(me_ref, m0, m1, m2, m3, pos_ref, tab_ref, cnt_ref, mid_ref, top_ref):
    me = me_ref[0]
    n_tok = m0.shape[1]
    before = (lax.broadcasted_iota(I32, (n_tok, n_tok), 0)
              < lax.broadcasted_iota(I32, (n_tok, n_tok), 1)).astype(BF16)
    metas = [m[...] for m in (m0, m1, m2, m3)]
    for mb in range(2):
        r0 = [m[2 * mb:2 * mb + 1] for m in metas]
        r1 = [m[2 * mb + 1:2 * mb + 2] for m in metas]
        g0 = [m[4 + 2 * mb:5 + 2 * mb] for m in metas]
        g1 = [m[5 + 2 * mb:6 + 2 * mb] for m in metas]
        sel, gate = [], []
        for l in range(2):
            e = (2 * me + l).astype(F32)
            for s in range(N_SRC):
                h0 = (r0[s] == e).astype(F32)
                h1 = (r1[s] == e).astype(F32)
                sel.append(h0 + h1)
                gate.append(h0 * g0[s] + h1 * g1[s])
        both = []
        for s in range(N_SRC):
            b = sel[s] + sel[N_SRC + s] > 1.5
            both += [b.astype(F32), jnp.where(b, gate[s], 1.0), jnp.where(b, gate[N_SRC + s], 1.0)]
        sel = jnp.concatenate(sel, axis=0)
        rank = jnp.dot(sel.astype(BF16), before, preferred_element_type=F32)
        pos = jnp.where(sel > 0, rank, -1.0)
        pos_ref[mb] = pos
        cnt_ref[mb] = jnp.broadcast_to(jnp.sum(sel, axis=1, keepdims=True), cnt_ref.shape[1:]).astype(I32)

        def owners(s):
            counts, gates = [], []
            for k in range(N_SRC):
                lo = (2 * jnp.bitwise_xor(me, k)).astype(F32)
                o0 = jnp.logical_or(r0[s] == lo, r0[s] == lo + 1).astype(F32)
                o1 = jnp.logical_or(r1[s] == lo, r1[s] == lo + 1).astype(F32)
                counts.append(o0 + o1)
                gates.append(o0 * g0[s] + o1 * g1[s])
            return counts, gates

        def coefs(mix, gates):
            return [jnp.where(mix, 1.0, 0.0)] + [jnp.where(mix, g, 1.0) for g in gates]

        c, g = owners(0)
        c2, g2 = owners(2)
        rows = [pos] + gate + both
        rows += coefs(jnp.logical_and(c[0] == 1.0, c[1] == 1.0), g[:2])
        rows += coefs(jnp.logical_and(c2[0] == 1.0, c2[1] == 1.0), g2[:2])
        rows += coefs(c[0] + c[1] == 1.0, [g[0] + g[1], g[2] + g[3]])
        rows = jnp.concatenate(rows + [jnp.zeros((128 - COL_TOP - 3, n_tok), F32)], axis=0)
        t = rows.T
        tab_ref[mb] = t
        for ref, cols in ((mid_ref, range(COL_CNT, COL_CNT + 3)),
                          (top_ref, [*range(COL_OWN, COL_OWN + 3), *range(COL_TOP, COL_TOP + 3)])):
            for k, c in enumerate(cols):
                ref[len(cols) * mb + k] = jnp.broadcast_to(t[:, c:c + 1], (n_tok, 128))


def route(me, metas):
    n_tok = metas[0].shape[1]
    return pl.pallas_call(
        route_kernel,
        out_shape=[jax.ShapeDtypeStruct((2, 8, n_tok), F32), jax.ShapeDtypeStruct((2, n_tok, 128), F32),
                   jax.ShapeDtypeStruct((2, 8, 128), I32), jax.ShapeDtypeStruct((6, n_tok, 128), F32),
                   jax.ShapeDtypeStruct((12, n_tok, 128), F32)],
        in_specs=[pl.BlockSpec(memory_space=pltpu.SMEM)] + [pl.BlockSpec(memory_space=pltpu.VMEM)] * 4,
        out_specs=[pl.BlockSpec(memory_space=pltpu.VMEM)] * 5,
        name='route',
    )(me, *metas)


def offset(cnt, l, loc, k):
    off = 0
    for q in range(4 if not isinstance(k, int) else k):
        n = lax.div(cnt[q // 2, l * N_SRC + 2 * loc + q % 2, 0] + 15, 16) * 16
        off = off + (n if isinstance(k, int) else jnp.where(q < k, n, 0))
    return off


def for_rows(m, body):
    lo = 0
    for rows in VARIANTS:
        pl.when(jnp.logical_and(m > lo, m <= rows))(functools.partial(body, rows))
        lo = rows


def up_step(loc, i, n, nc, cnt, pos, us, wg, wu, x, w, sem, h, whole):
    ns = w.shape[0]

    def copies(j):
        l, c, s = lax.div(j, nc), lax.rem(j, nc), lax.rem(j, ns)
        cols = pl.ds(pl.multiple_of(c * FC, 128), FC)
        return [pltpu.make_async_copy(wg.at[l, :, cols], w.at[s, :, pl.ds(0, FC)], sem.at[s, 0]),
                pltpu.make_async_copy(wu.at[l, :, cols], w.at[s, :, pl.ds(FC, FC)], sem.at[s, 1])]

    @pl.when(i == 0)
    def _():
        for j in range(ns - 1):
            for c in copies(j):
                c.start()
        x[...] = jnp.zeros_like(x)
        for l in range(2):
            for k in range(4):
                q = l * N_SRC + 2 * loc + k % 2
                p = pos[k // 2, q:q + 1, :]
                pick = (lax.broadcasted_iota(I32, (SLOTS, p.shape[1]), 0).astype(F32) == p).astype(BF16)
                rows = jnp.dot(pick, us[k][...], preferred_element_type=F32)
                x[l, pl.ds(pl.multiple_of(offset(cnt, l, loc, k), 16), SLOTS), :] = rows.astype(BF16)

    @pl.when(i + ns - 1 < n)
    def _():
        for c in copies(i + ns - 1):
            c.start()

    @pl.when(i < n)
    def _():
        for c in copies(i):
            c.wait()
        l, s = lax.div(i, nc), lax.rem(i, ns)
        cols = pl.ds(pl.multiple_of(lax.rem(i, nc) * FC, 128), FC)

        def body(rows):
            r = jnp.dot(x[l, :rows], w[s], preferred_element_type=F32)
            res = (jax.nn.silu(r[:, :FC]) * r[:, FC:]).astype(BF16)
            if whole:
                h[l, :rows, cols] = res
            else:
                h[0, :rows] = res

        for_rows(offset(cnt, l, loc, 4), body)


def up_kernel(loc, nc, cnt, pos, ua0, ua1, ub0, ub1, wg, wu, h, x, w, sem):
    up_step(loc, pl.program_id(0), 2 * nc, nc, cnt, pos, (ua0, ua1, ub0, ub1), wg, wu, x, w, sem, h, False)


def up(loc, cnt, pos, us, wg, wu):
    d, ff = wg.shape[1:]
    ns = 3
    vmem, hbm = pl.BlockSpec(memory_space=pltpu.VMEM), pl.BlockSpec(memory_space=pl.ANY)
    flops = 4 * d * ff * 2 * HALF
    return pl.pallas_call(
        functools.partial(up_kernel, loc, ff // FC),
        out_shape=jax.ShapeDtypeStruct((2, HALF, ff), BF16),
        grid_spec=pltpu.PrefetchScalarGridSpec(
            num_scalar_prefetch=1, grid=(2 * (ff // FC),), in_specs=[vmem] * 5 + [hbm, hbm],
            out_specs=pl.BlockSpec((1, HALF, FC), lambda i, c: (lax.div(i, ff // FC), 0, lax.rem(i, ff // FC))),
            scratch_shapes=[pltpu.VMEM((2, HALF, d), BF16), pltpu.VMEM((ns, d, 2 * FC), BF16),
                            pltpu.SemaphoreType.DMA((ns, 2))]),
        compiler_params=pltpu.CompilerParams(vmem_limit_bytes=63 * MIB),
        cost_estimate=pl.CostEstimate(flops=flops, bytes_accessed=flops // 512, transcendentals=0),
    )(cnt, pos, *us, wg, wu)


def ffn_kernel(loc, n1, nc, cnt, tab, *refs):
    it = iter(refs)
    pos = next(it) if n1 else None
    us = [next(it) for _ in range(4)]
    wg, wu = (next(it), next(it)) if n1 else (None, None)
    h_in = None if n1 else next(it)
    wd, keep, send, h, y, w2, pick, coef, s2 = [next(it) for _ in range(9)]
    x, w1, s1 = [next(it) for _ in range(3)] if n1 else (None,) * 3
    sh = None if n1 else next(it)
    i = pl.program_id(0)
    n_tok = tab.shape[1]
    j = i - n1
    n2 = pl.num_programs(0) - n1

    def copy2(j):
        cols = pl.ds(pl.multiple_of(lax.div(j, 2) * DC, 128), DC)
        return pltpu.make_async_copy(wd.at[lax.rem(j, 2), :, cols], w2.at[lax.rem(j, 2)], s2.at[lax.rem(j, 2)])

    def h_copy(e, rows):
        return pltpu.make_async_copy(h_in.at[e, pl.ds(0, rows)], h.at[e, pl.ds(0, rows)], sh.at[e])

    def h_copies(e, act):
        for_rows(offset(cnt, e, loc, 4), lambda rows: act(h_copy(e, rows)))

    if not n1:
        @pl.when(i == 0)
        def _():
            h_copies(0, lambda c: c.start())
            copy2(0).start()

    @pl.when(i == 0)
    def _():
        y[...] = jnp.zeros_like(y)
        lane = lax.broadcasted_iota(I32, (n_tok, SLOTS), 1).astype(F32)
        for mb in range(2):
            t = tab[mb]
            for e in range(2):
                for par in range(2):
                    c = COL_POS + e * N_SRC + 2 * loc + par
                    pick[4 * mb + 2 * e + par] = (t[:, c:c + 1] == lane).astype(BF16)
            for par in range(2):
                for k in range(3):
                    c = COL_BOTH + 3 * (2 * loc + par) + k
                    coef[6 * mb + 3 * par + k] = jnp.broadcast_to(t[:, c:c + 1], (n_tok, 128))

    if n1:
        up_step(loc, i, n1, nc, cnt, pos, us, wg, wu, x, w1, s1, h, True)

        @pl.when(i == n1 - 2)
        def _():
            copy2(0).start()

    @pl.when(j >= 0)
    def _():
        l = lax.rem(j, 2)
        if not n1:
            @pl.when(j == 0)
            def _():
                h_copies(0, lambda c: c.wait())
                h_copies(1, lambda c: c.start())

            @pl.when(j == 1)
            def _():
                h_copies(1, lambda c: c.wait())

        @pl.when(j + 1 < n2)
        def _():
            copy2(j + 1).start()

        copy2(j).wait()

        def body(rows):
            y[l, :rows] = jnp.dot(h[l, :rows], w2[l], preferred_element_type=F32).astype(BF16)

        for_rows(offset(cnt, l, loc, 4), body)

        @pl.when(l == 1)
        def _():
            def part(mb, carry):
                for par, out in enumerate((keep, send)):
                    vals = []
                    for e in range(2):
                        r0 = pl.multiple_of(offset(cnt, e, loc, 2 * mb + par), 16)
                        vals.append(jnp.dot(pick[4 * mb + 2 * e + par], y[e, pl.ds(r0, SLOTS), :],
                                            preferred_element_type=F32))
                    a, c0, c1 = [coef[6 * mb + 3 * par + k] for k in range(3)]
                    u = us[par], us[2 + par]
                    for c in lanes(DC):
                        if n1:
                            cols = pl.ds(pl.multiple_of(lax.div(j, 2) * DC + c.start, 128), 128)
                        else:
                            cols = c
                        uc = jnp.where(mb == 0, u[0][:, cols], u[1][:, cols]).astype(F32)
                        mixed = c0 * vals[0][:, c] + c1 * vals[1][:, c]
                        out[pl.ds(pl.multiple_of(mb * n_tok, 256), n_tok), c] = (a * uc + mixed).astype(BF16)
                return carry

            lax.fori_loop(0, 2, part, 0)


def ffn(loc, cnt, tab, us, wd, *, pos=None, wg=None, wu=None, h_in=None):
    n_tok, d = us[0].shape
    ff = wd.shape[1]
    nc = ff // FC
    n1 = 2 * nc if h_in is None else 0
    ns1 = 2
    once = lambda a: pl.BlockSpec(a.shape, lambda i, c: (0,) * a.ndim, pipeline_mode=pl.Buffered(1))
    hbm = pl.BlockSpec(memory_space=pl.ANY)
    col = lambda i, c: (0, lax.div(jnp.maximum(i - n1, 0), 2))
    scratch = [pltpu.VMEM((2, HALF, ff), BF16), pltpu.VMEM((2, HALF, DC), BF16), pltpu.VMEM((2, ff, DC), BF16),
               pltpu.VMEM((8, n_tok, SLOTS), BF16), pltpu.VMEM((12, n_tok, 128), F32), pltpu.SemaphoreType.DMA((2,))]
    if n1:
        args = [tab, pos, *us, wg, wu, wd]
        specs = [once(tab), once(pos)] + [once(u) for u in us] + [hbm] * 3
        scratch += [pltpu.VMEM((2, HALF, d), BF16), pltpu.VMEM((ns1, d, 2 * FC), BF16), pltpu.SemaphoreType.DMA((ns1, 2))]
    else:
        args = [tab, *us, h_in, wd]
        specs = [once(tab)] + [pl.BlockSpec((n_tok, DC), col)] * 4 + [hbm] * 2
        scratch += [pltpu.SemaphoreType.DMA((2,))]
    out = jax.ShapeDtypeStruct((2 * n_tok, d), BF16)
    out_spec = pl.BlockSpec((2 * n_tok, DC), col)
    flops = (2 if h_in is not None else 6) * d * ff * 2 * HALF
    return pl.pallas_call(
        functools.partial(ffn_kernel, loc, n1, nc), out_shape=[out, out],
        grid_spec=pltpu.PrefetchScalarGridSpec(num_scalar_prefetch=1, grid=(n1 + 2 * (d // DC),), in_specs=specs,
                                               out_specs=[out_spec, out_spec], scratch_shapes=scratch),
        compiler_params=pltpu.CompilerParams(vmem_limit_bytes=67043328),
        cost_estimate=pl.CostEstimate(flops=flops, bytes_accessed=flops // 512, transcendentals=0),
    )(cnt, *args)


def lincomb(c, k, u, a, b):
    return (c[k] * u.astype(F32) + (c[k + 1] * a.astype(F32) + c[k + 2] * b.astype(F32))).astype(BF16)


def lanes(width):
    return [slice(c * 128, (c + 1) * 128) for c in range(width // 128)]


def there_kernel(coef, u0, u1, keep, got, out):
    n = u0.shape[0]
    for mb, u in enumerate((u0, u1)):
        r = slice(mb * n, (mb + 1) * n)
        for c in lanes(u.shape[1]):
            out[r, c] = lincomb(coef, 3 * mb, u[:, c], keep[r, c], got[r, c])


def top_kernel(coef, u0, u1, keep, got, back, *outs):
    n = u0.shape[0]
    for mb, u in enumerate((u0, u1)):
        r = slice(mb * n, (mb + 1) * n)
        for c in lanes(u.shape[1]):
            here = lincomb(coef, 6 * mb, u[:, c], keep[r, c], got[r, c])
            outs[mb][:, c] = lincomb(coef, 6 * mb + 3, u[:, c], here, back[r, c])


def mix(kernel, coef, us, rows, outs):
    n, d = us[0].shape
    bw = 768
    at = lambda r: pl.BlockSpec((r, bw), lambda i: (0, i))
    return pl.pallas_call(
        kernel, out_shape=[jax.ShapeDtypeStruct((r, d), BF16) for r in outs], grid=(d // bw,),
        in_specs=[pl.BlockSpec(coef.shape, lambda i: (0, 0, 0))] + [at(n)] * 2 + [at(2 * n)] * len(rows),
        out_specs=[at(r) for r in outs],
        cost_estimate=pl.CostEstimate(flops=10 ** 9, bytes_accessed=10 ** 6, transcendentals=0),
    )(coef, *us, *rows)


def dense_kernel(x, w, *refs):
    p = jnp.dot(x[...], w[...], preferred_element_type=F32).astype(BF16)
    if len(refs) > 1:
        p = (refs[0][...].astype(F32) + p.astype(F32)).astype(BF16)
    refs[-1][...] = p


def dense(x, w, residual):
    n, d = x.shape
    width, bw = w.shape[1], 768
    cols = pl.BlockSpec((n, bw), lambda i: (0, i))
    return pl.pallas_call(
        dense_kernel, out_shape=jax.ShapeDtypeStruct((n, width), BF16), grid=(width // bw,),
        in_specs=[pl.BlockSpec((n, d), lambda i: (0, 0)),
                  pl.BlockSpec((d, bw), lambda i: (0, i))] + [cols] * len(residual),
        out_specs=cols,
        cost_estimate=pl.CostEstimate(flops=2 * n * d * width, bytes_accessed=2 * d * width, transcendentals=0),
    )(x, w, *residual)


def solution(mesh):
    def layer(x_a, route_a, gate_a, h_b, attn_b, route_b, gate_b, w_qkv, w_o, w_gate, w_up, w_down):
        n = x_a.shape[0]
        me = lax.axis_index('ep').astype(I32).reshape(1)
        meta = jnp.concatenate([route_a.T.astype(F32), route_b.T.astype(F32), gate_a.T, gate_b.T], axis=0)
        metas = [meta] + [swap(meta, k) for k in (1, 2, 3)]
        x_par, x_cnt = swap(x_a, 1), swap(x_a, 2)
        mid_b = dense(attn_b, w_o, [h_b])
        b_par, b_cnt = swap(mid_b, 1), swap(mid_b, 2)
        pos, tab, cnt, mid, top = route(me, metas)

        h_loc = up(0, cnt, pos, (x_a, x_par, mid_b, b_par), w_gate, w_up)
        x_cnt, b_cnt = after((x_cnt, b_cnt), h_loc)
        x_dia, b_dia = swap(x_cnt, 1), swap(b_cnt, 1)
        keep, send = ffn(1, cnt, tab, (x_cnt, x_dia, b_cnt, b_dia), w_down, pos=pos, wg=w_gate, wu=w_up)
        got = swap(send, 1)
        there, = mix(there_kernel, mid, (x_cnt, b_cnt), (keep, got), [2 * n])
        back = swap(there, 2)
        keep, send = ffn(0, after(cnt, there), tab, (x_a, x_par, mid_b, b_par), w_down, h_in=h_loc)
        got = swap(send, 1)
        qkv = dense(after(h_b, keep), w_qkv, [])
        out_a, out_b = mix(top_kernel, top, (x_a, mid_b), (keep, got, back), [n, n])
        return out_a, out_b, qkv

    row = P(('dp', 'ep'), None)
    full = P(None, None)
    expert = P('ep', None, None)
    return jax.shard_map(
        layer, mesh=mesh,
        in_specs=(row,) * 7 + (full, full, expert, expert, expert),
        out_specs=(row, row, row), check_vma=False)
```

```python
import functools

import jax
import jax.numpy as jnp
from jax import lax
from jax.experimental import pallas as pl
from jax.experimental.pallas import tpu as pltpu
from jax.sharding import PartitionSpec as P


BF16, F32, I32 = jnp.bfloat16, jnp.float32, jnp.int32
N_SRC = 4
SLOTS = 128
HALF = 512
VARIANTS = (256, 384, 512)
FC, DC = 640, 768
MIB = 2 ** 20

COL_POS, COL_BOTH, COL_OWN, COL_CNT, COL_TOP = 0, 16, 28, 31, 34


def swap(x, k):
    return lax.ppermute(x, 'ep', [(i, i ^ k) for i in range(N_SRC)])


def after(x, dep):
    return lax.optimization_barrier((x, dep))[0]


def route_kernel(me_ref, m0, m1, m2, m3, pos_ref, tab_ref, cnt_ref):
    me = me_ref[0]
    n_tok = m0.shape[1]
    before = (lax.broadcasted_iota(I32, (n_tok, n_tok), 0)
              < lax.broadcasted_iota(I32, (n_tok, n_tok), 1)).astype(BF16)
    metas = [m[...] for m in (m0, m1, m2, m3)]
    for mb in range(2):
        r0 = [m[2 * mb:2 * mb + 1] for m in metas]
        r1 = [m[2 * mb + 1:2 * mb + 2] for m in metas]
        g0 = [m[4 + 2 * mb:5 + 2 * mb] for m in metas]
        g1 = [m[5 + 2 * mb:6 + 2 * mb] for m in metas]
        sel, gate = [], []
        for l in range(2):
            e = (2 * me + l).astype(F32)
            for s in range(N_SRC):
                h0 = (r0[s] == e).astype(F32)
                h1 = (r1[s] == e).astype(F32)
                sel.append(h0 + h1)
                gate.append(h0 * g0[s] + h1 * g1[s])
        both = []
        for s in range(N_SRC):
            b = sel[s] + sel[N_SRC + s] > 1.5
            both += [b.astype(F32), jnp.where(b, gate[s], 1.0), jnp.where(b, gate[N_SRC + s], 1.0)]
        sel = jnp.concatenate(sel, axis=0)
        rank = jnp.dot(sel.astype(BF16), before, preferred_element_type=F32)
        pos = jnp.where(sel > 0, rank, -1.0)
        pos_ref[mb] = pos
        cnt_ref[mb] = jnp.broadcast_to(jnp.sum(sel, axis=1, keepdims=True), cnt_ref.shape[1:]).astype(I32)

        def owners(s):
            counts, gates = [], []
            for k in range(N_SRC):
                lo = (2 * jnp.bitwise_xor(me, k)).astype(F32)
                o0 = jnp.logical_or(r0[s] == lo, r0[s] == lo + 1).astype(F32)
                o1 = jnp.logical_or(r1[s] == lo, r1[s] == lo + 1).astype(F32)
                counts.append(o0 + o1)
                gates.append(o0 * g0[s] + o1 * g1[s])
            return counts, gates

        def coefs(mix, gates):
            return [jnp.where(mix, 1.0, 0.0)] + [jnp.where(mix, g, 1.0) for g in gates]

        c, g = owners(0)
        c2, g2 = owners(2)
        rows = [pos] + gate + both
        rows += coefs(jnp.logical_and(c[0] == 1.0, c[1] == 1.0), g[:2])
        rows += coefs(jnp.logical_and(c2[0] == 1.0, c2[1] == 1.0), g2[:2])
        rows += coefs(c[0] + c[1] == 1.0, [g[0] + g[1], g[2] + g[3]])
        rows = jnp.concatenate(rows + [jnp.zeros((128 - COL_TOP - 3, n_tok), F32)], axis=0)
        tab_ref[mb] = rows.T


def spread_kernel(tab, mid_ref, top_ref):
    for mb in range(2):
        t = tab[mb]
        for ref, cols in ((mid_ref, range(COL_CNT, COL_CNT + 3)),
                          (top_ref, [*range(COL_OWN, COL_OWN + 3), *range(COL_TOP, COL_TOP + 3)])):
            for k, c in enumerate(cols):
                ref[len(cols) * mb + k] = jnp.broadcast_to(t[:, c:c + 1], (t.shape[0], 128))


def spread(tab):
    n_tok = tab.shape[1]
    return pl.pallas_call(
        spread_kernel,
        out_shape=[jax.ShapeDtypeStruct((k, n_tok, 128), F32) for k in (6, 12)],
        cost_estimate=pl.CostEstimate(flops=10 ** 8, bytes_accessed=10 ** 6, transcendentals=0), name='spread',
    )(tab)


def route(me, metas):
    n_tok = metas[0].shape[1]
    return pl.pallas_call(
        route_kernel,
        out_shape=[jax.ShapeDtypeStruct((2, 8, n_tok), F32), jax.ShapeDtypeStruct((2, n_tok, 128), F32),
                   jax.ShapeDtypeStruct((2, 8, 128), I32)],
        in_specs=[pl.BlockSpec(memory_space=pltpu.SMEM)] + [pl.BlockSpec(memory_space=pltpu.VMEM)] * 4,
        out_specs=[pl.BlockSpec(memory_space=pltpu.VMEM)] * 3,
        name='route',
    )(me, *metas)


def offset(cnt, l, loc, k):
    off = 0
    for q in range(4 if not isinstance(k, int) else k):
        n = lax.div(cnt[q // 2, l * N_SRC + 2 * loc + q % 2, 0] + 15, 16) * 16
        off = off + (n if isinstance(k, int) else jnp.where(q < k, n, 0))
    return off


def for_rows(m, body):
    lo = 0
    for rows in VARIANTS:
        pl.when(jnp.logical_and(m > lo, m <= rows))(functools.partial(body, rows))
        lo = rows


def up_step(loc, i, n, nc, cnt, pos, us, wg, wu, x, w, sem, h, whole):
    ns = w.shape[0]

    def copies(j):
        l, c, s = lax.div(j, nc), lax.rem(j, nc), lax.rem(j, ns)
        cols = pl.ds(pl.multiple_of(c * FC, 128), FC)
        return [pltpu.make_async_copy(wg.at[l, :, cols], w.at[s, :, pl.ds(0, FC)], sem.at[s, 0]),
                pltpu.make_async_copy(wu.at[l, :, cols], w.at[s, :, pl.ds(FC, FC)], sem.at[s, 1])]

    def gather(l):
        x[l] = jnp.zeros(x.shape[1:], BF16)
        for k in range(4):
            q = l * N_SRC + 2 * loc + k % 2
            p = pos[k // 2, q:q + 1, :]
            pick = (lax.broadcasted_iota(I32, (SLOTS, p.shape[1]), 0).astype(F32) == p).astype(BF16)
            rows = jnp.dot(pick, us[k][...], preferred_element_type=F32)
            x[l, pl.ds(pl.multiple_of(offset(cnt, l, loc, k), 16), SLOTS), :] = rows.astype(BF16)

    @pl.when(i == 0)
    def _():
        for j in range(ns - 1):
            for c in copies(j):
                c.start()
        gather(0)

    @pl.when(i == 1)
    def _():
        gather(1)

    @pl.when(i + ns - 1 < n)
    def _():
        for c in copies(i + ns - 1):
            c.start()

    @pl.when(i < n)
    def _():
        for c in copies(i):
            c.wait()
        l, s = lax.div(i, nc), lax.rem(i, ns)
        cols = pl.ds(pl.multiple_of(lax.rem(i, nc) * FC, 128), FC)

        def body(rows):
            r = jnp.dot(x[l, :rows], w[s], preferred_element_type=F32)
            res = (jax.nn.silu(r[:, :FC]) * r[:, FC:]).astype(BF16)
            if whole:
                h[l, :rows, cols] = res
            else:
                h[0, :rows] = res

        for_rows(offset(cnt, l, loc, 4), body)


def up_kernel(loc, nc, cnt, pos, ua0, ua1, ub0, ub1, wg, wu, h, x, w, sem):
    up_step(loc, pl.program_id(0), 2 * nc, nc, cnt, pos, (ua0, ua1, ub0, ub1), wg, wu, x, w, sem, h, False)


def up(loc, cnt, pos, us, wg, wu):
    d, ff = wg.shape[1:]
    ns = 3
    vmem, hbm = pl.BlockSpec(memory_space=pltpu.VMEM), pl.BlockSpec(memory_space=pl.ANY)
    flops = 4 * d * ff * 2 * HALF
    return pl.pallas_call(
        functools.partial(up_kernel, loc, ff // FC),
        out_shape=jax.ShapeDtypeStruct((2, HALF, ff), BF16),
        grid_spec=pltpu.PrefetchScalarGridSpec(
            num_scalar_prefetch=1, grid=(2 * (ff // FC),), in_specs=[vmem] * 5 + [hbm, hbm],
            out_specs=pl.BlockSpec((1, HALF, FC), lambda i, c: (lax.div(i, ff // FC), 0, lax.rem(i, ff // FC))),
            scratch_shapes=[pltpu.VMEM((2, HALF, d), BF16), pltpu.VMEM((ns, d, 2 * FC), BF16),
                            pltpu.SemaphoreType.DMA((ns, 2))]),
        compiler_params=pltpu.CompilerParams(vmem_limit_bytes=63 * MIB),
        cost_estimate=pl.CostEstimate(flops=flops, bytes_accessed=flops // 512, transcendentals=0),
    )(cnt, pos, *us, wg, wu)


def ffn_kernel(loc, n1, nc, cnt, tab, *refs):
    it = iter(refs)
    pos = next(it) if n1 else None
    us = [next(it) for _ in range(4)]
    wg, wu = (next(it), next(it)) if n1 else (None, None)
    h_in = None if n1 else next(it)
    wd, keep, send, h, y, w2, pick, coef, s2 = [next(it) for _ in range(9)]
    x, w1, s1 = [next(it) for _ in range(3)] if n1 else (None,) * 3
    sh = None if n1 else next(it)
    i = pl.program_id(0)
    n_tok = tab.shape[1]
    j = i - n1
    n2 = pl.num_programs(0) - n1

    def copy2(j):
        cols = pl.ds(pl.multiple_of(lax.div(j, 2) * DC, 128), DC)
        return pltpu.make_async_copy(wd.at[lax.rem(j, 2), :, cols], w2.at[lax.rem(j, 2)], s2.at[lax.rem(j, 2)])

    def h_copy(e, rows):
        return pltpu.make_async_copy(h_in.at[e, pl.ds(0, rows)], h.at[e, pl.ds(0, rows)], sh.at[e])

    def h_copies(e, act):
        for_rows(offset(cnt, e, loc, 4), lambda rows: act(h_copy(e, rows)))

    if not n1:
        @pl.when(i == 0)
        def _():
            h_copies(0, lambda c: c.start())
            copy2(0).start()

    @pl.when(i == 0)
    def _():
        y[...] = jnp.zeros_like(y)
        lane = lax.broadcasted_iota(I32, (n_tok, SLOTS), 1).astype(F32)
        for mb in range(2):
            t = tab[mb]
            for e in range(2):
                for par in range(2):
                    c = COL_POS + e * N_SRC + 2 * loc + par
                    pick[4 * mb + 2 * e + par] = (t[:, c:c + 1] == lane).astype(BF16)
            for par in range(2):
                for k in range(3):
                    c = COL_BOTH + 3 * (2 * loc + par) + k
                    coef[6 * mb + 3 * par + k] = jnp.broadcast_to(t[:, c:c + 1], (n_tok, 128))

    if n1:
        up_step(loc, i, n1, nc, cnt, pos, us, wg, wu, x, w1, s1, h, True)

        @pl.when(i == n1 - 2)
        def _():
            copy2(0).start()

    @pl.when(j >= 0)
    def _():
        l = lax.rem(j, 2)
        if not n1:
            @pl.when(j == 0)
            def _():
                h_copies(0, lambda c: c.wait())
                h_copies(1, lambda c: c.start())

            @pl.when(j == 1)
            def _():
                h_copies(1, lambda c: c.wait())

        @pl.when(j + 1 < n2)
        def _():
            copy2(j + 1).start()

        copy2(j).wait()

        def body(rows):
            y[l, :rows] = jnp.dot(h[l, :rows], w2[l], preferred_element_type=F32).astype(BF16)

        for_rows(offset(cnt, l, loc, 4), body)

        @pl.when(l == 1)
        def _():
            def part(mb, carry):
                for par, out in enumerate((keep, send)):
                    vals = []
                    for e in range(2):
                        r0 = pl.multiple_of(offset(cnt, e, loc, 2 * mb + par), 16)
                        vals.append(jnp.dot(pick[4 * mb + 2 * e + par], y[e, pl.ds(r0, SLOTS), :],
                                            preferred_element_type=F32))
                    a, c0, c1 = [coef[6 * mb + 3 * par + k] for k in range(3)]
                    u = us[par], us[2 + par]
                    for c in lanes(DC):
                        if n1:
                            cols = pl.ds(pl.multiple_of(lax.div(j, 2) * DC + c.start, 128), 128)
                        else:
                            cols = c
                        uc = jnp.where(mb == 0, u[0][:, cols], u[1][:, cols]).astype(F32)
                        mixed = c0 * vals[0][:, c] + c1 * vals[1][:, c]
                        out[pl.ds(pl.multiple_of(mb * n_tok, 256), n_tok), c] = (a * uc + mixed).astype(BF16)
                return carry

            lax.fori_loop(0, 2, part, 0)


def ffn(loc, cnt, tab, us, wd, *, pos=None, wg=None, wu=None, h_in=None):
    n_tok, d = us[0].shape
    ff = wd.shape[1]
    nc = ff // FC
    n1 = 2 * nc if h_in is None else 0
    ns1 = 2
    once = lambda a: pl.BlockSpec(a.shape, lambda i, c: (0,) * a.ndim, pipeline_mode=pl.Buffered(1))
    hbm = pl.BlockSpec(memory_space=pl.ANY)
    col = lambda i, c: (0, lax.div(jnp.maximum(i - n1, 0), 2))
    scratch = [pltpu.VMEM((2, HALF, ff), BF16), pltpu.VMEM((2, HALF, DC), BF16), pltpu.VMEM((2, ff, DC), BF16),
               pltpu.VMEM((8, n_tok, SLOTS), BF16), pltpu.VMEM((12, n_tok, 128), F32), pltpu.SemaphoreType.DMA((2,))]
    if n1:
        args = [tab, pos, *us, wg, wu, wd]
        specs = [once(tab), once(pos)] + [once(u) for u in us] + [hbm] * 3
        scratch += [pltpu.VMEM((2, HALF, d), BF16), pltpu.VMEM((ns1, d, 2 * FC), BF16), pltpu.SemaphoreType.DMA((ns1, 2))]
    else:
        args = [tab, *us, h_in, wd]
        specs = [once(tab)] + [pl.BlockSpec((n_tok, DC), col)] * 4 + [hbm] * 2
        scratch += [pltpu.SemaphoreType.DMA((2,))]
    out = jax.ShapeDtypeStruct((2 * n_tok, d), BF16)
    out_spec = pl.BlockSpec((2 * n_tok, DC), col)
    flops = (2 if h_in is not None else 6) * d * ff * 2 * HALF
    return pl.pallas_call(
        functools.partial(ffn_kernel, loc, n1, nc), out_shape=[out, out],
        grid_spec=pltpu.PrefetchScalarGridSpec(num_scalar_prefetch=1, grid=(n1 + 2 * (d // DC),), in_specs=specs,
                                               out_specs=[out_spec, out_spec], scratch_shapes=scratch),
        compiler_params=pltpu.CompilerParams(vmem_limit_bytes=67043328),
        cost_estimate=pl.CostEstimate(flops=flops, bytes_accessed=flops // 512, transcendentals=0),
    )(cnt, *args)


def lincomb(c, k, u, a, b):
    return (c[k] * u.astype(F32) + (c[k + 1] * a.astype(F32) + c[k + 2] * b.astype(F32))).astype(BF16)


def lanes(width):
    return [slice(c * 128, (c + 1) * 128) for c in range(width // 128)]


def there_kernel(coef, u0, u1, keep, got, out):
    n = u0.shape[0]
    for mb, u in enumerate((u0, u1)):
        r = slice(mb * n, (mb + 1) * n)
        for c in lanes(u.shape[1]):
            out[r, c] = lincomb(coef, 3 * mb, u[:, c], keep[r, c], got[r, c])


def top_kernel(coef, u0, u1, keep, got, back, *outs):
    n = u0.shape[0]
    for mb, u in enumerate((u0, u1)):
        r = slice(mb * n, (mb + 1) * n)
        for c in lanes(u.shape[1]):
            here = lincomb(coef, 6 * mb, u[:, c], keep[r, c], got[r, c])
            outs[mb][:, c] = lincomb(coef, 6 * mb + 3, u[:, c], here, back[r, c])


def mix(kernel, coef, us, rows, outs):
    n, d = us[0].shape
    bw = 384
    at = lambda r: pl.BlockSpec((r, bw), lambda i: (0, i))
    return pl.pallas_call(
        kernel, out_shape=[jax.ShapeDtypeStruct((r, d), BF16) for r in outs], grid=(d // bw,),
        in_specs=[pl.BlockSpec(coef.shape, lambda i: (0, 0, 0))] + [at(n)] * 2 + [at(2 * n)] * len(rows),
        out_specs=[at(r) for r in outs],
        compiler_params=pltpu.CompilerParams(vmem_limit_bytes=67043328),
        cost_estimate=pl.CostEstimate(flops=10 ** 9, bytes_accessed=10 ** 6, transcendentals=0),
    )(coef, *us, *rows)


def dense_kernel(x, w, *refs):
    p = jnp.dot(x[...], w[...], preferred_element_type=F32).astype(BF16)
    if len(refs) > 1:
        p = (refs[0][...].astype(F32) + p.astype(F32)).astype(BF16)
    refs[-1][...] = p


def dense(x, w, residual):
    n, d = x.shape
    width, bw = w.shape[1], 768
    cols = pl.BlockSpec((n, bw), lambda i: (0, i))
    return pl.pallas_call(
        dense_kernel, out_shape=jax.ShapeDtypeStruct((n, width), BF16), grid=(width // bw,),
        in_specs=[pl.BlockSpec((n, d), lambda i: (0, 0)),
                  pl.BlockSpec((d, bw), lambda i: (0, i))] + [cols] * len(residual),
        out_specs=cols,
        cost_estimate=pl.CostEstimate(flops=2 * n * d * width, bytes_accessed=2 * d * width, transcendentals=0),
    )(x, w, *residual)


def solution(mesh):
    def layer(x_a, route_a, gate_a, h_b, attn_b, route_b, gate_b, w_qkv, w_o, w_gate, w_up, w_down):
        n = x_a.shape[0]
        me = lax.axis_index('ep').astype(I32).reshape(1)
        meta = jnp.concatenate([route_a.T.astype(F32), route_b.T.astype(F32), gate_a.T, gate_b.T], axis=0)
        metas = [meta] + [swap(meta, k) for k in (1, 2, 3)]
        x_par, x_cnt = swap(x_a, 1), swap(x_a, 2)
        mid_b = dense(attn_b, w_o, [h_b])
        b_par, b_cnt = swap(mid_b, 1), swap(mid_b, 2)
        pos, tab, cnt = route(me, metas)

        h_loc = up(0, cnt, pos, (x_a, x_par, mid_b, b_par), w_gate, w_up)
        x_cnt, b_cnt = after((x_cnt, b_cnt), h_loc)
        x_dia, b_dia = swap(x_cnt, 1), swap(b_cnt, 1)
        mid, top = spread(after(tab, h_loc))
        keep, send = ffn(1, after(cnt, mid), tab, (x_cnt, x_dia, b_cnt, b_dia), w_down, pos=pos, wg=w_gate, wu=w_up)
        got = swap(send, 1)
        there, = mix(there_kernel, mid, (x_cnt, b_cnt), (keep, got), [2 * n])
        back = swap(there, 2)
        keep, send = ffn(0, after(cnt, there), tab, (x_a, x_par, mid_b, b_par), w_down, h_in=h_loc)
        got = swap(send, 1)
        qkv = dense(after(h_b, keep), w_qkv, [])
        out_a, out_b = mix(top_kernel, top, (x_a, mid_b), (keep, got, back), [n, n])
        return out_a, out_b, qkv

    row = P(('dp', 'ep'), None)
    full = P(None, None)
    expert = P('ep', None, None)
    return jax.shard_map(
        layer, mesh=mesh,
        in_specs=(row,) * 7 + (full, full, expert, expert, expert),
        out_specs=(row, row, row), check_vma=False)
```

```python
import functools

import jax
import jax.numpy as jnp
from jax import lax
from jax.experimental import pallas as pl
from jax.experimental.pallas import tpu as pltpu
from jax.sharding import PartitionSpec as P


BF16, F32, I32 = jnp.bfloat16, jnp.float32, jnp.int32
N_SRC = 4
SLOTS = 128
HALF = 512
VARIANTS = (256, 384, 512)
FC, DC = 640, 768
MIB = 2 ** 20

COL_POS, COL_BOTH, COL_OWN, COL_CNT, COL_TOP = 0, 16, 28, 31, 34


def swap(x, k):
    return lax.ppermute(x, 'ep', [(i, i ^ k) for i in range(N_SRC)])


def after(x, dep):
    return lax.optimization_barrier((x, dep))[0]


def route_kernel(me_ref, m0, m1, m2, m3, pos_ref, tab_ref, cnt_ref):
    me = me_ref[0]
    n_tok = m0.shape[1]
    before = (lax.broadcasted_iota(I32, (n_tok, n_tok), 0)
              < lax.broadcasted_iota(I32, (n_tok, n_tok), 1)).astype(BF16)
    metas = [m[...] for m in (m0, m1, m2, m3)]
    for mb in range(2):
        r0 = [m[2 * mb:2 * mb + 1] for m in metas]
        r1 = [m[2 * mb + 1:2 * mb + 2] for m in metas]
        g0 = [m[4 + 2 * mb:5 + 2 * mb] for m in metas]
        g1 = [m[5 + 2 * mb:6 + 2 * mb] for m in metas]
        sel, gate = [], []
        for l in range(2):
            e = (2 * me + l).astype(F32)
            for s in range(N_SRC):
                h0 = (r0[s] == e).astype(F32)
                h1 = (r1[s] == e).astype(F32)
                sel.append(h0 + h1)
                gate.append(h0 * g0[s] + h1 * g1[s])
        both = []
        for s in range(N_SRC):
            b = sel[s] + sel[N_SRC + s] > 1.5
            both += [b.astype(F32), jnp.where(b, gate[s], 1.0), jnp.where(b, gate[N_SRC + s], 1.0)]
        sel = jnp.concatenate(sel, axis=0)
        rank = jnp.dot(sel.astype(BF16), before, preferred_element_type=F32)
        pos = jnp.where(sel > 0, rank, -1.0)
        pos_ref[mb] = pos
        cnt_ref[mb] = jnp.broadcast_to(jnp.sum(sel, axis=1, keepdims=True), cnt_ref.shape[1:]).astype(I32)

        def owners(s):
            counts, gates = [], []
            for k in range(N_SRC):
                lo = (2 * jnp.bitwise_xor(me, k)).astype(F32)
                o0 = jnp.logical_or(r0[s] == lo, r0[s] == lo + 1).astype(F32)
                o1 = jnp.logical_or(r1[s] == lo, r1[s] == lo + 1).astype(F32)
                counts.append(o0 + o1)
                gates.append(o0 * g0[s] + o1 * g1[s])
            return counts, gates

        def coefs(mix, gates):
            return [jnp.where(mix, 1.0, 0.0)] + [jnp.where(mix, g, 1.0) for g in gates]

        c, g = owners(0)
        c2, g2 = owners(2)
        rows = [pos] + gate + both
        rows += coefs(jnp.logical_and(c[0] == 1.0, c[1] == 1.0), g[:2])
        rows += coefs(jnp.logical_and(c2[0] == 1.0, c2[1] == 1.0), g2[:2])
        rows += coefs(c[0] + c[1] == 1.0, [g[0] + g[1], g[2] + g[3]])
        rows = jnp.concatenate(rows + [jnp.zeros((128 - COL_TOP - 3, n_tok), F32)], axis=0)
        tab_ref[mb] = rows.T


def spread_kernel(tab, mid_ref, top_ref):
    for mb in range(2):
        t = tab[mb]
        for ref, cols in ((mid_ref, range(COL_CNT, COL_CNT + 3)),
                          (top_ref, [*range(COL_OWN, COL_OWN + 3), *range(COL_TOP, COL_TOP + 3)])):
            for k, c in enumerate(cols):
                ref[len(cols) * mb + k] = jnp.broadcast_to(t[:, c:c + 1], (t.shape[0], 128))


def spread(tab):
    n_tok = tab.shape[1]
    return pl.pallas_call(
        spread_kernel,
        out_shape=[jax.ShapeDtypeStruct((k, n_tok, 128), F32) for k in (6, 12)],
        cost_estimate=pl.CostEstimate(flops=10 ** 8, bytes_accessed=10 ** 6, transcendentals=0), name='spread',
    )(tab)


def route(me, metas):
    n_tok = metas[0].shape[1]
    return pl.pallas_call(
        route_kernel,
        out_shape=[jax.ShapeDtypeStruct((2, 8, n_tok), F32), jax.ShapeDtypeStruct((2, n_tok, 128), F32),
                   jax.ShapeDtypeStruct((2, 8, 128), I32)],
        in_specs=[pl.BlockSpec(memory_space=pltpu.SMEM)] + [pl.BlockSpec(memory_space=pltpu.VMEM)] * 4,
        out_specs=[pl.BlockSpec(memory_space=pltpu.VMEM)] * 3,
        name='route',
    )(me, *metas)


def offset(cnt, l, loc, k):
    off = 0
    for q in range(4 if not isinstance(k, int) else k):
        n = lax.div(cnt[q // 2, l * N_SRC + 2 * loc + q % 2, 0] + 15, 16) * 16
        off = off + (n if isinstance(k, int) else jnp.where(q < k, n, 0))
    return off


def for_rows(m, body):
    lo = 0
    for rows in VARIANTS:
        pl.when(jnp.logical_and(m > lo, m <= rows))(functools.partial(body, rows))
        lo = rows


def up_step(loc, i, n, nc, cnt, pos, us, wg, wu, x, w, sem, h, whole):
    ns = w.shape[0]

    def copies(j):
        l, c, s = lax.div(j, nc), lax.rem(j, nc), lax.rem(j, ns)
        cols = pl.ds(pl.multiple_of(c * FC, 128), FC)
        return [pltpu.make_async_copy(wg.at[l, :, cols], w.at[s, :, pl.ds(0, FC)], sem.at[s, 0]),
                pltpu.make_async_copy(wu.at[l, :, cols], w.at[s, :, pl.ds(FC, FC)], sem.at[s, 1])]

    def gather(l):
        x[l] = jnp.zeros(x.shape[1:], BF16)
        for k in range(4):
            q = l * N_SRC + 2 * loc + k % 2
            p = pos[k // 2, q:q + 1, :]
            pick = (lax.broadcasted_iota(I32, (SLOTS, p.shape[1]), 0).astype(F32) == p).astype(BF16)
            rows = jnp.dot(pick, us[k][...], preferred_element_type=F32)
            x[l, pl.ds(pl.multiple_of(offset(cnt, l, loc, k), 16), SLOTS), :] = rows.astype(BF16)

    @pl.when(i == 0)
    def _():
        for j in range(ns - 1):
            for c in copies(j):
                c.start()
        gather(0)

    @pl.when(i == 1)
    def _():
        gather(1)

    @pl.when(i + ns - 1 < n)
    def _():
        for c in copies(i + ns - 1):
            c.start()

    @pl.when(i < n)
    def _():
        for c in copies(i):
            c.wait()
        l, s = lax.div(i, nc), lax.rem(i, ns)
        cols = pl.ds(pl.multiple_of(lax.rem(i, nc) * FC, 128), FC)

        def body(rows):
            r = jnp.dot(x[l, :rows], w[s], preferred_element_type=F32)
            res = (jax.nn.silu(r[:, :FC]) * r[:, FC:]).astype(BF16)
            if whole:
                h[l, :rows, cols] = res
            else:
                h[0, :rows] = res

        for_rows(offset(cnt, l, loc, 4), body)


def up_kernel(loc, nc, cnt, pos, ua0, ua1, ub0, ub1, wg, wu, h, x, w, sem):
    up_step(loc, pl.program_id(0), 2 * nc, nc, cnt, pos, (ua0, ua1, ub0, ub1), wg, wu, x, w, sem, h, False)


def up(loc, cnt, pos, us, wg, wu):
    d, ff = wg.shape[1:]
    ns = 3
    vmem, hbm = pl.BlockSpec(memory_space=pltpu.VMEM), pl.BlockSpec(memory_space=pl.ANY)
    flops = 4 * d * ff * 2 * HALF
    return pl.pallas_call(
        functools.partial(up_kernel, loc, ff // FC),
        out_shape=jax.ShapeDtypeStruct((2, HALF, ff), BF16),
        grid_spec=pltpu.PrefetchScalarGridSpec(
            num_scalar_prefetch=1, grid=(2 * (ff // FC),), in_specs=[vmem] * 5 + [hbm, hbm],
            out_specs=pl.BlockSpec((1, HALF, FC), lambda i, c: (lax.div(i, ff // FC), 0, lax.rem(i, ff // FC))),
            scratch_shapes=[pltpu.VMEM((2, HALF, d), BF16), pltpu.VMEM((ns, d, 2 * FC), BF16),
                            pltpu.SemaphoreType.DMA((ns, 2))]),
        compiler_params=pltpu.CompilerParams(vmem_limit_bytes=63 * MIB),
        cost_estimate=pl.CostEstimate(flops=flops, bytes_accessed=flops // 512, transcendentals=0),
    )(cnt, pos, *us, wg, wu)


def ffn_kernel(loc, n0, n1, nc, cnt, tab, *refs):
    it = iter(refs)
    pos = next(it) if n1 else None
    us = [next(it) for _ in range(4)]
    wg, wu = (next(it), next(it)) if n1 else (None, None)
    h_in, xd, wq = (None, None, None) if n1 else [next(it) for _ in range(3)]
    wd, keep, send = next(it), next(it), next(it)
    dense_out = None if n1 else next(it)
    h, y, w2, pick, coef, s2 = [next(it) for _ in range(6)]
    x, w1, s1 = [next(it) for _ in range(3)] if n1 else (None,) * 3
    w0, s0, sh = (None, None, None) if n1 else [next(it) for _ in range(3)]
    i = pl.program_id(0)
    n_tok = tab.shape[1]
    j = i - n1 - n0
    n2 = pl.num_programs(0) - n1 - n0

    def copy2(j):
        cols = pl.ds(pl.multiple_of(lax.div(j, 2) * DC, 128), DC)
        return pltpu.make_async_copy(wd.at[lax.rem(j, 2), :, cols], w2.at[lax.rem(j, 2)], s2.at[lax.rem(j, 2)])

    def h_copy(e, rows):
        return pltpu.make_async_copy(h_in.at[e, pl.ds(0, rows)], h.at[e, pl.ds(0, rows)], sh.at[e])

    def h_copies(e, act):
        for_rows(offset(cnt, e, loc, 4), lambda rows: act(h_copy(e, rows)))

    if not n1:
        def copy0(j):
            cols = pl.ds(pl.multiple_of(j * DC, 128), DC)
            return pltpu.make_async_copy(wq.at[:, cols], w0.at[lax.rem(j, 3)], s0.at[lax.rem(j, 3)])

        @pl.when(i == 0)
        def _():
            copy0(0).start()
            copy0(1).start()

        @pl.when(i + 2 < n0)
        def _():
            copy0(i + 2).start()

        @pl.when(i == 2)
        def _():
            h_copies(0, lambda c: c.start())

        @pl.when(i == 4)
        def _():
            h_copies(1, lambda c: c.start())

        @pl.when(i == 6)
        def _():
            copy2(0).start()

        @pl.when(i < n0)
        def _():
            copy0(i).wait()
            dense_out[...] = jnp.dot(xd[...], w0[lax.rem(i, 3)], preferred_element_type=F32).astype(BF16)

    @pl.when(i == 0)
    def _():
        y[...] = jnp.zeros_like(y)
        lane = lax.broadcasted_iota(I32, (n_tok, SLOTS), 1).astype(F32)
        for mb in range(2):
            t = tab[mb]
            for e in range(2):
                for par in range(2):
                    c = COL_POS + e * N_SRC + 2 * loc + par
                    pick[4 * mb + 2 * e + par] = (t[:, c:c + 1] == lane).astype(BF16)
            for par in range(2):
                for k in range(3):
                    c = COL_BOTH + 3 * (2 * loc + par) + k
                    coef[6 * mb + 3 * par + k] = jnp.broadcast_to(t[:, c:c + 1], (n_tok, 128))

    if n1:
        up_step(loc, i, n1, nc, cnt, pos, us, wg, wu, x, w1, s1, h, True)

        @pl.when(i == n1 - 2)
        def _():
            copy2(0).start()

    @pl.when(j >= 0)
    def _():
        l = lax.rem(j, 2)
        if not n1:
            @pl.when(j < 2)
            def _():
                for_rows(offset(cnt, l, loc, 4), lambda rows: h_copy(l, rows).wait())

        @pl.when(j + 1 < n2)
        def _():
            copy2(j + 1).start()

        copy2(j).wait()

        def body(rows):
            y[l, :rows] = jnp.dot(h[l, :rows], w2[l], preferred_element_type=F32).astype(BF16)

        for_rows(offset(cnt, l, loc, 4), body)

        @pl.when(l == 1)
        def _():
            def part(mb, carry):
                for par, out in enumerate((keep, send)):
                    vals = []
                    for e in range(2):
                        r0 = pl.multiple_of(offset(cnt, e, loc, 2 * mb + par), 16)
                        vals.append(jnp.dot(pick[4 * mb + 2 * e + par], y[e, pl.ds(r0, SLOTS), :],
                                            preferred_element_type=F32))
                    a, c0, c1 = [coef[6 * mb + 3 * par + k] for k in range(3)]
                    u = us[par], us[2 + par]
                    for c in lanes(DC):
                        if n1:
                            cols = pl.ds(pl.multiple_of(lax.div(j, 2) * DC + c.start, 128), 128)
                        else:
                            cols = c
                        uc = jnp.where(mb == 0, u[0][:, cols], u[1][:, cols]).astype(F32)
                        mixed = c0 * vals[0][:, c] + c1 * vals[1][:, c]
                        out[pl.ds(pl.multiple_of(mb * n_tok, 256), n_tok), c] = (a * uc + mixed).astype(BF16)
                return carry

            lax.fori_loop(0, 2, part, 0)


def ffn(loc, cnt, tab, us, wd, *, pos=None, wg=None, wu=None, h_in=None, xd=None, wq=None):
    n_tok, d = us[0].shape
    ff = wd.shape[1]
    nc = ff // FC
    n1 = 2 * nc if h_in is None else 0
    n0 = 0 if n1 else wq.shape[1] // DC
    ns1 = 2
    once = lambda a: pl.BlockSpec(a.shape, lambda i, c: (0,) * a.ndim, pipeline_mode=pl.Buffered(1))
    hbm = pl.BlockSpec(memory_space=pl.ANY)
    col = lambda i, c: (0, lax.div(jnp.maximum(i - n1 - n0, 0), 2))
    scratch = [pltpu.VMEM((2, HALF, ff), BF16), pltpu.VMEM((2, HALF, DC), BF16), pltpu.VMEM((2, ff, DC), BF16),
               pltpu.VMEM((8, n_tok, SLOTS), BF16), pltpu.VMEM((12, n_tok, 128), F32), pltpu.SemaphoreType.DMA((2,))]
    if n1:
        args = [tab, pos, *us, wg, wu, wd]
        specs = [once(tab), once(pos)] + [once(u) for u in us] + [hbm] * 3
        scratch += [pltpu.VMEM((2, HALF, d), BF16), pltpu.VMEM((ns1, d, 2 * FC), BF16), pltpu.SemaphoreType.DMA((ns1, 2))]
    else:
        args = [tab, *us, h_in, xd, wq, wd]
        specs = [once(tab)] + [pl.BlockSpec((n_tok, DC), col)] * 4 + [hbm, once(xd), hbm, hbm]
        scratch += [pltpu.VMEM((3, d, DC), BF16), pltpu.SemaphoreType.DMA((3,)), pltpu.SemaphoreType.DMA((2,))]
    outs = [jax.ShapeDtypeStruct((2 * n_tok, d), BF16)] * 2
    out_specs = [pl.BlockSpec((2 * n_tok, DC), col)] * 2
    if n0:
        outs.append(jax.ShapeDtypeStruct((n_tok, wq.shape[1]), BF16))
        out_specs.append(pl.BlockSpec((n_tok, DC), lambda i, c: (0, jnp.minimum(i, n0 - 1))))
    flops = (3 if h_in is not None else 6) * d * ff * 2 * HALF
    return pl.pallas_call(
        functools.partial(ffn_kernel, loc, n0, n1, nc), out_shape=outs,
        grid_spec=pltpu.PrefetchScalarGridSpec(num_scalar_prefetch=1, grid=(n0 + n1 + 2 * (d // DC),), in_specs=specs,
                                               out_specs=out_specs, scratch_shapes=scratch),
        compiler_params=pltpu.CompilerParams(vmem_limit_bytes=67043328),
        cost_estimate=pl.CostEstimate(flops=flops, bytes_accessed=flops // 512, transcendentals=0),
    )(cnt, *args)


def lincomb(c, k, u, a, b):
    return (c[k] * u.astype(F32) + (c[k + 1] * a.astype(F32) + c[k + 2] * b.astype(F32))).astype(BF16)


def lanes(width):
    return [slice(c * 128, (c + 1) * 128) for c in range(width // 128)]


def there_mix(coef, u, rows, mb, r, c):
    keep, got = rows
    return lincomb(coef, 3 * mb, u[:, c], keep[r, c], got[r, c])


def top_mix(coef, u, rows, mb, r, c):
    keep, got = rows[:2]
    here = lincomb(coef, 6 * mb, u[:, c], keep[r, c], got[r, c])
    return lincomb(coef, 6 * mb + 3, u[:, c], here, rows[2 + mb][:, c])


def mix_kernel(fn, n_in, bw, coef, *refs):
    srcs, outs = refs[:n_in], refs[n_in:n_in + 2]
    dst, res, sem_i, sem_o = refs[n_in + 2:2 * n_in + 2], refs[2 * n_in + 2], refs[-2], refs[-1]
    n, d = srcs[0].shape
    steps = d // bw

    def cut(c, start=0, width=bw):
        return pl.ds(pl.multiple_of(c * bw + start, 128), width)

    def loads(c):
        return [pltpu.make_async_copy(s.at[:, cut(c)], t.at[:, cut(c)], sem_i.at[c, q])
                for q, (s, t) in enumerate(zip(srcs, dst))]

    def saves(c):
        return [pltpu.make_async_copy(res.at[mb, :, cut(c)], outs[mb].at[:, cut(c)], sem_o.at[c, mb]) for mb in range(2)]

    for c in range(steps):
        for copy in loads(c):
            copy.start()

    def step(c, carry):
        for copy in loads(c):
            copy.wait()
        for mb, save in enumerate(saves(c)):
            for lane in lanes(bw):
                cols = cut(c, lane.start, 128)
                res[mb, :, cols] = fn(coef, dst[mb], dst[2:], mb, slice(mb * n, (mb + 1) * n), cols)
            save.start()
        return carry

    lax.fori_loop(0, steps, step, 0)
    for c in range(steps):
        for copy in saves(c):
            copy.wait()


def mix(fn, coef, us, rows):
    n, d = us[0].shape
    bw = 384
    srcs = [*us, *rows]
    hbm = pl.BlockSpec(memory_space=pl.ANY)
    return pl.pallas_call(
        functools.partial(mix_kernel, fn, len(srcs), bw), out_shape=[jax.ShapeDtypeStruct((n, d), BF16)] * 2,
        in_specs=[pl.BlockSpec(memory_space=pltpu.VMEM)] + [hbm] * len(srcs), out_specs=[hbm] * 2,
        scratch_shapes=[pltpu.VMEM(a.shape, BF16) for a in srcs]
        + [pltpu.VMEM((2, n, d), BF16), pltpu.SemaphoreType.DMA((d // bw, len(srcs))), pltpu.SemaphoreType.DMA((d // bw, 2))],
        compiler_params=pltpu.CompilerParams(vmem_limit_bytes=67043328),
        cost_estimate=pl.CostEstimate(flops=10 ** 9, bytes_accessed=10 ** 6, transcendentals=0),
    )(coef, *srcs)


def dense_kernel(x, w, *refs):
    p = jnp.dot(x[...], w[...], preferred_element_type=F32).astype(BF16)
    if len(refs) > 1:
        p = (refs[0][...].astype(F32) + p.astype(F32)).astype(BF16)
    refs[-1][...] = p


def dense(x, w, residual):
    n, d = x.shape
    width, bw = w.shape[1], 768
    cols = pl.BlockSpec((n, bw), lambda i: (0, i))
    return pl.pallas_call(
        dense_kernel, out_shape=jax.ShapeDtypeStruct((n, width), BF16), grid=(width // bw,),
        in_specs=[pl.BlockSpec((n, d), lambda i: (0, 0)),
                  pl.BlockSpec((d, bw), lambda i: (0, i))] + [cols] * len(residual),
        out_specs=cols,
        cost_estimate=pl.CostEstimate(flops=2 * n * d * width, bytes_accessed=2 * d * width, transcendentals=0),
    )(x, w, *residual)


def solution(mesh):
    def layer(x_a, route_a, gate_a, h_b, attn_b, route_b, gate_b, w_qkv, w_o, w_gate, w_up, w_down):
        me = lax.axis_index('ep').astype(I32).reshape(1)
        meta = jnp.concatenate([route_a.T.astype(F32), route_b.T.astype(F32), gate_a.T, gate_b.T], axis=0)
        metas = [meta] + [swap(meta, k) for k in (1, 2, 3)]
        x_par, x_cnt = swap(x_a, 1), swap(x_a, 2)
        mid_b = dense(attn_b, w_o, [h_b])
        b_par, b_cnt = swap(mid_b, 1), swap(mid_b, 2)
        pos, tab, cnt = route(me, metas)

        h_loc = up(0, cnt, pos, (x_a, x_par, mid_b, b_par), w_gate, w_up)
        x_cnt, b_cnt = after((x_cnt, b_cnt), h_loc)
        x_dia, b_dia = swap(x_cnt, 1), swap(b_cnt, 1)
        mid, top = spread(after(tab, h_loc))
        keep, send = ffn(1, after(cnt, mid), tab, (x_cnt, x_dia, b_cnt, b_dia), w_down, pos=pos, wg=w_gate, wu=w_up)
        got = swap(send, 1)
        there = mix(there_mix, mid, (x_cnt, b_cnt), (keep, got))
        back = [swap(t, 2) for t in there]
        keep, send, qkv = ffn(0, after(cnt, there), tab, (x_a, x_par, mid_b, b_par), w_down, h_in=h_loc, xd=h_b, wq=w_qkv)
        got = swap(send, 1)
        out_a, out_b = mix(top_mix, top, (x_a, mid_b), (keep, got, *back))
        return out_a, out_b, qkv

    row = P(('dp', 'ep'), None)
    full = P(None, None)
    expert = P('ep', None, None)
    return jax.shard_map(
        layer, mesh=mesh,
        in_specs=(row,) * 7 + (full, full, expert, expert, expert),
        out_specs=(row, row, row), check_vma=False)
```

```python
import functools

import jax
import jax.numpy as jnp
from jax import lax
from jax.experimental import pallas as pl
from jax.experimental.pallas import tpu as pltpu
from jax.sharding import PartitionSpec as P


BF16, F32, I32 = jnp.bfloat16, jnp.float32, jnp.int32
N_SRC = 4
SLOTS = 128
HALF = 512
UP_ROWS = (320, 384, 448, 512)
DOWN_ROWS = ((384, 512), (384, 448, 512))
FC, DC = 640, 768
MIB = 2 ** 20

COL_POS, COL_BOTH, COL_OWN, COL_CNT, COL_TOP = 0, 16, 28, 31, 34


def swap(x, k):
    return lax.ppermute(x, 'ep', [(i, i ^ k) for i in range(N_SRC)])


def after(x, dep):
    return lax.optimization_barrier((x, dep))[0]


def route_kernel(me_ref, m0, m1, m2, m3, pos_ref, tab_ref, cnt_ref):
    me = me_ref[0]
    n_tok = m0.shape[1]
    before = (lax.broadcasted_iota(I32, (n_tok, n_tok), 0)
              < lax.broadcasted_iota(I32, (n_tok, n_tok), 1)).astype(BF16)
    metas = [m[...] for m in (m0, m1, m2, m3)]
    for mb in range(2):
        r0 = [m[2 * mb:2 * mb + 1] for m in metas]
        r1 = [m[2 * mb + 1:2 * mb + 2] for m in metas]
        g0 = [m[4 + 2 * mb:5 + 2 * mb] for m in metas]
        g1 = [m[5 + 2 * mb:6 + 2 * mb] for m in metas]
        sel, gate = [], []
        for l in range(2):
            e = (2 * me + l).astype(F32)
            for s in range(N_SRC):
                h0 = (r0[s] == e).astype(F32)
                h1 = (r1[s] == e).astype(F32)
                sel.append(h0 + h1)
                gate.append(h0 * g0[s] + h1 * g1[s])
        both = []
        for s in range(N_SRC):
            b = sel[s] + sel[N_SRC + s] > 1.5
            both += [b.astype(F32), jnp.where(b, gate[s], 1.0), jnp.where(b, gate[N_SRC + s], 1.0)]
        sel = jnp.concatenate(sel, axis=0)
        rank = jnp.dot(sel.astype(BF16), before, preferred_element_type=F32)
        pos = jnp.where(sel > 0, rank, -1.0)
        pos_ref[mb] = pos
        cnt_ref[mb] = jnp.broadcast_to(jnp.sum(sel, axis=1, keepdims=True), cnt_ref.shape[1:]).astype(I32)

        def owners(s):
            counts, gates = [], []
            for k in range(N_SRC):
                lo = (2 * jnp.bitwise_xor(me, k)).astype(F32)
                o0 = jnp.logical_or(r0[s] == lo, r0[s] == lo + 1).astype(F32)
                o1 = jnp.logical_or(r1[s] == lo, r1[s] == lo + 1).astype(F32)
                counts.append(o0 + o1)
                gates.append(o0 * g0[s] + o1 * g1[s])
            return counts, gates

        def coefs(mix, gates):
            return [jnp.where(mix, 1.0, 0.0)] + [jnp.where(mix, g, 1.0) for g in gates]

        c, g = owners(0)
        c2, g2 = owners(2)
        rows = [pos] + gate + both
        rows += coefs(jnp.logical_and(c[0] == 1.0, c[1] == 1.0), g[:2])
        rows += coefs(jnp.logical_and(c2[0] == 1.0, c2[1] == 1.0), g2[:2])
        rows += coefs(c[0] + c[1] == 1.0, [g[0] + g[1], g[2] + g[3]])
        rows = jnp.concatenate(rows + [jnp.zeros((128 - COL_TOP - 3, n_tok), F32)], axis=0)
        tab_ref[mb] = rows.T


def spread_kernel(tab, mid_ref, top_ref):
    for mb in range(2):
        t = tab[mb]
        for ref, cols in ((mid_ref, range(COL_CNT, COL_CNT + 3)),
                          (top_ref, [*range(COL_OWN, COL_OWN + 3), *range(COL_TOP, COL_TOP + 3)])):
            for k, c in enumerate(cols):
                ref[len(cols) * mb + k] = jnp.broadcast_to(t[:, c:c + 1], (t.shape[0], 128))


def spread(tab):
    n_tok = tab.shape[1]
    return pl.pallas_call(
        spread_kernel,
        out_shape=[jax.ShapeDtypeStruct((k, n_tok, 128), F32) for k in (6, 12)],
        cost_estimate=pl.CostEstimate(flops=10 ** 8, bytes_accessed=10 ** 6, transcendentals=0), name='spread',
    )(tab)


def route(me, metas):
    n_tok = metas[0].shape[1]
    return pl.pallas_call(
        route_kernel,
        out_shape=[jax.ShapeDtypeStruct((2, 8, n_tok), F32), jax.ShapeDtypeStruct((2, n_tok, 128), F32),
                   jax.ShapeDtypeStruct((2, 8, 128), I32)],
        in_specs=[pl.BlockSpec(memory_space=pltpu.SMEM)] + [pl.BlockSpec(memory_space=pltpu.VMEM)] * 4,
        out_specs=[pl.BlockSpec(memory_space=pltpu.VMEM)] * 3,
        name='route',
    )(me, *metas)


def offset(cnt, l, loc, k):
    off = 0
    for q in range(4 if not isinstance(k, int) else k):
        n = lax.div(cnt[q // 2, l * N_SRC + 2 * loc + q % 2, 0] + 15, 16) * 16
        off = off + (n if isinstance(k, int) else jnp.where(q < k, n, 0))
    return off


def for_rows(variants, m, body):
    lo = 0
    for rows in variants:
        pl.when(jnp.logical_and(m > lo, m <= rows))(functools.partial(body, rows))
        lo = rows


def up_step(loc, i, n, nc, cnt, pos, us, wg, wu, x, w, sem, h, whole):
    ns = w.shape[0]

    def copies(j):
        l, c, s = lax.div(j, nc), lax.rem(j, nc), lax.rem(j, ns)
        cols = pl.ds(pl.multiple_of(c * FC, 128), FC)
        return [pltpu.make_async_copy(wg.at[l, :, cols], w.at[s, :, pl.ds(0, FC)], sem.at[s, 0]),
                pltpu.make_async_copy(wu.at[l, :, cols], w.at[s, :, pl.ds(FC, FC)], sem.at[s, 1])]

    @pl.when(i == 0)
    def _():
        for j in range(ns - 1):
            for c in copies(j):
                c.start()

    @pl.when(i < 2)
    def _():
        x[i] = jnp.zeros(x.shape[1:], BF16)
        for k in range(4):
            p = pos[k // 2, pl.ds(i * N_SRC + 2 * loc + k % 2, 1), :]
            pick = (lax.broadcasted_iota(I32, (SLOTS, p.shape[1]), 0).astype(F32) == p).astype(BF16)
            rows = jnp.dot(pick, us[k][...], preferred_element_type=F32)
            x[i, pl.ds(pl.multiple_of(offset(cnt, i, loc, k), 16), SLOTS), :] = rows.astype(BF16)

    @pl.when(i + ns - 1 < n)
    def _():
        for c in copies(i + ns - 1):
            c.start()

    @pl.when(i < n)
    def _():
        for c in copies(i):
            c.wait()
        l, s = lax.div(i, nc), lax.rem(i, ns)
        cols = pl.ds(pl.multiple_of(lax.rem(i, nc) * FC, 128), FC)

        def body(rows):
            r = jnp.dot(x[l, :rows], w[s], preferred_element_type=F32)
            res = (jax.nn.silu(r[:, :FC]) * r[:, FC:]).astype(BF16)
            rest = jnp.zeros((HALF - rows, FC), BF16)
            if whole:
                h[l, :rows, cols] = res
                if rows < HALF:
                    h[l, rows:, cols] = rest
            else:
                h[0, :rows] = res
                if rows < HALF:
                    h[0, rows:] = rest

        for_rows(UP_ROWS, offset(cnt, l, loc, 4), body)


def up_kernel(loc, nc, cnt, pos, ua0, ua1, ub0, ub1, wg, wu, h, x, w, sem):
    up_step(loc, pl.program_id(0), 2 * nc, nc, cnt, pos, (ua0, ua1, ub0, ub1), wg, wu, x, w, sem, h, False)


def up(loc, cnt, pos, us, wg, wu):
    d, ff = wg.shape[1:]
    ns = 3
    vmem, hbm = pl.BlockSpec(memory_space=pltpu.VMEM), pl.BlockSpec(memory_space=pl.ANY)
    flops = 4 * d * ff * 2 * HALF
    return pl.pallas_call(
        functools.partial(up_kernel, loc, ff // FC),
        out_shape=jax.ShapeDtypeStruct((2, HALF, ff), BF16),
        grid_spec=pltpu.PrefetchScalarGridSpec(
            num_scalar_prefetch=1, grid=(2 * (ff // FC),), in_specs=[vmem] * 5 + [hbm, hbm],
            out_specs=pl.BlockSpec((1, HALF, FC), lambda i, c: (lax.div(i, ff // FC), 0, lax.rem(i, ff // FC))),
            scratch_shapes=[pltpu.VMEM((2, HALF, d), BF16), pltpu.VMEM((ns, d, 2 * FC), BF16),
                            pltpu.SemaphoreType.DMA((ns, 2))]),
        compiler_params=pltpu.CompilerParams(vmem_limit_bytes=63 * MIB),
        cost_estimate=pl.CostEstimate(flops=flops, bytes_accessed=flops // 512, transcendentals=0),
    )(cnt, pos, *us, wg, wu)


def ffn_kernel(loc, n0, n1, nc, cnt, tab, *refs):
    it = iter(refs)
    pos = next(it) if n1 else None
    us = [next(it) for _ in range(4)]
    wg, wu = (next(it), next(it)) if n1 else (None, None)
    h_in, xd, wq = (None, None, None) if n1 else [next(it) for _ in range(3)]
    wd, keep, send = next(it), next(it), next(it)
    dense_out = None if n1 else next(it)
    h, y, w2, pick, coef, s2 = [next(it) for _ in range(6)]
    x, w1, s1 = [next(it) for _ in range(3)] if n1 else (None,) * 3
    w0, s0, sh = (None, None, None) if n1 else [next(it) for _ in range(3)]
    i = pl.program_id(0)
    n_tok = tab.shape[1]
    j = i - n1 - n0
    n2 = pl.num_programs(0) - n1 - n0

    def copy2(j):
        cols = pl.ds(pl.multiple_of(lax.div(j, 2) * DC, 128), DC)
        return pltpu.make_async_copy(wd.at[lax.rem(j, 2), :, cols], w2.at[lax.rem(j, 2)], s2.at[lax.rem(j, 2)])

    def h_copy(e, rows):
        return pltpu.make_async_copy(h_in.at[e, pl.ds(0, rows)], h.at[e, pl.ds(0, rows)], sh.at[e])

    def h_copies(e, act):
        for_rows(DOWN_ROWS[loc], offset(cnt, e, loc, 4), lambda rows: act(h_copy(e, rows)))

    if not n1:
        def copy0(j):
            cols = pl.ds(pl.multiple_of(j * DC, 128), DC)
            return pltpu.make_async_copy(wq.at[:, cols], w0.at[lax.rem(j, 3)], s0.at[lax.rem(j, 3)])

        @pl.when(i == 0)
        def _():
            copy0(0).start()
            copy0(1).start()

        @pl.when(i + 2 < n0)
        def _():
            copy0(i + 2).start()

        @pl.when(i == 2)
        def _():
            h_copies(0, lambda c: c.start())

        @pl.when(i == 4)
        def _():
            h_copies(1, lambda c: c.start())

        @pl.when(i == 6)
        def _():
            copy2(0).start()

        @pl.when(i < n0)
        def _():
            copy0(i).wait()
            dense_out[...] = jnp.dot(xd[...], w0[lax.rem(i, 3)], preferred_element_type=F32).astype(BF16)

    @pl.when(i == 0)
    def _():
        y[...] = jnp.zeros_like(y)
        lane = lax.broadcasted_iota(I32, (n_tok, SLOTS), 1).astype(F32)
        for mb in range(2):
            t = tab[mb]
            for e in range(2):
                for par in range(2):
                    c = COL_POS + e * N_SRC + 2 * loc + par
                    pick[4 * mb + 2 * e + par] = (t[:, c:c + 1] == lane).astype(BF16)
            for par in range(2):
                for k in range(3):
                    c = COL_BOTH + 3 * (2 * loc + par) + k
                    coef[6 * mb + 3 * par + k] = jnp.broadcast_to(t[:, c:c + 1], (n_tok, 128))

    if n1:
        up_step(loc, i, n1, nc, cnt, pos, us, wg, wu, x, w1, s1, h, True)

        @pl.when(i == n1 - 2)
        def _():
            copy2(0).start()

    @pl.when(j >= 0)
    def _():
        l = lax.rem(j, 2)
        if not n1:
            @pl.when(j < 2)
            def _():
                for_rows(DOWN_ROWS[loc], offset(cnt, l, loc, 4), lambda rows: h_copy(l, rows).wait())

        @pl.when(j + 1 < n2)
        def _():
            copy2(j + 1).start()

        copy2(j).wait()

        def body(rows):
            y[l, :rows] = jnp.dot(h[l, :rows], w2[l], preferred_element_type=F32).astype(BF16)

        for_rows(DOWN_ROWS[loc], offset(cnt, l, loc, 4), body)

        @pl.when(l == 1)
        def _():
            def part(mb, carry):
                for par, out in enumerate((keep, send)):
                    vals = []
                    for e in range(2):
                        r0 = pl.multiple_of(offset(cnt, e, loc, 2 * mb + par), 16)
                        vals.append(jnp.dot(pick[4 * mb + 2 * e + par], y[e, pl.ds(r0, SLOTS), :],
                                            preferred_element_type=F32))
                    a, c0, c1 = [coef[6 * mb + 3 * par + k] for k in range(3)]
                    u = us[par], us[2 + par]
                    for c in lanes(DC):
                        if n1:
                            cols = pl.ds(pl.multiple_of(lax.div(j, 2) * DC + c.start, 128), 128)
                        else:
                            cols = c
                        uc = jnp.where(mb == 0, u[0][:, cols], u[1][:, cols]).astype(F32)
                        mixed = c0 * vals[0][:, c] + c1 * vals[1][:, c]
                        out[pl.ds(pl.multiple_of(mb * n_tok, 256), n_tok), c] = (a * uc + mixed).astype(BF16)
                return carry

            lax.fori_loop(0, 2, part, 0)


def ffn(loc, cnt, tab, us, wd, *, pos=None, wg=None, wu=None, h_in=None, xd=None, wq=None):
    n_tok, d = us[0].shape
    ff = wd.shape[1]
    nc = ff // FC
    n1 = 2 * nc if h_in is None else 0
    n0 = 0 if n1 else wq.shape[1] // DC
    ns1 = 2
    once = lambda a: pl.BlockSpec(a.shape, lambda i, c: (0,) * a.ndim, pipeline_mode=pl.Buffered(1))
    hbm = pl.BlockSpec(memory_space=pl.ANY)
    col = lambda i, c: (0, lax.div(jnp.maximum(i - n1 - n0, 0), 2))
    scratch = [pltpu.VMEM((2, HALF, ff), BF16), pltpu.VMEM((2, HALF, DC), BF16), pltpu.VMEM((2, ff, DC), BF16),
               pltpu.VMEM((8, n_tok, SLOTS), BF16), pltpu.VMEM((12, n_tok, 128), F32), pltpu.SemaphoreType.DMA((2,))]
    if n1:
        args = [tab, pos, *us, wg, wu, wd]
        specs = [once(tab), once(pos)] + [once(u) for u in us] + [hbm] * 3
        scratch += [pltpu.VMEM((2, HALF, d), BF16), pltpu.VMEM((ns1, d, 2 * FC), BF16), pltpu.SemaphoreType.DMA((ns1, 2))]
    else:
        args = [tab, *us, h_in, xd, wq, wd]
        specs = [once(tab)] + [pl.BlockSpec((n_tok, DC), col)] * 4 + [hbm, once(xd), hbm, hbm]
        scratch += [pltpu.VMEM((3, d, DC), BF16), pltpu.SemaphoreType.DMA((3,)), pltpu.SemaphoreType.DMA((2,))]
    outs = [jax.ShapeDtypeStruct((2 * n_tok, d), BF16)] * 2
    out_specs = [pl.BlockSpec((2 * n_tok, DC), col)] * 2
    if n0:
        outs.append(jax.ShapeDtypeStruct((n_tok, wq.shape[1]), BF16))
        out_specs.append(pl.BlockSpec((n_tok, DC), lambda i, c: (0, jnp.minimum(i, n0 - 1))))
    flops = (3 if h_in is not None else 6) * d * ff * 2 * HALF
    return pl.pallas_call(
        functools.partial(ffn_kernel, loc, n0, n1, nc), out_shape=outs,
        grid_spec=pltpu.PrefetchScalarGridSpec(num_scalar_prefetch=1, grid=(n0 + n1 + 2 * (d // DC),), in_specs=specs,
                                               out_specs=out_specs, scratch_shapes=scratch),
        compiler_params=pltpu.CompilerParams(vmem_limit_bytes=67043328),
        cost_estimate=pl.CostEstimate(flops=flops, bytes_accessed=flops // 512, transcendentals=0),
    )(cnt, *args)


def lincomb(c, k, u, a, b):
    return (c[k] * u.astype(F32) + (c[k + 1] * a.astype(F32) + c[k + 2] * b.astype(F32))).astype(BF16)


def lanes(width):
    return [slice(c * 128, (c + 1) * 128) for c in range(width // 128)]


def there_mix(coef, u, rows, mb, r, c):
    keep, got = rows
    return lincomb(coef, 3 * mb, u[:, c], keep[r, c], got[r, c])


def top_mix(coef, u, rows, mb, r, c):
    keep, got = rows[:2]
    here = lincomb(coef, 6 * mb, u[:, c], keep[r, c], got[r, c])
    return lincomb(coef, 6 * mb + 3, u[:, c], here, rows[2 + mb][:, c])


def mix_kernel(fn, n_in, bw, coef, *refs):
    srcs, outs = refs[:n_in], refs[n_in:n_in + 2]
    dst, res, sem_i, sem_o = refs[n_in + 2:2 * n_in + 2], refs[2 * n_in + 2], refs[-2], refs[-1]
    n, d = srcs[0].shape
    steps = d // bw

    def cut(c, start=0, width=bw):
        return pl.ds(pl.multiple_of(c * bw + start, 128), width)

    def loads(c):
        return [pltpu.make_async_copy(s.at[:, cut(c)], t.at[:, cut(c)], sem_i.at[c, q])
                for q, (s, t) in enumerate(zip(srcs, dst))]

    def saves(c):
        return [pltpu.make_async_copy(res.at[mb, :, cut(c)], outs[mb].at[:, cut(c)], sem_o.at[c, mb]) for mb in range(2)]

    for c in range(steps):
        for copy in loads(c):
            copy.start()

    def step(c, carry):
        for copy in loads(c):
            copy.wait()
        for mb, save in enumerate(saves(c)):
            for lane in lanes(bw):
                cols = cut(c, lane.start, 128)
                res[mb, :, cols] = fn(coef, dst[mb], dst[2:], mb, slice(mb * n, (mb + 1) * n), cols)
            save.start()
        return carry

    lax.fori_loop(0, steps, step, 0)
    for c in range(steps):
        for copy in saves(c):
            copy.wait()


def mix(fn, coef, us, rows):
    n, d = us[0].shape
    bw = 384
    srcs = [*us, *rows]
    hbm = pl.BlockSpec(memory_space=pl.ANY)
    return pl.pallas_call(
        functools.partial(mix_kernel, fn, len(srcs), bw), out_shape=[jax.ShapeDtypeStruct((n, d), BF16)] * 2,
        in_specs=[pl.BlockSpec(memory_space=pltpu.VMEM)] + [hbm] * len(srcs), out_specs=[hbm] * 2,
        scratch_shapes=[pltpu.VMEM(a.shape, BF16) for a in srcs]
        + [pltpu.VMEM((2, n, d), BF16), pltpu.SemaphoreType.DMA((d // bw, len(srcs))), pltpu.SemaphoreType.DMA((d // bw, 2))],
        compiler_params=pltpu.CompilerParams(vmem_limit_bytes=67043328),
        cost_estimate=pl.CostEstimate(flops=10 ** 9, bytes_accessed=10 ** 6, transcendentals=0),
    )(coef, *srcs)


def dense_kernel(x, w, *refs):
    p = jnp.dot(x[...], w[...], preferred_element_type=F32).astype(BF16)
    if len(refs) > 1:
        p = (refs[0][...].astype(F32) + p.astype(F32)).astype(BF16)
    refs[-1][...] = p


def dense(x, w, residual):
    n, d = x.shape
    width, bw = w.shape[1], 768
    cols = pl.BlockSpec((n, bw), lambda i: (0, i))
    return pl.pallas_call(
        dense_kernel, out_shape=jax.ShapeDtypeStruct((n, width), BF16), grid=(width // bw,),
        in_specs=[pl.BlockSpec((n, d), lambda i: (0, 0)),
                  pl.BlockSpec((d, bw), lambda i: (0, i))] + [cols] * len(residual),
        out_specs=cols,
        cost_estimate=pl.CostEstimate(flops=2 * n * d * width, bytes_accessed=2 * d * width, transcendentals=0),
    )(x, w, *residual)


def solution(mesh):
    def layer(x_a, route_a, gate_a, h_b, attn_b, route_b, gate_b, w_qkv, w_o, w_gate, w_up, w_down):
        me = lax.axis_index('ep').astype(I32).reshape(1)
        meta = jnp.concatenate([route_a.T.astype(F32), route_b.T.astype(F32), gate_a.T, gate_b.T], axis=0)
        metas = [meta] + [swap(meta, k) for k in (1, 2, 3)]
        x_par, x_cnt = swap(x_a, 1), swap(x_a, 2)
        mid_b = dense(attn_b, w_o, [h_b])
        b_par, b_cnt = swap(mid_b, 1), swap(mid_b, 2)
        pos, tab, cnt = route(me, metas)

        h_loc = up(0, cnt, pos, (x_a, x_par, mid_b, b_par), w_gate, w_up)
        x_cnt, b_cnt = after((x_cnt, b_cnt), h_loc)
        x_dia, b_dia = swap(x_cnt, 1), swap(b_cnt, 1)
        mid, top = spread(after(tab, h_loc))
        keep, send = ffn(1, after(cnt, mid), tab, (x_cnt, x_dia, b_cnt, b_dia), w_down, pos=pos, wg=w_gate, wu=w_up)
        got = swap(send, 1)
        there = mix(there_mix, mid, (x_cnt, b_cnt), (keep, got))
        back = [swap(t, 2) for t in there]
        keep, send, qkv = ffn(0, after(cnt, there), tab, (x_a, x_par, mid_b, b_par), w_down, h_in=h_loc, xd=h_b, wq=w_qkv)
        got = swap(send, 1)
        out_a, out_b = mix(top_mix, top, (x_a, mid_b), (keep, got, *back))
        return out_a, out_b, qkv

    row = P(('dp', 'ep'), None)
    full = P(None, None)
    expert = P('ep', None, None)
    return jax.shard_map(
        layer, mesh=mesh,
        in_specs=(row,) * 7 + (full, full, expert, expert, expert),
        out_specs=(row, row, row), check_vma=False)
```

```python
import functools

import jax
import jax.numpy as jnp
from jax import lax
from jax.experimental import pallas as pl
from jax.experimental.pallas import tpu as pltpu
from jax.sharding import PartitionSpec as P


BF16, F32, I32 = jnp.bfloat16, jnp.float32, jnp.int32
N_SRC = 4
SLOTS = 128
HALF = 512
UP_ROWS = (320, 384, 448, 512)
DOWN_ROWS = ((384, 512), (384, 448, 512))
FC, DC = 640, 768
MIB = 2 ** 20

COL_POS, COL_BOTH, COL_OWN, COL_CNT, COL_TOP = 0, 16, 28, 31, 34


def swap(x, k):
    return lax.ppermute(x, 'ep', [(i, i ^ k) for i in range(N_SRC)])


def after(x, dep):
    return lax.optimization_barrier((x, dep))[0]


def route_kernel(me_ref, m0, m1, m2, m3, pos_ref, tab_ref, cnt_ref):
    me = me_ref[0]
    n_tok = m0.shape[1]
    before = (lax.broadcasted_iota(I32, (n_tok, n_tok), 0)
              < lax.broadcasted_iota(I32, (n_tok, n_tok), 1)).astype(BF16)
    metas = [m[...] for m in (m0, m1, m2, m3)]
    for mb in range(2):
        r0 = [m[2 * mb:2 * mb + 1] for m in metas]
        r1 = [m[2 * mb + 1:2 * mb + 2] for m in metas]
        g0 = [m[4 + 2 * mb:5 + 2 * mb] for m in metas]
        g1 = [m[5 + 2 * mb:6 + 2 * mb] for m in metas]
        sel, gate = [], []
        for l in range(2):
            e = (2 * me + l).astype(F32)
            for s in range(N_SRC):
                h0 = (r0[s] == e).astype(F32)
                h1 = (r1[s] == e).astype(F32)
                sel.append(h0 + h1)
                gate.append(h0 * g0[s] + h1 * g1[s])
        both = []
        for s in range(N_SRC):
            b = sel[s] + sel[N_SRC + s] > 1.5
            both += [b.astype(F32), jnp.where(b, gate[s], 1.0), jnp.where(b, gate[N_SRC + s], 1.0)]
        sel = jnp.concatenate(sel, axis=0)
        rank = jnp.dot(sel.astype(BF16), before, preferred_element_type=F32)
        pos = jnp.where(sel > 0, rank, -1.0)
        pos_ref[mb] = pos
        cnt_ref[mb] = jnp.broadcast_to(jnp.sum(sel, axis=1, keepdims=True), cnt_ref.shape[1:]).astype(I32)

        def owners(s):
            counts, gates = [], []
            for k in range(N_SRC):
                lo = (2 * jnp.bitwise_xor(me, k)).astype(F32)
                o0 = jnp.logical_or(r0[s] == lo, r0[s] == lo + 1).astype(F32)
                o1 = jnp.logical_or(r1[s] == lo, r1[s] == lo + 1).astype(F32)
                counts.append(o0 + o1)
                gates.append(o0 * g0[s] + o1 * g1[s])
            return counts, gates

        def coefs(mix, gates):
            return [jnp.where(mix, 1.0, 0.0)] + [jnp.where(mix, g, 1.0) for g in gates]

        c, g = owners(0)
        c2, g2 = owners(2)
        rows = [pos] + gate + both
        rows += coefs(jnp.logical_and(c[0] == 1.0, c[1] == 1.0), g[:2])
        rows += coefs(jnp.logical_and(c2[0] == 1.0, c2[1] == 1.0), g2[:2])
        rows += coefs(c[0] + c[1] == 1.0, [g[0] + g[1], g[2] + g[3]])
        rows = jnp.concatenate(rows + [jnp.zeros((128 - COL_TOP - 3, n_tok), F32)], axis=0)
        tab_ref[mb] = rows.T


def spread_kernel(tab, mid_ref, top_ref):
    for mb in range(2):
        t = tab[mb]
        for ref, cols in ((mid_ref, range(COL_CNT, COL_CNT + 3)),
                          (top_ref, [*range(COL_OWN, COL_OWN + 3), *range(COL_TOP, COL_TOP + 3)])):
            for k, c in enumerate(cols):
                ref[len(cols) * mb + k] = jnp.broadcast_to(t[:, c:c + 1], (t.shape[0], 128))


def spread(tab):
    n_tok = tab.shape[1]
    return pl.pallas_call(
        spread_kernel,
        out_shape=[jax.ShapeDtypeStruct((k, n_tok, 128), F32) for k in (6, 12)],
        cost_estimate=pl.CostEstimate(flops=10 ** 8, bytes_accessed=10 ** 6, transcendentals=0), name='spread',
    )(tab)


def route(me, metas):
    n_tok = metas[0].shape[1]
    return pl.pallas_call(
        route_kernel,
        out_shape=[jax.ShapeDtypeStruct((2, 8, n_tok), F32), jax.ShapeDtypeStruct((2, n_tok, 128), F32),
                   jax.ShapeDtypeStruct((2, 8, 128), I32)],
        in_specs=[pl.BlockSpec(memory_space=pltpu.SMEM)] + [pl.BlockSpec(memory_space=pltpu.VMEM)] * 4,
        out_specs=[pl.BlockSpec(memory_space=pltpu.VMEM)] * 3,
        name='route',
    )(me, *metas)


def offset(cnt, l, loc, k):
    off = 0
    for q in range(4 if not isinstance(k, int) else k):
        n = lax.div(cnt[q // 2, l * N_SRC + 2 * loc + q % 2, 0] + 15, 16) * 16
        off = off + (n if isinstance(k, int) else jnp.where(q < k, n, 0))
    return off


def for_rows(variants, m, body):
    lo = 0
    for rows in variants:
        pl.when(jnp.logical_and(m > lo, m <= rows))(functools.partial(body, rows))
        lo = rows


def up_step(loc, i, n, nc, cnt, pos, us, wg, wu, x, w, sem, u, sem_u, h, whole):
    ns = w.shape[0]

    def copies(j):
        l, c, s = lax.div(j, nc), lax.rem(j, nc), lax.rem(j, ns)
        cols = pl.ds(pl.multiple_of(c * FC, 128), FC)
        return [pltpu.make_async_copy(wg.at[l, :, cols], w.at[s, :, pl.ds(0, FC)], sem.at[s, 0]),
                pltpu.make_async_copy(wu.at[l, :, cols], w.at[s, :, pl.ds(FC, FC)], sem.at[s, 1])]

    @pl.when(i == 0)
    def _():
        tokens = [pltpu.make_async_copy(us[k], u.at[k], sem_u.at[k]) for k in range(4)]
        for c in tokens:
            c.start()
        for j in range(ns - 1):
            for c in copies(j):
                c.start()
        for c in tokens:
            c.wait()

    @pl.when(i < 2)
    def _():
        x[i] = jnp.zeros(x.shape[1:], BF16)
        for k in range(4):
            p = pos[k // 2, pl.ds(i * N_SRC + 2 * loc + k % 2, 1), :]
            pick = (lax.broadcasted_iota(I32, (SLOTS, p.shape[1]), 0).astype(F32) == p).astype(BF16)
            rows = jnp.dot(pick, u[k], preferred_element_type=F32)
            x[i, pl.ds(pl.multiple_of(offset(cnt, i, loc, k), 16), SLOTS), :] = rows.astype(BF16)

    @pl.when(i + ns - 1 < n)
    def _():
        for c in copies(i + ns - 1):
            c.start()

    @pl.when(i < n)
    def _():
        for c in copies(i):
            c.wait()
        l, s = lax.div(i, nc), lax.rem(i, ns)
        cols = pl.ds(pl.multiple_of(lax.rem(i, nc) * FC, 128), FC)

        def body(rows):
            r = jnp.dot(x[l, :rows], w[s], preferred_element_type=F32)
            res = (jax.nn.silu(r[:, :FC]) * r[:, FC:]).astype(BF16)
            rest = jnp.zeros((HALF - rows, FC), BF16)
            if whole:
                h[l, :rows, cols] = res
                if rows < HALF:
                    h[l, rows:, cols] = rest
            else:
                h[0, :rows] = res
                if rows < HALF:
                    h[0, rows:] = rest

        for_rows(UP_ROWS, offset(cnt, l, loc, 4), body)


def up_kernel(loc, nc, cnt, pos, ua0, ua1, ub0, ub1, wg, wu, h, x, w, sem, u, sem_u):
    up_step(loc, pl.program_id(0), 2 * nc, nc, cnt, pos, (ua0, ua1, ub0, ub1), wg, wu, x, w, sem, u, sem_u, h, False)


def up(loc, cnt, pos, us, wg, wu):
    d, ff = wg.shape[1:]
    ns = 3
    vmem, hbm = pl.BlockSpec(memory_space=pltpu.VMEM), pl.BlockSpec(memory_space=pl.ANY)
    flops = 4 * d * ff * 2 * HALF
    return pl.pallas_call(
        functools.partial(up_kernel, loc, ff // FC),
        out_shape=jax.ShapeDtypeStruct((2, HALF, ff), BF16),
        grid_spec=pltpu.PrefetchScalarGridSpec(
            num_scalar_prefetch=1, grid=(2 * (ff // FC),), in_specs=[vmem] + [hbm] * 6,
            out_specs=pl.BlockSpec((1, HALF, FC), lambda i, c: (lax.div(i, ff // FC), 0, lax.rem(i, ff // FC))),
            scratch_shapes=[pltpu.VMEM((2, HALF, d), BF16), pltpu.VMEM((ns, d, 2 * FC), BF16),
                            pltpu.SemaphoreType.DMA((ns, 2)), pltpu.VMEM((4,) + us[0].shape, BF16),
                            pltpu.SemaphoreType.DMA((4,))]),
        compiler_params=pltpu.CompilerParams(vmem_limit_bytes=63 * MIB),
        cost_estimate=pl.CostEstimate(flops=flops, bytes_accessed=flops // 512, transcendentals=0),
    )(cnt, pos, *us, wg, wu)


def ffn_kernel(loc, n0, n1, nc, cnt, tab, *refs):
    it = iter(refs)
    pos = next(it) if n1 else None
    us = [next(it) for _ in range(4)]
    wg, wu = (next(it), next(it)) if n1 else (None, None)
    h_in, xd, wq = (None, None, None) if n1 else [next(it) for _ in range(3)]
    wd, keep, send = next(it), next(it), next(it)
    dense_out = None if n1 else next(it)
    h, y, w2, pick, coef, s2 = [next(it) for _ in range(6)]
    x, w1, s1, uv, su = [next(it) for _ in range(5)] if n1 else (None,) * 5
    w0, s0, sh = (None, None, None) if n1 else [next(it) for _ in range(3)]
    i = pl.program_id(0)
    n_tok = tab.shape[1]
    j = i - n1 - n0
    n2 = pl.num_programs(0) - n1 - n0

    def copy2(j):
        cols = pl.ds(pl.multiple_of(lax.div(j, 2) * DC, 128), DC)
        return pltpu.make_async_copy(wd.at[lax.rem(j, 2), :, cols], w2.at[lax.rem(j, 2)], s2.at[lax.rem(j, 2)])

    def h_copy(e, rows):
        return pltpu.make_async_copy(h_in.at[e, pl.ds(0, rows)], h.at[e, pl.ds(0, rows)], sh.at[e])

    def h_copies(e, act):
        for_rows(DOWN_ROWS[loc], offset(cnt, e, loc, 4), lambda rows: act(h_copy(e, rows)))

    if not n1:
        def copy0(j):
            cols = pl.ds(pl.multiple_of(j * DC, 128), DC)
            return pltpu.make_async_copy(wq.at[:, cols], w0.at[lax.rem(j, 3)], s0.at[lax.rem(j, 3)])

        @pl.when(i == 0)
        def _():
            copy0(0).start()
            copy0(1).start()

        @pl.when(i + 2 < n0)
        def _():
            copy0(i + 2).start()

        @pl.when(i == 2)
        def _():
            h_copies(0, lambda c: c.start())

        @pl.when(i == 4)
        def _():
            h_copies(1, lambda c: c.start())

        @pl.when(i == 6)
        def _():
            copy2(0).start()

        @pl.when(i < n0)
        def _():
            copy0(i).wait()
            dense_out[...] = jnp.dot(xd[...], w0[lax.rem(i, 3)], preferred_element_type=F32).astype(BF16)

    @pl.when(i == 0)
    def _():
        y[...] = jnp.zeros_like(y)
        lane = lax.broadcasted_iota(I32, (n_tok, SLOTS), 1).astype(F32)
        for mb in range(2):
            t = tab[mb]
            for e in range(2):
                for par in range(2):
                    c = COL_POS + e * N_SRC + 2 * loc + par
                    pick[4 * mb + 2 * e + par] = (t[:, c:c + 1] == lane).astype(BF16)
            for par in range(2):
                for k in range(3):
                    c = COL_BOTH + 3 * (2 * loc + par) + k
                    coef[6 * mb + 3 * par + k] = jnp.broadcast_to(t[:, c:c + 1], (n_tok, 128))

    if n1:
        up_step(loc, i, n1, nc, cnt, pos, us, wg, wu, x, w1, s1, uv, su, h, True)

        @pl.when(i == n1 - 2)
        def _():
            copy2(0).start()

    @pl.when(j >= 0)
    def _():
        l = lax.rem(j, 2)
        if not n1:
            @pl.when(j < 2)
            def _():
                for_rows(DOWN_ROWS[loc], offset(cnt, l, loc, 4), lambda rows: h_copy(l, rows).wait())

        @pl.when(j + 1 < n2)
        def _():
            copy2(j + 1).start()

        copy2(j).wait()

        def body(rows):
            y[l, :rows] = jnp.dot(h[l, :rows], w2[l], preferred_element_type=F32).astype(BF16)

        for_rows(DOWN_ROWS[loc], offset(cnt, l, loc, 4), body)

        @pl.when(l == 1)
        def _():
            def part(mb, carry):
                for par, out in enumerate((keep, send)):
                    vals = []
                    for e in range(2):
                        r0 = pl.multiple_of(offset(cnt, e, loc, 2 * mb + par), 16)
                        vals.append(jnp.dot(pick[4 * mb + 2 * e + par], y[e, pl.ds(r0, SLOTS), :],
                                            preferred_element_type=F32))
                    a, c0, c1 = [coef[6 * mb + 3 * par + k] for k in range(3)]
                    u = [uv.at[q] if n1 else us[q] for q in (par, 2 + par)]
                    for c in lanes(DC):
                        if n1:
                            cols = pl.ds(pl.multiple_of(lax.div(j, 2) * DC + c.start, 128), 128)
                        else:
                            cols = c
                        uc = jnp.where(mb == 0, u[0][:, cols], u[1][:, cols]).astype(F32)
                        mixed = c0 * vals[0][:, c] + c1 * vals[1][:, c]
                        out[pl.ds(pl.multiple_of(mb * n_tok, 256), n_tok), c] = (a * uc + mixed).astype(BF16)
                return carry

            lax.fori_loop(0, 2, part, 0)


def ffn(loc, cnt, tab, us, wd, *, pos=None, wg=None, wu=None, h_in=None, xd=None, wq=None):
    n_tok, d = us[0].shape
    ff = wd.shape[1]
    nc = ff // FC
    n1 = 2 * nc if h_in is None else 0
    n0 = 0 if n1 else wq.shape[1] // DC
    ns1 = 2
    once = lambda a: pl.BlockSpec(a.shape, lambda i, c: (0,) * a.ndim, pipeline_mode=pl.Buffered(1))
    hbm = pl.BlockSpec(memory_space=pl.ANY)
    col = lambda i, c: (0, lax.div(jnp.maximum(i - n1 - n0, 0), 2))
    scratch = [pltpu.VMEM((2, HALF, ff), BF16), pltpu.VMEM((2, HALF, DC), BF16), pltpu.VMEM((2, ff, DC), BF16),
               pltpu.VMEM((8, n_tok, SLOTS), BF16), pltpu.VMEM((12, n_tok, 128), F32), pltpu.SemaphoreType.DMA((2,))]
    if n1:
        args = [tab, pos, *us, wg, wu, wd]
        specs = [once(tab), once(pos)] + [hbm] * 7
        scratch += [pltpu.VMEM((2, HALF, d), BF16), pltpu.VMEM((ns1, d, 2 * FC), BF16), pltpu.SemaphoreType.DMA((ns1, 2)),
                    pltpu.VMEM((4,) + us[0].shape, BF16), pltpu.SemaphoreType.DMA((4,))]
    else:
        args = [tab, *us, h_in, xd, wq, wd]
        specs = [once(tab)] + [pl.BlockSpec((n_tok, DC), col)] * 4 + [hbm, once(xd), hbm, hbm]
        scratch += [pltpu.VMEM((3, d, DC), BF16), pltpu.SemaphoreType.DMA((3,)), pltpu.SemaphoreType.DMA((2,))]
    outs = [jax.ShapeDtypeStruct((2 * n_tok, d), BF16)] * 2
    out_specs = [pl.BlockSpec((2 * n_tok, DC), col)] * 2
    if n0:
        outs.append(jax.ShapeDtypeStruct((n_tok, wq.shape[1]), BF16))
        out_specs.append(pl.BlockSpec((n_tok, DC), lambda i, c: (0, jnp.minimum(i, n0 - 1))))
    flops = (3 if h_in is not None else 6) * d * ff * 2 * HALF
    return pl.pallas_call(
        functools.partial(ffn_kernel, loc, n0, n1, nc), out_shape=outs,
        grid_spec=pltpu.PrefetchScalarGridSpec(num_scalar_prefetch=1, grid=(n0 + n1 + 2 * (d // DC),), in_specs=specs,
                                               out_specs=out_specs, scratch_shapes=scratch),
        compiler_params=pltpu.CompilerParams(vmem_limit_bytes=67043328),
        cost_estimate=pl.CostEstimate(flops=flops, bytes_accessed=flops // 512, transcendentals=0),
    )(cnt, *args)


def lincomb(c, k, u, a, b):
    return (c[k] * u.astype(F32) + (c[k + 1] * a.astype(F32) + c[k + 2] * b.astype(F32))).astype(BF16)


def lanes(width):
    return [slice(c * 128, (c + 1) * 128) for c in range(width // 128)]


def there_mix(coef, u, rows, mb, r, c):
    keep, got = rows
    return lincomb(coef, 3 * mb, u[:, c], keep[r, c], got[r, c])


def top_mix(coef, u, rows, mb, r, c):
    keep, got = rows[:2]
    here = lincomb(coef, 6 * mb, u[:, c], keep[r, c], got[r, c])
    return lincomb(coef, 6 * mb + 3, u[:, c], here, rows[2 + mb][:, c])


def mix_kernel(fn, n_in, bw, coef, *refs):
    srcs, outs = refs[:n_in], refs[n_in:n_in + 2]
    dst, res, sem_i, sem_o = refs[n_in + 2:2 * n_in + 2], refs[2 * n_in + 2], refs[-2], refs[-1]
    n, d = srcs[0].shape
    steps = d // bw

    def cut(c, start=0, width=bw):
        return pl.ds(pl.multiple_of(c * bw + start, 128), width)

    def loads(c):
        return [pltpu.make_async_copy(s.at[:, cut(c)], t.at[:, cut(c)], sem_i.at[c, q])
                for q, (s, t) in enumerate(zip(srcs, dst))]

    def saves(c):
        return [pltpu.make_async_copy(res.at[mb, :, cut(c)], outs[mb].at[:, cut(c)], sem_o.at[c, mb]) for mb in range(2)]

    for c in range(steps):
        for copy in loads(c):
            copy.start()

    def step(c, carry):
        for copy in loads(c):
            copy.wait()
        for mb, save in enumerate(saves(c)):
            for lane in lanes(bw):
                cols = cut(c, lane.start, 128)
                res[mb, :, cols] = fn(coef, dst[mb], dst[2:], mb, slice(mb * n, (mb + 1) * n), cols)
            save.start()
        return carry

    lax.fori_loop(0, steps, step, 0)
    for c in range(steps):
        for copy in saves(c):
            copy.wait()


def mix(fn, coef, us, rows):
    n, d = us[0].shape
    bw = 384
    srcs = [*us, *rows]
    hbm = pl.BlockSpec(memory_space=pl.ANY)
    return pl.pallas_call(
        functools.partial(mix_kernel, fn, len(srcs), bw), out_shape=[jax.ShapeDtypeStruct((n, d), BF16)] * 2,
        in_specs=[pl.BlockSpec(memory_space=pltpu.VMEM)] + [hbm] * len(srcs), out_specs=[hbm] * 2,
        scratch_shapes=[pltpu.VMEM(a.shape, BF16) for a in srcs]
        + [pltpu.VMEM((2, n, d), BF16), pltpu.SemaphoreType.DMA((d // bw, len(srcs))), pltpu.SemaphoreType.DMA((d // bw, 2))],
        compiler_params=pltpu.CompilerParams(vmem_limit_bytes=67043328),
        cost_estimate=pl.CostEstimate(flops=10 ** 9, bytes_accessed=10 ** 6, transcendentals=0),
    )(coef, *srcs)


def dense_kernel(x, w, *refs):
    p = jnp.dot(x[...], w[...], preferred_element_type=F32).astype(BF16)
    if len(refs) > 1:
        p = (refs[0][...].astype(F32) + p.astype(F32)).astype(BF16)
    refs[-1][...] = p


def dense(x, w, residual):
    n, d = x.shape
    width, bw = w.shape[1], 768
    cols = pl.BlockSpec((n, bw), lambda i: (0, i))
    return pl.pallas_call(
        dense_kernel, out_shape=jax.ShapeDtypeStruct((n, width), BF16), grid=(width // bw,),
        in_specs=[pl.BlockSpec((n, d), lambda i: (0, 0)),
                  pl.BlockSpec((d, bw), lambda i: (0, i))] + [cols] * len(residual),
        out_specs=cols,
        cost_estimate=pl.CostEstimate(flops=2 * n * d * width, bytes_accessed=2 * d * width, transcendentals=0),
    )(x, w, *residual)


def solution(mesh):
    def layer(x_a, route_a, gate_a, h_b, attn_b, route_b, gate_b, w_qkv, w_o, w_gate, w_up, w_down):
        me = lax.axis_index('ep').astype(I32).reshape(1)
        mid_b = dense(attn_b, w_o, [h_b])
        meta = jnp.concatenate([route_a.T.astype(F32), route_b.T.astype(F32), gate_a.T, gate_b.T], axis=0)
        meta, x_a = after((meta, x_a), mid_b)
        metas = [meta] + [swap(meta, k) for k in (1, 2, 3)]
        x_par, x_cnt = swap(x_a, 1), swap(x_a, 2)
        b_par, b_cnt = swap(mid_b, 1), swap(mid_b, 2)
        pos, tab, cnt = route(me, metas)

        h_loc = up(0, cnt, pos, (x_a, x_par, mid_b, b_par), w_gate, w_up)
        x_cnt, b_cnt = after((x_cnt, b_cnt), h_loc)
        x_dia, b_dia = swap(x_cnt, 1), swap(b_cnt, 1)
        mid, top = spread(after(tab, h_loc))
        keep, send = ffn(1, after(cnt, mid), tab, (x_cnt, x_dia, b_cnt, b_dia), w_down, pos=pos, wg=w_gate, wu=w_up)
        got = swap(send, 1)
        there = mix(there_mix, mid, (x_cnt, b_cnt), (keep, got))
        back = [swap(t, 2) for t in there]
        keep, send, qkv = ffn(0, after(cnt, there), tab, (x_a, x_par, mid_b, b_par), w_down, h_in=h_loc, xd=h_b, wq=w_qkv)
        got = swap(send, 1)
        out_a, out_b = mix(top_mix, top, (x_a, mid_b), (keep, got, *back))
        return out_a, out_b, qkv

    row = P(('dp', 'ep'), None)
    full = P(None, None)
    expert = P('ep', None, None)
    return jax.shard_map(
        layer, mesh=mesh,
        in_specs=(row,) * 7 + (full, full, expert, expert, expert),
        out_specs=(row, row, row), check_vma=False)
```

```python
import functools

import jax
import jax.numpy as jnp
from jax import lax
from jax.experimental import pallas as pl
from jax.experimental.pallas import tpu as pltpu
from jax.sharding import PartitionSpec as P


BF16, F32, I32 = jnp.bfloat16, jnp.float32, jnp.int32
N_SRC = 4
SLOTS = 128
HALF = 512
UP_ROWS = (320, 384, 448, 512)
DOWN_ROWS = ((384, 512), (384, 448, 512))
FC, DC = 640, 768
MIB = 2 ** 20

COL_POS, COL_BOTH, COL_OWN, COL_CNT, COL_TOP = 0, 16, 28, 31, 34


def swap(x, k):
    return lax.ppermute(x, 'ep', [(i, i ^ k) for i in range(N_SRC)])


def after(x, dep):
    return lax.optimization_barrier((x, dep))[0]


def route_kernel(me_ref, m0, m1, m2, m3, pos_ref, tab_ref, cnt_ref):
    me = me_ref[0]
    n_tok = m0.shape[1]
    before = (lax.broadcasted_iota(I32, (n_tok, n_tok), 0)
              < lax.broadcasted_iota(I32, (n_tok, n_tok), 1)).astype(BF16)
    metas = [m[...] for m in (m0, m1, m2, m3)]
    for mb in range(2):
        r0 = [m[2 * mb:2 * mb + 1] for m in metas]
        r1 = [m[2 * mb + 1:2 * mb + 2] for m in metas]
        g0 = [m[4 + 2 * mb:5 + 2 * mb] for m in metas]
        g1 = [m[5 + 2 * mb:6 + 2 * mb] for m in metas]
        sel, gate = [], []
        for l in range(2):
            e = (2 * me + l).astype(F32)
            for s in range(N_SRC):
                h0 = (r0[s] == e).astype(F32)
                h1 = (r1[s] == e).astype(F32)
                sel.append(h0 + h1)
                gate.append(h0 * g0[s] + h1 * g1[s])
        both = []
        for s in range(N_SRC):
            b = sel[s] + sel[N_SRC + s] > 1.5
            both += [b.astype(F32), jnp.where(b, gate[s], 1.0), jnp.where(b, gate[N_SRC + s], 1.0)]
        sel = jnp.concatenate(sel, axis=0)
        rank = jnp.dot(sel.astype(BF16), before, preferred_element_type=F32)
        pos = jnp.where(sel > 0, rank, -1.0)
        pos_ref[mb] = pos
        cnt_ref[mb] = jnp.broadcast_to(jnp.sum(sel, axis=1, keepdims=True), cnt_ref.shape[1:]).astype(I32)

        def owners(s):
            counts, gates = [], []
            for k in range(N_SRC):
                lo = (2 * jnp.bitwise_xor(me, k)).astype(F32)
                o0 = jnp.logical_or(r0[s] == lo, r0[s] == lo + 1).astype(F32)
                o1 = jnp.logical_or(r1[s] == lo, r1[s] == lo + 1).astype(F32)
                counts.append(o0 + o1)
                gates.append(o0 * g0[s] + o1 * g1[s])
            return counts, gates

        def coefs(mix, gates):
            return [jnp.where(mix, 1.0, 0.0)] + [jnp.where(mix, g, 1.0) for g in gates]

        c, g = owners(0)
        c2, g2 = owners(2)
        rows = [pos] + gate + both
        rows += coefs(jnp.logical_and(c[0] == 1.0, c[1] == 1.0), g[:2])
        rows += coefs(jnp.logical_and(c2[0] == 1.0, c2[1] == 1.0), g2[:2])
        rows += coefs(c[0] + c[1] == 1.0, [g[0] + g[1], g[2] + g[3]])
        rows = jnp.concatenate(rows + [jnp.zeros((128 - COL_TOP - 3, n_tok), F32)], axis=0)
        tab_ref[mb] = rows.T


def spread_kernel(tab, mid_ref, top_ref):
    for mb in range(2):
        t = tab[mb]
        for ref, cols in ((mid_ref, range(COL_CNT, COL_CNT + 3)),
                          (top_ref, [*range(COL_OWN, COL_OWN + 3), *range(COL_TOP, COL_TOP + 3)])):
            for k, c in enumerate(cols):
                ref[len(cols) * mb + k] = jnp.broadcast_to(t[:, c:c + 1], (t.shape[0], 128))


def spread(tab):
    n_tok = tab.shape[1]
    return pl.pallas_call(
        spread_kernel,
        out_shape=[jax.ShapeDtypeStruct((k, n_tok, 128), F32) for k in (6, 12)],
        cost_estimate=pl.CostEstimate(flops=10 ** 8, bytes_accessed=10 ** 6, transcendentals=0), name='spread',
    )(tab)


def route(me, metas):
    n_tok = metas[0].shape[1]
    return pl.pallas_call(
        route_kernel,
        out_shape=[jax.ShapeDtypeStruct((2, 8, n_tok), F32), jax.ShapeDtypeStruct((2, n_tok, 128), F32),
                   jax.ShapeDtypeStruct((2, 8, 128), I32)],
        in_specs=[pl.BlockSpec(memory_space=pltpu.SMEM)] + [pl.BlockSpec(memory_space=pltpu.VMEM)] * 4,
        out_specs=[pl.BlockSpec(memory_space=pltpu.VMEM)] * 3,
        name='route',
    )(me, *metas)


def offset(cnt, l, loc, k):
    off = 0
    for q in range(4 if not isinstance(k, int) else k):
        n = lax.div(cnt[q // 2, l * N_SRC + 2 * loc + q % 2, 0] + 15, 16) * 16
        off = off + (n if isinstance(k, int) else jnp.where(q < k, n, 0))
    return off


def for_rows(variants, m, body):
    lo = 0
    for rows in variants:
        pl.when(jnp.logical_and(m > lo, m <= rows))(functools.partial(body, rows))
        lo = rows


def up_step(loc, i, n, nc, cnt, pos, us, wg, wu, x, w, sem, h, whole):
    ns = w.shape[0]

    def copies(j):
        l, c, s = lax.div(j, nc), lax.rem(j, nc), lax.rem(j, ns)
        cols = pl.ds(pl.multiple_of(c * FC, 128), FC)
        return [pltpu.make_async_copy(wg.at[l, :, cols], w.at[s, :, pl.ds(0, FC)], sem.at[s, 0]),
                pltpu.make_async_copy(wu.at[l, :, cols], w.at[s, :, pl.ds(FC, FC)], sem.at[s, 1])]

    @pl.when(i == 0)
    def _():
        for j in range(ns - 1):
            for c in copies(j):
                c.start()

    @pl.when(i < 2)
    def _():
        x[i] = jnp.zeros(x.shape[1:], BF16)
        for k in range(4):
            p = pos[k // 2, pl.ds(i * N_SRC + 2 * loc + k % 2, 1), :]
            pick = (lax.broadcasted_iota(I32, (SLOTS, p.shape[1]), 0).astype(F32) == p).astype(BF16)
            rows = jnp.dot(pick, us[k][...], preferred_element_type=F32)
            x[i, pl.ds(pl.multiple_of(offset(cnt, i, loc, k), 16), SLOTS), :] = rows.astype(BF16)

    @pl.when(i + ns - 1 < n)
    def _():
        for c in copies(i + ns - 1):
            c.start()

    @pl.when(i < n)
    def _():
        for c in copies(i):
            c.wait()
        l, s = lax.div(i, nc), lax.rem(i, ns)
        cols = pl.ds(pl.multiple_of(lax.rem(i, nc) * FC, 128), FC)

        def body(rows):
            r = jnp.dot(x[l, :rows], w[s], preferred_element_type=F32)
            res = (jax.nn.silu(r[:, :FC]) * r[:, FC:]).astype(BF16)
            rest = jnp.zeros((HALF - rows, FC), BF16)
            if whole:
                h[l, :rows, cols] = res
                if rows < HALF:
                    h[l, rows:, cols] = rest
            else:
                h[0, :rows] = res
                if rows < HALF:
                    h[0, rows:] = rest

        for_rows(UP_ROWS, offset(cnt, l, loc, 4), body)


def up_kernel(loc, nc, cnt, pos, ua0, ua1, ub0, ub1, wg, wu, h, x, w, sem):
    up_step(loc, pl.program_id(0), 2 * nc, nc, cnt, pos, (ua0, ua1, ub0, ub1), wg, wu, x, w, sem, h, False)


def up(loc, cnt, pos, us, wg, wu):
    d, ff = wg.shape[1:]
    ns = 3
    vmem, hbm = pl.BlockSpec(memory_space=pltpu.VMEM), pl.BlockSpec(memory_space=pl.ANY)
    flops = 4 * d * ff * 2 * HALF
    return pl.pallas_call(
        functools.partial(up_kernel, loc, ff // FC),
        out_shape=jax.ShapeDtypeStruct((2, HALF, ff), BF16),
        grid_spec=pltpu.PrefetchScalarGridSpec(
            num_scalar_prefetch=1, grid=(2 * (ff // FC),), in_specs=[vmem] * 5 + [hbm, hbm],
            out_specs=pl.BlockSpec((1, HALF, FC), lambda i, c: (lax.div(i, ff // FC), 0, lax.rem(i, ff // FC))),
            scratch_shapes=[pltpu.VMEM((2, HALF, d), BF16), pltpu.VMEM((ns, d, 2 * FC), BF16),
                            pltpu.SemaphoreType.DMA((ns, 2))]),
        compiler_params=pltpu.CompilerParams(vmem_limit_bytes=63 * MIB),
        cost_estimate=pl.CostEstimate(flops=flops, bytes_accessed=flops // 512, transcendentals=0),
    )(cnt, pos, *us, wg, wu)


def ffn_kernel(loc, n0, n1, nc, cnt, tab, *refs):
    it = iter(refs)
    pos = next(it) if n1 else None
    us = [next(it) for _ in range(4)]
    wg, wu = (next(it), next(it)) if n1 else (None, None)
    h_in, xd, wq = (None, None, None) if n1 else [next(it) for _ in range(3)]
    wd, keep, send = next(it), next(it), next(it)
    dense_out = None if n1 else next(it)
    h, y, w2, pick, coef, s2 = [next(it) for _ in range(6)]
    x, w1, s1 = [next(it) for _ in range(3)] if n1 else (None,) * 3
    w0, s0, sh = (None, None, None) if n1 else [next(it) for _ in range(3)]
    i = pl.program_id(0)
    n_tok = tab.shape[1]
    j = i - n1 - n0
    n2 = pl.num_programs(0) - n1 - n0

    def copy2(j):
        cols = pl.ds(pl.multiple_of(lax.div(j, 2) * DC, 128), DC)
        return pltpu.make_async_copy(wd.at[lax.rem(j, 2), :, cols], w2.at[lax.rem(j, 2)], s2.at[lax.rem(j, 2)])

    def h_copy(e, rows):
        return pltpu.make_async_copy(h_in.at[e, pl.ds(0, rows)], h.at[e, pl.ds(0, rows)], sh.at[e])

    def h_copies(e, act):
        for_rows(DOWN_ROWS[loc], offset(cnt, e, loc, 4), lambda rows: act(h_copy(e, rows)))

    if not n1:
        def copy0(j):
            cols = pl.ds(pl.multiple_of(j * DC, 128), DC)
            return pltpu.make_async_copy(wq.at[:, cols], w0.at[lax.rem(j, 3)], s0.at[lax.rem(j, 3)])

        @pl.when(i == 0)
        def _():
            copy0(0).start()
            copy0(1).start()

        @pl.when(i + 2 < n0)
        def _():
            copy0(i + 2).start()

        @pl.when(i == 2)
        def _():
            h_copies(0, lambda c: c.start())

        @pl.when(i == 4)
        def _():
            h_copies(1, lambda c: c.start())

        @pl.when(i == 6)
        def _():
            copy2(0).start()

        @pl.when(i < n0)
        def _():
            copy0(i).wait()
            dense_out[...] = jnp.dot(xd[...], w0[lax.rem(i, 3)], preferred_element_type=F32).astype(BF16)

    @pl.when(i == 0)
    def _():
        y[...] = jnp.zeros_like(y)
        lane = lax.broadcasted_iota(I32, (n_tok, SLOTS), 1).astype(F32)
        for mb in range(2):
            t = tab[mb]
            for e in range(2):
                for par in range(2):
                    c = COL_POS + e * N_SRC + 2 * loc + par
                    pick[4 * mb + 2 * e + par] = (t[:, c:c + 1] == lane).astype(BF16)
            for par in range(2):
                for k in range(3):
                    c = COL_BOTH + 3 * (2 * loc + par) + k
                    coef[6 * mb + 3 * par + k] = jnp.broadcast_to(t[:, c:c + 1], (n_tok, 128))

    if n1:
        up_step(loc, i, n1, nc, cnt, pos, us, wg, wu, x, w1, s1, h, True)

        @pl.when(i == n1 - 2)
        def _():
            copy2(0).start()

    @pl.when(j >= 0)
    def _():
        l = lax.rem(j, 2)
        if not n1:
            @pl.when(j < 2)
            def _():
                for_rows(DOWN_ROWS[loc], offset(cnt, l, loc, 4), lambda rows: h_copy(l, rows).wait())

        @pl.when(j + 1 < n2)
        def _():
            copy2(j + 1).start()

        copy2(j).wait()

        def body(rows):
            y[l, :rows] = jnp.dot(h[l, :rows], w2[l], preferred_element_type=F32).astype(BF16)

        for_rows(DOWN_ROWS[loc], offset(cnt, l, loc, 4), body)

        @pl.when(l == 1)
        def _():
            def part(mb, carry):
                for par, out in enumerate((keep, send)):
                    vals = []
                    for e in range(2):
                        r0 = pl.multiple_of(offset(cnt, e, loc, 2 * mb + par), 16)
                        vals.append(jnp.dot(pick[4 * mb + 2 * e + par], y[e, pl.ds(r0, SLOTS), :],
                                            preferred_element_type=F32))
                    a, c0, c1 = [coef[6 * mb + 3 * par + k] for k in range(3)]
                    u = us[par], us[2 + par]
                    for c in lanes(DC):
                        if n1:
                            cols = pl.ds(pl.multiple_of(lax.div(j, 2) * DC + c.start, 128), 128)
                        else:
                            cols = c
                        uc = jnp.where(mb == 0, u[0][:, cols], u[1][:, cols]).astype(F32)
                        mixed = c0 * vals[0][:, c] + c1 * vals[1][:, c]
                        out[pl.ds(pl.multiple_of(mb * n_tok, 256), n_tok), c] = (a * uc + mixed).astype(BF16)
                return carry

            lax.fori_loop(0, 2, part, 0)


def ffn(loc, cnt, tab, us, wd, *, pos=None, wg=None, wu=None, h_in=None, xd=None, wq=None):
    n_tok, d = us[0].shape
    ff = wd.shape[1]
    nc = ff // FC
    n1 = 2 * nc if h_in is None else 0
    n0 = 0 if n1 else wq.shape[1] // DC
    ns1 = 2
    once = lambda a: pl.BlockSpec(a.shape, lambda i, c: (0,) * a.ndim, pipeline_mode=pl.Buffered(1))
    hbm = pl.BlockSpec(memory_space=pl.ANY)
    col = lambda i, c: (0, lax.div(jnp.maximum(i - n1 - n0, 0), 2))
    scratch = [pltpu.VMEM((2, HALF, ff), BF16), pltpu.VMEM((2, HALF, DC), BF16), pltpu.VMEM((2, ff, DC), BF16),
               pltpu.VMEM((8, n_tok, SLOTS), BF16), pltpu.VMEM((12, n_tok, 128), F32), pltpu.SemaphoreType.DMA((2,))]
    if n1:
        args = [tab, pos, *us, wg, wu, wd]
        specs = [once(tab), once(pos)] + [once(u) for u in us] + [hbm] * 3
        scratch += [pltpu.VMEM((2, HALF, d), BF16), pltpu.VMEM((ns1, d, 2 * FC), BF16), pltpu.SemaphoreType.DMA((ns1, 2))]
    else:
        args = [tab, *us, h_in, xd, wq, wd]
        specs = [once(tab)] + [pl.BlockSpec((n_tok, DC), col)] * 4 + [hbm, once(xd), hbm, hbm]
        scratch += [pltpu.VMEM((3, d, DC), BF16), pltpu.SemaphoreType.DMA((3,)), pltpu.SemaphoreType.DMA((2,))]
    outs = [jax.ShapeDtypeStruct((2 * n_tok, d), BF16)] * 2
    out_specs = [pl.BlockSpec((2 * n_tok, DC), col)] * 2
    if n0:
        outs.append(jax.ShapeDtypeStruct((n_tok, wq.shape[1]), BF16))
        out_specs.append(pl.BlockSpec((n_tok, DC), lambda i, c: (0, jnp.minimum(i, n0 - 1))))
    flops = (3 if h_in is not None else 6) * d * ff * 2 * HALF
    return pl.pallas_call(
        functools.partial(ffn_kernel, loc, n0, n1, nc), out_shape=outs,
        grid_spec=pltpu.PrefetchScalarGridSpec(num_scalar_prefetch=1, grid=(n0 + n1 + 2 * (d // DC),), in_specs=specs,
                                               out_specs=out_specs, scratch_shapes=scratch),
        compiler_params=pltpu.CompilerParams(vmem_limit_bytes=67043328),
        cost_estimate=pl.CostEstimate(flops=flops, bytes_accessed=flops // 512, transcendentals=0),
    )(cnt, *args)


def lincomb(c, k, q, u, a, b):
    return (c[k, q] * u.astype(F32) + (c[k + 1, q] * a.astype(F32) + c[k + 2, q] * b.astype(F32))).astype(BF16)


def lanes(width):
    return [slice(c * 128, (c + 1) * 128) for c in range(width // 128)]


def there_mix(coef, mb, q, u, keep, got):
    return lincomb(coef, 3 * mb, q, u, keep, got)


def top_mix(coef, mb, q, u, keep, got, back):
    return lincomb(coef, 6 * mb + 3, q, u, lincomb(coef, 6 * mb, q, u, keep, got), back)


def mix_kernel(fn, n_in, br, coef, *refs):
    srcs, outs = refs[:n_in], refs[n_in:n_in + 2]
    dst, (res, sem_i, sem_o) = refs[n_in + 2:2 * n_in + 2], refs[2 * n_in + 2:]
    n, d = outs[0].shape
    steps = n // br
    pick = [[(0, 0), (2, 0), (3, 0)], [(1, 0), (2, n), (3, n)]]
    if n_in > 4:
        pick = [pick[0] + [(4, 0)], pick[1] + [(5, 0)]]

    def rows(c, r0=0):
        return pl.ds(pl.multiple_of(r0 + c * br, 16), br)

    def loads(c, mb):
        return [pltpu.make_async_copy(srcs[q].at[rows(c, r0)], dst[q].at[rows(c, r0)], sem_i.at[c, mb, k])
                for k, (q, r0) in enumerate(pick[mb])]

    def save(c, mb):
        return pltpu.make_async_copy(res.at[mb, rows(c)], outs[mb].at[rows(c)], sem_o.at[c, mb])

    for c in range(steps):
        for mb in range(2):
            for copy in loads(c, mb):
                copy.start()

    def step(c, carry):
        for mb in range(2):
            for copy in loads(c, mb):
                copy.wait()
            for lane in lanes(d):
                res[mb, rows(c), lane] = fn(coef, mb, rows(c), *[dst[q][rows(c, r0), lane] for q, r0 in pick[mb]])
            save(c, mb).start()
        return carry

    lax.fori_loop(0, steps, step, 0)
    for c in range(steps):
        for mb in range(2):
            save(c, mb).wait()


def mix(fn, coef, us, rows):
    n, d = us[0].shape
    br = 128
    srcs = [*us, *rows]
    hbm = pl.BlockSpec(memory_space=pl.ANY)
    return pl.pallas_call(
        functools.partial(mix_kernel, fn, len(srcs), br), out_shape=[jax.ShapeDtypeStruct((n, d), BF16)] * 2,
        in_specs=[pl.BlockSpec(memory_space=pltpu.VMEM)] + [hbm] * len(srcs), out_specs=[hbm] * 2,
        scratch_shapes=[pltpu.VMEM(a.shape, BF16) for a in srcs]
        + [pltpu.VMEM((2, n, d), BF16), pltpu.SemaphoreType.DMA((n // br, 2, 4)), pltpu.SemaphoreType.DMA((n // br, 2))],
        compiler_params=pltpu.CompilerParams(vmem_limit_bytes=67043328),
        cost_estimate=pl.CostEstimate(flops=10 ** 9, bytes_accessed=10 ** 6, transcendentals=0),
    )(coef, *srcs)


def dense_kernel(x, w, *refs):
    p = jnp.dot(x[...], w[...], preferred_element_type=F32).astype(BF16)
    if len(refs) > 1:
        p = (refs[0][...].astype(F32) + p.astype(F32)).astype(BF16)
    refs[-1][...] = p


def dense(x, w, residual):
    n, d = x.shape
    width, bw = w.shape[1], 768
    cols = pl.BlockSpec((n, bw), lambda i: (0, i))
    return pl.pallas_call(
        dense_kernel, out_shape=jax.ShapeDtypeStruct((n, width), BF16), grid=(width // bw,),
        in_specs=[pl.BlockSpec((n, d), lambda i: (0, 0)),
                  pl.BlockSpec((d, bw), lambda i: (0, i))] + [cols] * len(residual),
        out_specs=cols,
        cost_estimate=pl.CostEstimate(flops=2 * n * d * width, bytes_accessed=2 * d * width, transcendentals=0),
    )(x, w, *residual)


def solution(mesh):
    def layer(x_a, route_a, gate_a, h_b, attn_b, route_b, gate_b, w_qkv, w_o, w_gate, w_up, w_down):
        me = lax.axis_index('ep').astype(I32).reshape(1)
        mid_b = dense(attn_b, w_o, [h_b])
        meta = jnp.concatenate([route_a.T.astype(F32), route_b.T.astype(F32), gate_a.T, gate_b.T], axis=0)
        meta, x_a = after((meta, x_a), mid_b)
        metas = [meta] + [swap(meta, k) for k in (1, 2, 3)]
        x_par, x_cnt = swap(x_a, 1), swap(x_a, 2)
        b_par, b_cnt = swap(mid_b, 1), swap(mid_b, 2)
        pos, tab, cnt = route(me, metas)

        h_loc = up(0, cnt, pos, (x_a, x_par, mid_b, b_par), w_gate, w_up)
        x_cnt, b_cnt = after((x_cnt, b_cnt), h_loc)
        x_dia, b_dia = swap(x_cnt, 1), swap(b_cnt, 1)
        mid, top = spread(after(tab, h_loc))
        keep, send = ffn(1, after(cnt, mid), tab, (x_cnt, x_dia, b_cnt, b_dia), w_down, pos=pos, wg=w_gate, wu=w_up)
        got = swap(send, 1)
        there = mix(there_mix, mid, (x_cnt, b_cnt), (keep, got))
        back = [swap(t, 2) for t in there]
        keep, send, qkv = ffn(0, after(cnt, there), tab, (x_a, x_par, mid_b, b_par), w_down, h_in=h_loc, xd=h_b, wq=w_qkv)
        got = swap(send, 1)
        out_a, out_b = mix(top_mix, top, (x_a, mid_b), (keep, got, *back))
        return out_a, out_b, qkv

    row = P(('dp', 'ep'), None)
    full = P(None, None)
    expert = P('ep', None, None)
    return jax.shard_map(
        layer, mesh=mesh,
        in_specs=(row,) * 7 + (full, full, expert, expert, expert),
        out_specs=(row, row, row), check_vma=False)
```

```python
import functools

import jax
import jax.numpy as jnp
from jax import lax
from jax.experimental import pallas as pl
from jax.experimental.pallas import tpu as pltpu
from jax.sharding import PartitionSpec as P


BF16, F32, I32 = jnp.bfloat16, jnp.float32, jnp.int32
N_SRC = 4
SLOTS = 128
HALF = 512
UP_ROWS = (320, 384, 448, 512)
DOWN_ROWS = ((384, 512), (384, 448, 512))
FC, DC = 640, 768
MIB = 2 ** 20

COL_POS, COL_BOTH, COL_OWN, COL_CNT, COL_TOP = 0, 16, 28, 31, 34


def swap(x, k):
    return lax.ppermute(x, 'ep', [(i, i ^ k) for i in range(N_SRC)])


def after(x, dep):
    return lax.optimization_barrier((x, dep))[0]


def route_kernel(me_ref, m0, m1, m2, m3, pos_ref, tab_ref, cnt_ref):
    me = me_ref[0]
    n_tok = m0.shape[1]
    before = (lax.broadcasted_iota(I32, (n_tok, n_tok), 0)
              < lax.broadcasted_iota(I32, (n_tok, n_tok), 1)).astype(BF16)
    metas = [m[...] for m in (m0, m1, m2, m3)]
    for mb in range(2):
        r0 = [m[2 * mb:2 * mb + 1] for m in metas]
        r1 = [m[2 * mb + 1:2 * mb + 2] for m in metas]
        g0 = [m[4 + 2 * mb:5 + 2 * mb] for m in metas]
        g1 = [m[5 + 2 * mb:6 + 2 * mb] for m in metas]
        sel, gate = [], []
        for l in range(2):
            e = (2 * me + l).astype(F32)
            for s in range(N_SRC):
                h0 = (r0[s] == e).astype(F32)
                h1 = (r1[s] == e).astype(F32)
                sel.append(h0 + h1)
                gate.append(h0 * g0[s] + h1 * g1[s])
        both = []
        for s in range(N_SRC):
            b = sel[s] + sel[N_SRC + s] > 1.5
            both += [b.astype(F32), jnp.where(b, gate[s], 1.0), jnp.where(b, gate[N_SRC + s], 1.0)]
        sel = jnp.concatenate(sel, axis=0)
        rank = jnp.dot(sel.astype(BF16), before, preferred_element_type=F32)
        pos = jnp.where(sel > 0, rank, -1.0)
        pos_ref[mb] = pos
        cnt_ref[mb] = jnp.broadcast_to(jnp.sum(sel, axis=1, keepdims=True), cnt_ref.shape[1:]).astype(I32)

        def owners(s):
            counts, gates = [], []
            for k in range(N_SRC):
                lo = (2 * jnp.bitwise_xor(me, k)).astype(F32)
                o0 = jnp.logical_or(r0[s] == lo, r0[s] == lo + 1).astype(F32)
                o1 = jnp.logical_or(r1[s] == lo, r1[s] == lo + 1).astype(F32)
                counts.append(o0 + o1)
                gates.append(o0 * g0[s] + o1 * g1[s])
            return counts, gates

        def coefs(mix, gates):
            return [jnp.where(mix, 1.0, 0.0)] + [jnp.where(mix, g, 1.0) for g in gates]

        c, g = owners(0)
        c2, g2 = owners(2)
        rows = [pos] + gate + both
        rows += coefs(jnp.logical_and(c[0] == 1.0, c[1] == 1.0), g[:2])
        rows += coefs(jnp.logical_and(c2[0] == 1.0, c2[1] == 1.0), g2[:2])
        rows += coefs(c[0] + c[1] == 1.0, [g[0] + g[1], g[2] + g[3]])
        rows = jnp.concatenate(rows + [jnp.zeros((128 - COL_TOP - 3, n_tok), F32)], axis=0)
        tab_ref[mb] = rows.T


def spread_kernel(tab, mid_ref, top_ref):
    for mb in range(2):
        t = tab[mb]
        for ref, cols in ((mid_ref, range(COL_CNT, COL_CNT + 3)),
                          (top_ref, [*range(COL_OWN, COL_OWN + 3), *range(COL_TOP, COL_TOP + 3)])):
            for k, c in enumerate(cols):
                ref[len(cols) * mb + k] = jnp.broadcast_to(t[:, c:c + 1], (t.shape[0], 128))


def spread(tab):
    n_tok = tab.shape[1]
    return pl.pallas_call(
        spread_kernel,
        out_shape=[jax.ShapeDtypeStruct((k, n_tok, 128), F32) for k in (6, 12)],
        cost_estimate=pl.CostEstimate(flops=10 ** 8, bytes_accessed=10 ** 6, transcendentals=0), name='spread',
    )(tab)


def route(me, metas):
    n_tok = metas[0].shape[1]
    return pl.pallas_call(
        route_kernel,
        out_shape=[jax.ShapeDtypeStruct((2, 8, n_tok), F32), jax.ShapeDtypeStruct((2, n_tok, 128), F32),
                   jax.ShapeDtypeStruct((2, 8, 128), I32)],
        in_specs=[pl.BlockSpec(memory_space=pltpu.SMEM)] + [pl.BlockSpec(memory_space=pltpu.VMEM)] * 4,
        out_specs=[pl.BlockSpec(memory_space=pltpu.VMEM)] * 3,
        name='route',
    )(me, *metas)


def offset(cnt, l, loc, k):
    off = 0
    for q in range(4 if not isinstance(k, int) else k):
        n = lax.div(cnt[q // 2, l * N_SRC + 2 * loc + q % 2, 0] + 15, 16) * 16
        off = off + (n if isinstance(k, int) else jnp.where(q < k, n, 0))
    return off


def for_rows(variants, m, body):
    lo = 0
    for rows in variants:
        pl.when(jnp.logical_and(m > lo, m <= rows))(functools.partial(body, rows))
        lo = rows


def up_step(loc, i, n, nc, cnt, pos, us, wg, wu, x, w, sem, u, sem_u, h, whole):
    ns = w.shape[0]

    def copies(j):
        l, c, s = lax.div(j, nc), lax.rem(j, nc), lax.rem(j, ns)
        cols = pl.ds(pl.multiple_of(c * FC, 128), FC)
        return [pltpu.make_async_copy(wg.at[l, :, cols], w.at[s, :, pl.ds(0, FC)], sem.at[s, 0]),
                pltpu.make_async_copy(wu.at[l, :, cols], w.at[s, :, pl.ds(FC, FC)], sem.at[s, 1])]

    @pl.when(i == 0)
    def _():
        tokens = [] if u is None else [pltpu.make_async_copy(us[k], u.at[k], sem_u.at[k]) for k in range(4)]
        for c in tokens:
            c.start()
        for j in range(ns - 1):
            for c in copies(j):
                c.start()
        for c in tokens:
            c.wait()

    @pl.when(i < 2)
    def _():
        x[i] = jnp.zeros(x.shape[1:], BF16)
        for k in range(4):
            p = pos[k // 2, pl.ds(i * N_SRC + 2 * loc + k % 2, 1), :]
            pick = (lax.broadcasted_iota(I32, (SLOTS, p.shape[1]), 0).astype(F32) == p).astype(BF16)
            rows = jnp.dot(pick, us[k][...] if u is None else u[k], preferred_element_type=F32)
            x[i, pl.ds(pl.multiple_of(offset(cnt, i, loc, k), 16), SLOTS), :] = rows.astype(BF16)

    @pl.when(i + ns - 1 < n)
    def _():
        for c in copies(i + ns - 1):
            c.start()

    @pl.when(i < n)
    def _():
        for c in copies(i):
            c.wait()
        l, s = lax.div(i, nc), lax.rem(i, ns)
        cols = pl.ds(pl.multiple_of(lax.rem(i, nc) * FC, 128), FC)

        def body(rows):
            r = jnp.dot(x[l, :rows], w[s], preferred_element_type=F32)
            res = (jax.nn.silu(r[:, :FC]) * r[:, FC:]).astype(BF16)
            rest = jnp.zeros((HALF - rows, FC), BF16)
            if whole:
                h[l, :rows, cols] = res
                if rows < HALF:
                    h[l, rows:, cols] = rest
            else:
                h[0, :rows] = res
                if rows < HALF:
                    h[0, rows:] = rest

        for_rows(UP_ROWS, offset(cnt, l, loc, 4), body)


def up_kernel(loc, nc, cnt, pos, ua0, ua1, ub0, ub1, wg, wu, h, x, w, sem):
    up_step(loc, pl.program_id(0), 2 * nc, nc, cnt, pos, (ua0, ua1, ub0, ub1), wg, wu, x, w, sem, None, None, h, False)


def up(loc, cnt, pos, us, wg, wu):
    d, ff = wg.shape[1:]
    ns = 3
    vmem, hbm = pl.BlockSpec(memory_space=pltpu.VMEM), pl.BlockSpec(memory_space=pl.ANY)
    flops = 4 * d * ff * 2 * HALF
    return pl.pallas_call(
        functools.partial(up_kernel, loc, ff // FC),
        out_shape=jax.ShapeDtypeStruct((2, HALF, ff), BF16),
        grid_spec=pltpu.PrefetchScalarGridSpec(
            num_scalar_prefetch=1, grid=(2 * (ff // FC),), in_specs=[vmem] * 5 + [hbm] * 2,
            out_specs=pl.BlockSpec((1, HALF, FC), lambda i, c: (lax.div(i, ff // FC), 0, lax.rem(i, ff // FC))),
            scratch_shapes=[pltpu.VMEM((2, HALF, d), BF16), pltpu.VMEM((ns, d, 2 * FC), BF16),
                            pltpu.SemaphoreType.DMA((ns, 2))]),
        compiler_params=pltpu.CompilerParams(vmem_limit_bytes=63 * MIB),
        cost_estimate=pl.CostEstimate(flops=flops, bytes_accessed=flops // 512, transcendentals=0),
    )(cnt, pos, *us, wg, wu)


def ffn_kernel(loc, n0, n1, nc, cnt, tab, *refs):
    it = iter(refs)
    pos = next(it) if n1 else None
    us = [next(it) for _ in range(4)]
    wg, wu = (next(it), next(it)) if n1 else (None, None)
    h_in, xd, wq = (None, None, None) if n1 else [next(it) for _ in range(3)]
    wd, keep, send = next(it), next(it), next(it)
    dense_out = None if n1 else next(it)
    h, y, w2, pick, coef, s2 = [next(it) for _ in range(6)]
    x, w1, s1, uv, su = [next(it) for _ in range(5)] if n1 else (None,) * 5
    w0, s0, sh = (None, None, None) if n1 else [next(it) for _ in range(3)]
    i = pl.program_id(0)
    n_tok = tab.shape[1]
    j = i - n1 - n0
    n2 = pl.num_programs(0) - n1 - n0

    def copy2(j):
        cols = pl.ds(pl.multiple_of(lax.div(j, 2) * DC, 128), DC)
        return pltpu.make_async_copy(wd.at[lax.rem(j, 2), :, cols], w2.at[lax.rem(j, 2)], s2.at[lax.rem(j, 2)])

    def h_copy(e, rows):
        return pltpu.make_async_copy(h_in.at[e, pl.ds(0, rows)], h.at[e, pl.ds(0, rows)], sh.at[e])

    def h_copies(e, act):
        for_rows(DOWN_ROWS[loc], offset(cnt, e, loc, 4), lambda rows: act(h_copy(e, rows)))

    if not n1:
        def copy0(j):
            cols = pl.ds(pl.multiple_of(j * DC, 128), DC)
            return pltpu.make_async_copy(wq.at[:, cols], w0.at[lax.rem(j, 3)], s0.at[lax.rem(j, 3)])

        @pl.when(i == 0)
        def _():
            copy0(0).start()
            copy0(1).start()

        @pl.when(i + 2 < n0)
        def _():
            copy0(i + 2).start()

        @pl.when(i == 2)
        def _():
            h_copies(0, lambda c: c.start())

        @pl.when(i == 4)
        def _():
            h_copies(1, lambda c: c.start())

        @pl.when(i == 6)
        def _():
            copy2(0).start()

        @pl.when(i < n0)
        def _():
            copy0(i).wait()
            dense_out[...] = jnp.dot(xd[...], w0[lax.rem(i, 3)], preferred_element_type=F32).astype(BF16)

    @pl.when(i == 0)
    def _():
        y[...] = jnp.zeros_like(y)
        lane = lax.broadcasted_iota(I32, (n_tok, SLOTS), 1).astype(F32)
        for mb in range(2):
            t = tab[mb]
            for e in range(2):
                for par in range(2):
                    c = COL_POS + e * N_SRC + 2 * loc + par
                    pick[4 * mb + 2 * e + par] = (t[:, c:c + 1] == lane).astype(BF16)
            for par in range(2):
                for k in range(3):
                    c = COL_BOTH + 3 * (2 * loc + par) + k
                    coef[6 * mb + 3 * par + k] = jnp.broadcast_to(t[:, c:c + 1], (n_tok, 128))

    if n1:
        up_step(loc, i, n1, nc, cnt, pos, us, wg, wu, x, w1, s1, uv, su, h, True)

        @pl.when(i == n1 - 2)
        def _():
            copy2(0).start()

    @pl.when(j >= 0)
    def _():
        l = lax.rem(j, 2)
        if not n1:
            @pl.when(j < 2)
            def _():
                for_rows(DOWN_ROWS[loc], offset(cnt, l, loc, 4), lambda rows: h_copy(l, rows).wait())

        @pl.when(j + 1 < n2)
        def _():
            copy2(j + 1).start()

        copy2(j).wait()

        def body(rows):
            y[l, :rows] = jnp.dot(h[l, :rows], w2[l], preferred_element_type=F32).astype(BF16)

        for_rows(DOWN_ROWS[loc], offset(cnt, l, loc, 4), body)

        @pl.when(l == 1)
        def _():
            def part(mb, carry):
                for par, out in enumerate((keep, send)):
                    vals = []
                    for e in range(2):
                        r0 = pl.multiple_of(offset(cnt, e, loc, 2 * mb + par), 16)
                        vals.append(jnp.dot(pick[4 * mb + 2 * e + par], y[e, pl.ds(r0, SLOTS), :],
                                            preferred_element_type=F32))
                    a, c0, c1 = [coef[6 * mb + 3 * par + k] for k in range(3)]
                    u = [uv.at[q] if n1 else us[q] for q in (par, 2 + par)]
                    for c in lanes(DC):
                        if n1:
                            cols = pl.ds(pl.multiple_of(lax.div(j, 2) * DC + c.start, 128), 128)
                        else:
                            cols = c
                        uc = jnp.where(mb == 0, u[0][:, cols], u[1][:, cols]).astype(F32)
                        mixed = c0 * vals[0][:, c] + c1 * vals[1][:, c]
                        out[pl.ds(pl.multiple_of(mb * n_tok, 256), n_tok), c] = (a * uc + mixed).astype(BF16)
                return carry

            lax.fori_loop(0, 2, part, 0)


def ffn(loc, cnt, tab, us, wd, *, pos=None, wg=None, wu=None, h_in=None, xd=None, wq=None):
    n_tok, d = us[0].shape
    ff = wd.shape[1]
    nc = ff // FC
    n1 = 2 * nc if h_in is None else 0
    n0 = 0 if n1 else wq.shape[1] // DC
    ns1 = 2
    once = lambda a: pl.BlockSpec(a.shape, lambda i, c: (0,) * a.ndim, pipeline_mode=pl.Buffered(1))
    hbm = pl.BlockSpec(memory_space=pl.ANY)
    col = lambda i, c: (0, lax.div(jnp.maximum(i - n1 - n0, 0), 2))
    scratch = [pltpu.VMEM((2, HALF, ff), BF16), pltpu.VMEM((2, HALF, DC), BF16), pltpu.VMEM((2, ff, DC), BF16),
               pltpu.VMEM((8, n_tok, SLOTS), BF16), pltpu.VMEM((12, n_tok, 128), F32), pltpu.SemaphoreType.DMA((2,))]
    if n1:
        args = [tab, pos, *us, wg, wu, wd]
        specs = [once(tab), once(pos)] + [hbm] * 7
        scratch += [pltpu.VMEM((2, HALF, d), BF16), pltpu.VMEM((ns1, d, 2 * FC), BF16), pltpu.SemaphoreType.DMA((ns1, 2)),
                    pltpu.VMEM((4,) + us[0].shape, BF16), pltpu.SemaphoreType.DMA((4,))]
    else:
        args = [tab, *us, h_in, xd, wq, wd]
        specs = [once(tab)] + [pl.BlockSpec((n_tok, DC), col)] * 4 + [hbm, once(xd), hbm, hbm]
        scratch += [pltpu.VMEM((3, d, DC), BF16), pltpu.SemaphoreType.DMA((3,)), pltpu.SemaphoreType.DMA((2,))]
    outs = [jax.ShapeDtypeStruct((2 * n_tok, d), BF16)] * 2
    out_specs = [pl.BlockSpec((2 * n_tok, DC), col)] * 2
    if n0:
        outs.append(jax.ShapeDtypeStruct((n_tok, wq.shape[1]), BF16))
        out_specs.append(pl.BlockSpec((n_tok, DC), lambda i, c: (0, jnp.minimum(i, n0 - 1))))
    flops = (3 if h_in is not None else 6) * d * ff * 2 * HALF
    return pl.pallas_call(
        functools.partial(ffn_kernel, loc, n0, n1, nc), out_shape=outs,
        grid_spec=pltpu.PrefetchScalarGridSpec(num_scalar_prefetch=1, grid=(n0 + n1 + 2 * (d // DC),), in_specs=specs,
                                               out_specs=out_specs, scratch_shapes=scratch),
        compiler_params=pltpu.CompilerParams(vmem_limit_bytes=67043328),
        cost_estimate=pl.CostEstimate(flops=flops, bytes_accessed=flops // 512, transcendentals=0),
    )(cnt, *args)


def lincomb(c, k, u, a, b):
    return (c[k] * u.astype(F32) + (c[k + 1] * a.astype(F32) + c[k + 2] * b.astype(F32))).astype(BF16)


def lanes(width):
    return [slice(c * 128, (c + 1) * 128) for c in range(width // 128)]


def there_mix(coef, u, rows, mb, r, c):
    keep, got = rows
    return lincomb(coef, 3 * mb, u[:, c], keep[r, c], got[r, c])


def top_mix(coef, u, rows, mb, r, c):
    keep, got = rows[:2]
    here = lincomb(coef, 6 * mb, u[:, c], keep[r, c], got[r, c])
    return lincomb(coef, 6 * mb + 3, u[:, c], here, rows[2 + mb][:, c])


def mix_kernel(fn, n_in, bw, coef, *refs):
    srcs, outs = refs[:n_in], refs[n_in:n_in + 2]
    dst, res, sem_i, sem_o = refs[n_in + 2:2 * n_in + 2], refs[2 * n_in + 2], refs[-2], refs[-1]
    n, d = srcs[0].shape
    steps = d // bw

    def cut(c, start=0, width=bw):
        return pl.ds(pl.multiple_of(c * bw + start, 128), width)

    def loads(c):
        return [pltpu.make_async_copy(s.at[:, cut(c)], t.at[:, cut(c)], sem_i.at[c, q])
                for q, (s, t) in enumerate(zip(srcs, dst))]

    def saves(c):
        return [pltpu.make_async_copy(res.at[mb, :, cut(c)], outs[mb].at[:, cut(c)], sem_o.at[c, mb]) for mb in range(2)]

    for c in range(steps):
        for copy in loads(c):
            copy.start()

    def step(c, carry):
        for copy in loads(c):
            copy.wait()
        for mb, save in enumerate(saves(c)):
            for lane in lanes(bw):
                cols = cut(c, lane.start, 128)
                res[mb, :, cols] = fn(coef, dst[mb], dst[2:], mb, slice(mb * n, (mb + 1) * n), cols)
            save.start()
        return carry

    lax.fori_loop(0, steps, step, 0)
    for c in range(steps):
        for copy in saves(c):
            copy.wait()


def mix(fn, coef, us, rows):
    n, d = us[0].shape
    bw = 384
    srcs = [*us, *rows]
    hbm = pl.BlockSpec(memory_space=pl.ANY)
    return pl.pallas_call(
        functools.partial(mix_kernel, fn, len(srcs), bw), out_shape=[jax.ShapeDtypeStruct((n, d), BF16)] * 2,
        in_specs=[pl.BlockSpec(memory_space=pltpu.VMEM)] + [hbm] * len(srcs), out_specs=[hbm] * 2,
        scratch_shapes=[pltpu.VMEM(a.shape, BF16) for a in srcs]
        + [pltpu.VMEM((2, n, d), BF16), pltpu.SemaphoreType.DMA((d // bw, len(srcs))), pltpu.SemaphoreType.DMA((d // bw, 2))],
        compiler_params=pltpu.CompilerParams(vmem_limit_bytes=67043328),
        cost_estimate=pl.CostEstimate(flops=10 ** 9, bytes_accessed=10 ** 6, transcendentals=0),
    )(coef, *srcs)


def dense_kernel(x, w, *refs):
    p = jnp.dot(x[...], w[...], preferred_element_type=F32).astype(BF16)
    if len(refs) > 1:
        p = (refs[0][...].astype(F32) + p.astype(F32)).astype(BF16)
    refs[-1][...] = p


def dense(x, w, residual):
    n, d = x.shape
    width, bw = w.shape[1], 768
    cols = pl.BlockSpec((n, bw), lambda i: (0, i))
    return pl.pallas_call(
        dense_kernel, out_shape=jax.ShapeDtypeStruct((n, width), BF16), grid=(width // bw,),
        in_specs=[pl.BlockSpec((n, d), lambda i: (0, 0)),
                  pl.BlockSpec((d, bw), lambda i: (0, i))] + [cols] * len(residual),
        out_specs=cols,
        cost_estimate=pl.CostEstimate(flops=2 * n * d * width, bytes_accessed=2 * d * width, transcendentals=0),
    )(x, w, *residual)


def solution(mesh):
    def layer(x_a, route_a, gate_a, h_b, attn_b, route_b, gate_b, w_qkv, w_o, w_gate, w_up, w_down):
        me = lax.axis_index('ep').astype(I32).reshape(1)
        mid_b = dense(attn_b, w_o, [h_b])
        meta = jnp.concatenate([route_a.T.astype(F32), route_b.T.astype(F32), gate_a.T, gate_b.T], axis=0)
        meta, x_a = after((meta, x_a), mid_b)
        metas = [meta] + [swap(meta, k) for k in (1, 2, 3)]
        x_par, x_cnt = swap(x_a, 1), swap(x_a, 2)
        b_par, b_cnt = swap(mid_b, 1), swap(mid_b, 2)
        pos, tab, cnt = route(me, metas)

        h_loc = up(0, cnt, pos, (x_a, x_par, mid_b, b_par), w_gate, w_up)
        x_cnt, b_cnt = after((x_cnt, b_cnt), h_loc)
        x_dia, b_dia = swap(x_cnt, 1), swap(b_cnt, 1)
        mid, top = spread(after(tab, h_loc))
        keep, send = ffn(1, after(cnt, mid), tab, (x_cnt, x_dia, b_cnt, b_dia), w_down, pos=pos, wg=w_gate, wu=w_up)
        got = swap(send, 1)
        there = mix(there_mix, mid, (x_cnt, b_cnt), (keep, got))
        back = [swap(t, 2) for t in there]
        keep, send, qkv = ffn(0, after(cnt, there), tab, (x_a, x_par, mid_b, b_par), w_down, h_in=h_loc, xd=h_b, wq=w_qkv)
        got = swap(send, 1)
        out_a, out_b = mix(top_mix, top, (x_a, mid_b), (keep, got, *back))
        return out_a, out_b, qkv

    row = P(('dp', 'ep'), None)
    full = P(None, None)
    expert = P('ep', None, None)
    return jax.shard_map(
        layer, mesh=mesh,
        in_specs=(row,) * 7 + (full, full, expert, expert, expert),
        out_specs=(row, row, row), check_vma=False)
```
